32 devices in a mesh: rep: 2 (over y), span: 2 (over core), seq: 4 (over z), tp: 2 (over x).
Axes of the slice: x: 2, y: 2, z: 4, core: 2. Of those that a mesh axis runs over, the one named last changes fastest.
Arguments:
- queries: bfloat16 [8, 512, 24, 128], P(('rep', 'span'), 'seq', 'tp'), parts along dimension 0, may hold values from -110 to 110
- key_states: bfloat16 [8, 512, 4, 128], P(('rep', 'span'), 'seq', 'tp'), parts along dimension 0, may hold values from -11 to 11
- value_states: bfloat16 [8, 512, 4, 128], P(('rep', 'span'), 'seq', 'tp'), parts along dimension 0, may hold values from -6 to 6
- out_weight: bfloat16 [3072, 6144], P('tp', 'seq'), may hold values from -0.109375 to 0.109375
- noise_table: float32 [64, 6144], P(None, 'tp'), may hold values from 0.5 to 2
- plan: int32 [8], P('rep'), parts along dimension 0, may hold values from 0 to 63
Outputs:
- branch_out: bfloat16 [8, 512, 6144], P(('rep', 'span'), 'seq', 'tp'), parts along dimension 0
The draws below stay inside these ranges and needn't reach their ends.
There are 2 independent parts, one for each index of `rep`. The reference program is written for one: setup_inputs(seed, part) draws one part's arguments, and reference() takes and returns one part's arrays. A program takes and returns all parts, laid end to end along the dimension named above; an argument that names none is the same for every part. Nothing has to cross between parts.
All inputs are finite; a program needn't handle non-finite values.
Results may differ from the reference program's by a relative error of at most 0.014.
Values may be sent and summed in bfloat16 or wider, within the bound.
A program may use at most 128 MiB of HBM per device.

```python
import jax
import jax.numpy as jnp
from jax import lax

D = 6144
QH = 24
KVH = 4
HD = 128
STEPS = 64
SPANS = 4
CTOK = 512


def draw_together(key):
    base = jax.random.fold_in(key, 11)
    first, second = jax.random.split(base, 2)
    query_all = 1.6 * jax.random.truncated_normal(first, -6.0, 6.0, (SPANS, CTOK, QH, HD), jnp.float32)
    key_all = 1.6 * jax.random.truncated_normal(second, -6.0, 6.0, (SPANS, CTOK, KVH, HD), jnp.float32)
    return (query_all, key_all)


def draw_queries(key, part):
    return draw_together(key)[0].astype(jnp.bfloat16)


def draw_key_states(key, part):
    return draw_together(key)[1].astype(jnp.bfloat16)


def place_ends(drawn, own_key, least, top_value):
    place = [jax.random.randint(jax.random.fold_in(own_key, axis), (), 0, length) for axis, length in enumerate(drawn.shape)]
    widest = drawn.shape.index(max(drawn.shape))
    next_to = place[:widest] + [(place[widest] + 1) % drawn.shape[widest]] + place[widest + 1:]
    return drawn.at[tuple(place)].set(least).at[tuple(next_to)].set(top_value)


def block_scale(rng, dims, cuts, low, top_value):
    factor_of, own = 1.0, jax.random.fold_in(rng, 6)
    for axis_at, blocks in cuts:
        steps = jnp.exp(jax.random.uniform(jax.random.fold_in(own, axis_at), (blocks,), jnp.float32, low / len(cuts), top_value / len(cuts)))
        factor_of = factor_of * jnp.repeat(steps, dims[axis_at] // blocks).reshape([-1 if axis == axis_at else 1 for axis in range(len(dims))])
    return factor_of


def bell_draw(stream_key, extent, width, reach, cuts=(), kind=jnp.bfloat16):
    values = width * jax.random.normal(stream_key, extent, jnp.float32)
    if cuts:
        values = values * block_scale(stream_key, extent, cuts, -0.22, 0.18)
    return jnp.clip(values, -reach, reach).astype(kind)


def setup_inputs(seed: int = 0, part: int = 0) -> dict:
    arg_keys = jax.random.split(jax.random.key(seed), 7)
    part_splits = jax.random.split(jax.random.fold_in(arg_keys[6], part), 7)
    return {
        "queries": draw_queries(jax.random.fold_in(jax.random.fold_in(arg_keys[6], part), 71), part),
        "key_states": draw_key_states(jax.random.fold_in(jax.random.fold_in(arg_keys[6], part), 71), part),
        "value_states": bell_draw(part_splits[2], (SPANS, CTOK, KVH, HD), 1.0, 6.0, ((0, 2), (1, 4), (2, 2))),
        "out_weight": bell_draw(arg_keys[3], (QH * HD, D), (QH * HD) ** -0.5, 0.109375, ((0, 2), (1, 4))),
        "noise_table": jnp.clip(0.5 + 1.5 * jax.random.uniform(arg_keys[4], (STEPS, D), jnp.float32) ** block_scale(arg_keys[4], (STEPS, D), ((1, 2),), -0.2, 0.2), 0.5, 2.0),
        "plan": place_ends(jax.random.randint(part_splits[5], (SPANS,), 0, STEPS), jax.random.fold_in(part_splits[5], 1), 0, STEPS - 1).astype(jnp.int32),
    }


def reference(queries, key_states, value_states, out_weight, noise_table, plan):
    per_kv = QH // KVH
    factor = HD ** -0.5
    pieces = []
    for span in range(SPANS):
        key_all = key_states[:span + 1].reshape((span + 1) * CTOK, KVH, HD)
        value_all = value_states[:span + 1].reshape((span + 1) * CTOK, KVH, HD)

        def head_attend(head, span=span, key_all=key_all, value_all=value_all):
            owner = (head // per_kv).astype(jnp.int32)
            query_rows = lax.dynamic_index_in_dim(queries[span], head, 1, keepdims=False)
            key_rows = lax.dynamic_index_in_dim(key_all, owner, 1, keepdims=False)
            value_rows = lax.dynamic_index_in_dim(value_all, owner, 1, keepdims=False)
            scores = jnp.dot(query_rows, key_rows.T, preferred_element_type=jnp.float32) * factor
            highest = jnp.max(scores, axis=1, keepdims=True)
            weights = jnp.exp(scores - highest)
            totals = jnp.sum(weights, axis=1, keepdims=True)
            mixed = jnp.dot(weights.astype(jnp.bfloat16), value_rows, preferred_element_type=jnp.float32)
            return mixed / totals

        heads_out = lax.map(head_attend, jnp.arange(QH, dtype=jnp.int32))
        pieces.append(jnp.transpose(heads_out, (1, 0, 2)).reshape(CTOK, QH * HD).astype(jnp.bfloat16))
    attn = jnp.stack(pieces)
    projected = jnp.dot(attn.reshape(SPANS * CTOK, QH * HD), out_weight, preferred_element_type=jnp.float32).reshape(SPANS, CTOK, D)
    picks = (plan[:, None] == jnp.arange(STEPS, dtype=jnp.int32)[None, :]).astype(jnp.float32)
    gates = jnp.dot(picks, noise_table, precision=lax.Precision.HIGHEST)
    return (projected * gates[:, None, :]).astype(jnp.bfloat16)
```

```python
import functools
import math

import jax
import jax.numpy as jnp
from jax import lax
from jax.experimental import pallas as pl
from jax.experimental.pallas import tpu as pltpu
from jax.sharding import PartitionSpec as P

MESH = pl.DeviceIdType.MESH


def fused_kernel(
    parts, keep, late, plan_ref, q_ref, kv_ref, noise_ref, w_ref, out_ref,
    kvbuf, wbuf, abuf, pbuf, xsend, xbuf, csend, cbuf,
    kv_send, kv_recv, kvc_send, kvc_recv, loc, wz_send, wz_recv, wf_send, wf_recv,
    wc_send, wc_recv, wy_send, wy_recv, x_send, x_recv, a_send, a_recv, c_send, c_recv,
):
    y, c = lax.axis_index("rep"), lax.axis_index("span")
    z, t = lax.axis_index("seq"), lax.axis_index("tp")
    n = lax.axis_size("seq")
    cores, tps = lax.axis_size("span"), lax.axis_size("tp")
    spans, heads, tok, hd = q_ref.shape
    kvh = kv_ref.shape[1]
    per_kv = heads // kvh
    depth, cols = w_ref.shape
    quarter = depth // (cores * lax.axis_size("rep"))
    sub = cols // parts
    owned = n // tps
    rows_own = spans * tok
    first = c * spans
    last = n - 1
    steps = last * parts
    scale = hd ** (-0.5) * math.log2(math.e)
    both = jnp.logical_and

    is_end = jnp.logical_or(z == 0, z == last)
    inward = jnp.where(2 * z < n, 1, -1)
    is_host = jnp.logical_or(z == 1, z == n - 2)
    guest = z - inward

    def wanted(r, s, j):
        far = (jnp.abs(s - r) - 1) * parts + j >= keep
        return jnp.logical_not(both(jnp.logical_or(r == 0, r == last), far))

    def whole(s, j):
        return both(is_host, both(s == guest, j >= late))

    def rows(yy, cc):
        return pl.ds(pl.multiple_of((yy * cores + cc) * quarter, quarter), quarter)

    def columns(j):
        return pl.ds(pl.multiple_of(j * sub, sub), sub)

    def remote(src, dst, send, recv, where):
        return pltpu.make_async_remote_copy(
            src_ref=src, dst_ref=dst, send_sem=send, recv_sem=recv,
            device_id=where, device_id_type=MESH,
        )

    def z_copy(s, j, way, own):
        dst = wbuf.at[s, j, rows(y, c)]
        src = w_ref.at[rows(y, c), columns(j)] if own else dst
        to = z - 1 if way == 0 else z + 1
        return remote(src, dst, wz_send.at[way, s, j], wz_recv.at[s, j], {"seq": to})

    def rest_copy(s, j):
        src = w_ref.at[rows(1 - y, c), columns(j)]
        return remote(
            src, wbuf.at[s, j, rows(1 - y, c)], wf_send.at[j], wf_recv.at[j], {"seq": z + inward}
        )

    def core_copy(s, j, kind):
        part = wbuf.at[s, j, rows(y if kind == 0 else 1 - y, c)]
        return remote(part, part, wc_send.at[kind, s, j], wc_recv.at[kind, s, j], {"span": 1 - c})

    def y_copy(s, j):
        part = wbuf.at[s, j, rows(y, c)]
        return remote(part, part, wy_send.at[s, j], wy_recv.at[s, j], {"rep": 1 - y})

    def x_copy(s, j, src):
        at = lax.rem(s, owned)
        return remote(
            src.at[at, j], xbuf.at[at, j], x_send.at[at, j], x_recv.at[at, j], {"tp": 1 - t}
        )

    def a_copy(i):
        src = abuf.at[pl.ds(pl.multiple_of(i * tok, tok), tok)]
        dst = abuf.at[pl.ds(pl.multiple_of(rows_own + i * tok, tok), tok)]
        return remote(src, dst, a_send.at[i], a_recv.at[i], {"seq": z + inward})

    def c_copy(s, j):
        at = lax.rem(s, owned)
        return remote(
            csend.at[at, j], cbuf.at[at, j], c_send.at[at, j], c_recv.at[at, j],
            {"seq": z - inward},
        )

    def kv_copy(s, way, own):
        dst = kvbuf.at[pl.ds(first, spans), :, :, s]
        to = z - 1 if way == 0 else z + 1
        return remote(kv_ref if own else dst, dst, kv_send.at[way, s], kv_recv.at[s], {"seq": to})

    def kv_core(s):
        part = kvbuf.at[pl.ds(0, spans), :, :, s]
        return remote(part, part, kvc_send.at[s], kvc_recv.at[s], {"span": 1 - c})

    def local_w(j):
        return pltpu.make_async_copy(w_ref.at[:, columns(j)], wbuf.at[z, j], loc.at[j])

    def local_kv():
        return pltpu.make_async_copy(
            kv_ref, kvbuf.at[pl.ds(first, spans), :, :, z], loc.at[parts]
        )

    reach = ((0, z > 0), (1, z < last))

    barrier = pltpu.get_barrier_semaphore()
    for way, ok in reach:
        @pl.when(ok)
        def _(way=way):
            to = z - 1 if way == 0 else z + 1
            pl.semaphore_signal(barrier, inc=1, device_id={"seq": to}, device_id_type=MESH)
    pl.semaphore_signal(barrier, inc=1, device_id={"rep": 1 - y}, device_id_type=MESH)
    pl.semaphore_signal(barrier, inc=1, device_id={"span": 1 - c}, device_id_type=MESH)
    pl.semaphore_signal(barrier, inc=1, device_id={"tp": 1 - t}, device_id_type=MESH)
    pl.semaphore_wait(barrier, jnp.where(is_end, 4, 5))

    for way, ok in reach:
        @pl.when(ok)
        def _(way=way):
            kv_copy(z, way, True).start()
    local_kv().start()
    for way, ok in reach:
        @pl.when(ok)
        def _(way=way):
            z_copy(z, 0, way, True).start()

    def own_weights(way, ok):
        @pl.when(ok)
        def _():
            for j in range(1, parts):
                z_copy(z, j, way, True).start()

    for d in range(n):
        if d == 0:
            local_kv().wait()

            @pl.when(c == 0)
            def _():
                kv_core(z).start()
        else:
            for sign in (-1, 1):
                s = z + sign * d

                @pl.when(both(s >= 0, s < n))
                def _(s=s, sign=sign):
                    way = 0 if sign > 0 else 1
                    kv_copy(s, way, False).wait_recv()

                    @pl.when(reach[way][1])
                    def _():
                        kv_copy(s, way, False).start()

                    @pl.when(c == 0)
                    def _():
                        kv_core(s).start()
        own_weights(0, both(z > 0, last - z == d))
        own_weights(1, both(z < last, z == d))
        if d == 0:
            for j in range(parts):
                local_w(j).start()

    @pl.when(c != 0)
    def _():
        for s in range(n):
            kv_core(s).wait_recv()

    def each(e, low, do):
        ok = both(e >= low, e < steps)
        d, j = e // parts + 1, e % parts
        for sign in (-1, 1):
            s = z + sign * d

            @pl.when(both(ok, both(s >= 0, s < n)))
            def _(s=s, sign=sign):
                do(s, j, sign)

    def arrive(s, j, sign):
        way = 0 if sign > 0 else 1

        @pl.when(wanted(z, s, j))
        def _():
            z_copy(s, j, way, False).wait_recv()

            @pl.when(both(reach[way][1], wanted(z - sign, s, j)))
            def _():
                z_copy(s, j, way, False).start()

            @pl.when(jnp.logical_not(whole(s, j)))
            def _():
                y_copy(s, j).start()

            core_copy(s, j, 0).start()

    def pass_on(s, j, sign):
        @pl.when(both(wanted(z, s, j), jnp.logical_not(whole(s, j))))
        def _():
            y_copy(s, j).wait_recv()
            core_copy(s, j, 1).start()

    def project(s, j):
        part = jnp.dot(
            abuf[pl.ds(0, rows_own)], wbuf[s, j], preferred_element_type=jnp.float32
        )
        at = lax.rem(s, owned)

        @pl.when(s // owned == t)
        def _():
            pbuf[at, j] = part

        @pl.when(s // owned != t)
        def _():
            xsend[at, j] = part.astype(jnp.bfloat16)
            x_copy(s, j, xsend).start()

    def project_guest(s, j):
        part = jnp.dot(
            abuf[pl.ds(rows_own, rows_own)], wbuf[s, j], preferred_element_type=jnp.float32
        )
        csend[lax.rem(s, owned), j] = part.astype(jnp.bfloat16)
        c_copy(s, j).start()

    def gathered(s, j):
        core_copy(s, j, 0).wait_recv()
        core_copy(s, j, 1).wait_recv()
        project(s, j)

    def gather_project(s, j, sign):
        @pl.when(both(wanted(z, s, j), jnp.logical_not(whole(s, j))))
        def _():
            gathered(s, j)

        @pl.when(jnp.logical_not(wanted(z, s, j)))
        def _():
            c_copy(s, j).wait_recv()

            @pl.when(s // owned != t)
            def _():
                x_copy(s, j, cbuf).start()

    def finish(s, j):
        @pl.when(s // owned == t)
        def _():
            x_copy(s, j, xsend).wait_recv()
            at = lax.rem(s, owned)
            where = pl.ds(pl.multiple_of(at * cols + j * sub, 128), sub)

            def put(mine):
                for i in range(spans):
                    level = plan_ref[first + i]
                    gate = noise_ref[pl.ds(level, 1), where]
                    span = pl.ds(i * tok, tok)
                    total = mine(at, span) + xbuf[at, j, span, :].astype(jnp.float32)
                    out_ref[span, where] = (total * gate).astype(out_ref.dtype)

            @pl.when(wanted(z, s, j))
            def _():
                put(lambda at, span: pbuf[at, j, span, :])

            @pl.when(jnp.logical_not(wanted(z, s, j)))
            def _():
                put(lambda at, span: cbuf[at, j, span, :].astype(jnp.float32))

    def finish_in_line(s, j, sign):
        @pl.when(jnp.logical_not(whole(s, j)))
        def _():
            finish(s, j)

    units = spans * kvh
    lag = 2
    lead = per_kv * tok

    def attend(u, carry):
        i, g = u // kvh, u % kvh
        query = q_ref[i, pl.ds(g * per_kv, per_kv)].reshape(lead, hd)

        def fold(k, state):
            top, total, mixed = state
            keys = kvbuf[k, g, 0].reshape(n * tok, hd)
            values = kvbuf[k, g, 1].reshape(n * tok, hd)
            scores = lax.dot_general(
                query, keys, (((1,), (1,)), ((), ())), preferred_element_type=jnp.float32
            )
            high = jnp.maximum(top, jnp.max(scores, axis=1, keepdims=True))
            shrink = jnp.exp2((top - high) * scale)
            weights = jnp.exp2((scores - high) * scale)
            total = total * shrink + jnp.sum(weights, axis=1, keepdims=True)
            mixed = mixed * shrink + jnp.dot(
                weights.astype(jnp.bfloat16), values, preferred_element_type=jnp.float32
            )
            return high, total, mixed

        start = (
            jnp.full((lead, 1), -1e30, jnp.float32),
            jnp.zeros((lead, 1), jnp.float32),
            jnp.zeros((lead, hd), jnp.float32),
        )
        _, total, mixed = lax.fori_loop(0, first + i + 1, fold, start)
        result = (mixed / total).astype(jnp.bfloat16).reshape(per_kv, tok, hd)
        for h in range(per_kv):
            abuf[
                pl.ds(pl.multiple_of(i * tok, tok), tok),
                pl.ds(pl.multiple_of((g * per_kv + h) * hd, hd), hd),
            ] = result[h]

        @pl.when(both(is_end, g == kvh - 1))
        def _():
            a_copy(i).start()

        each(u, 0, arrive)
        each(u - lag, 0, pass_on)
        return carry

    lax.fori_loop(0, units, attend, 0)

    @pl.when(is_end)
    def _():
        for j in range(late, parts):
            rest_copy(z, j).start()

    def own(j, carry):
        local_w(j).wait()
        project(z, j)
        return carry

    lax.fori_loop(0, parts, own, 0)

    turn = jnp.where(c == 0, 6, 7)
    due = 12
    own_done = 10

    def run(e, carry):
        each(e, units, arrive)
        each(e - lag, units - lag, pass_on)

        @pl.when(both(is_host, e == turn))
        def _():
            for i in range(spans):
                a_copy(i).wait_recv()

            def catch_up(f, carry):
                project_guest(z + inward * (f // parts + 1), f % parts)
                return carry

            lax.fori_loop(keep - parts, turn - lag - 1, catch_up, 0)

        each(e - lag - 1, 0, gather_project)
        f = e - lag - 1
        s = z + inward * (f // parts + 1)
        inside = both(f >= keep - parts, f < (n - 2) * parts)

        @pl.when(both(both(is_host, e >= turn), inside))
        def _():
            project_guest(s, f % parts)

        k = e - due + late

        @pl.when(both(is_host, both(k >= late, k < parts)))
        def _():
            rest_copy(guest, k).wait_recv()
            core_copy(guest, k, 1).start()

        @pl.when(both(is_host, both(k - 1 >= late, k - 1 < parts)))
        def _():
            gathered(guest, k - 1)

        each(e - lag - 3, 0, finish_in_line)

        @pl.when(both(is_host, both(k - 3 >= late, k - 3 < parts)))
        def _():
            finish(guest, k - 3)

        m = e - own_done

        @pl.when(both(m >= 0, m < parts))
        def _():
            finish(z, m)

        return carry

    lax.fori_loop(lag + 1, max(steps + lag + 3, due + parts - late + 3, own_done + parts), run, 0)

    for s in range(n):
        for way, ok in reach:
            @pl.when(both(ok, (z <= s) if way == 0 else (z >= s)))
            def _(s=s, way=way):
                kv_copy(s, way, False).wait_send()

        @pl.when(c == 0)
        def _(s=s):
            kv_core(s).wait_send()

    @pl.when(is_end)
    def _():
        for i in range(spans):
            a_copy(i).wait_send()
        for j in range(late, parts):
            rest_copy(z, j).wait_send()

    def drain(f, carry):
        s, j = f // parts, f % parts

        @pl.when(both(both(z > 0, s >= z), wanted(z - 1, s, j)))
        def _():
            z_copy(s, j, 0, False).wait_send()

        @pl.when(both(both(z < last, s <= z), wanted(z + 1, s, j)))
        def _():
            z_copy(s, j, 1, False).wait_send()

        @pl.when(both(s != z, wanted(z, s, j)))
        def _():
            core_copy(s, j, 0).wait_send()
            core_copy(s, j, 1).wait_send()

            @pl.when(jnp.logical_not(whole(s, j)))
            def _():
                y_copy(s, j).wait_send()

        @pl.when(s // owned != t)
        def _():
            x_copy(s, j, xsend).wait_send()

        @pl.when(both(is_host, both(s != z, jnp.logical_not(wanted(guest, s, j)))))
        def _():
            c_copy(s, j).wait_send()

        return carry

    lax.fori_loop(0, n * parts, drain, 0)


def fused(parts, queries, key_states, value_states, out_weight, noise_table, plan):
    spans, tok, heads, hd = queries.shape
    kvh = key_states.shape[2]
    depth, cols = out_weight.shape
    n, tps, cores = lax.axis_size("seq"), lax.axis_size("tp"), lax.axis_size("span")
    sub, owned, wide = cols // parts, n // tps, noise_table.shape[1]
    keep, late = parts, parts // 3
    q = jnp.transpose(queries, (0, 2, 1, 3))
    kv = jnp.stack([key_states, value_states], axis=0).transpose(1, 3, 0, 2, 4)
    vmem = pl.BlockSpec(memory_space=pltpu.VMEM)
    dma = pltpu.SemaphoreType.DMA
    tile = (owned, parts, spans * tok, sub)
    out = pl.pallas_call(
        functools.partial(fused_kernel, parts, keep, late),
        out_shape=jax.ShapeDtypeStruct((spans * tok, wide), jnp.bfloat16),
        in_specs=[
            pl.BlockSpec(memory_space=pltpu.SMEM), vmem, vmem, vmem,
            pl.BlockSpec(memory_space=pl.ANY),
        ],
        out_specs=vmem,
        scratch_shapes=[
            pltpu.VMEM((spans * cores, kvh, 2, n, tok, hd), jnp.bfloat16),
            pltpu.VMEM((n, parts, depth, sub), jnp.bfloat16),
            pltpu.VMEM((2 * spans * tok, depth), jnp.bfloat16),
            pltpu.VMEM(tile, jnp.float32),
            pltpu.VMEM(tile, jnp.bfloat16),
            pltpu.VMEM(tile, jnp.bfloat16),
            pltpu.VMEM(tile, jnp.bfloat16),
            pltpu.VMEM(tile, jnp.bfloat16),
            dma((2, n)), dma((n,)), dma((n,)), dma((n,)), dma((parts + 1,)),
            dma((2, n, parts)), dma((n, parts)), dma((parts,)), dma((parts,)),
            dma((2, n, parts)), dma((2, n, parts)), dma((n, parts)), dma((n, parts)),
            dma((owned, parts)), dma((owned, parts)), dma((spans,)), dma((spans,)),
            dma((owned, parts)), dma((owned, parts)),
        ],
        compiler_params=pltpu.CompilerParams(
            collective_id=0, has_side_effects=True, vmem_limit_bytes=60 * 1024 * 1024
        ),
        name="relay_attention",
    )(plan, q, kv, noise_table, out_weight)
    return out.reshape(spans, tok, wide)


def fold_block(carried, query_rows, key_rows, value_rows, factor):
    maxima, totals, weighted = carried
    scores = (
        jnp.einsum("tkgd,skd->tkgs", query_rows, key_rows, preferred_element_type=jnp.float32)
        * factor
    )
    highest = jnp.maximum(maxima, jnp.max(scores, axis=-1))
    shrink = jnp.exp(maxima - highest)
    weights = jnp.exp(scores - highest[..., None])
    totals = totals * shrink + jnp.sum(weights, axis=-1)
    weighted = weighted * shrink[..., None] + jnp.einsum(
        "tkgs,skd->tkgd",
        weights.astype(jnp.bfloat16),
        value_rows,
        preferred_element_type=jnp.float32,
    )
    return (maxima * 0.0 + highest, totals, weighted)


def per_device(queries, key_states, value_states, out_weight, noise_table, plan):
    ch_dev, tok_dev, heads_local, head_size = queries.shape
    kv_local = key_states.shape[2]
    per_kv = heads_local // kv_local
    span_count = ch_dev * lax.axis_size("span")
    first_span = lax.axis_index("span") * ch_dev
    factor = head_size ** (-0.5)
    grouped = queries.reshape(ch_dev, tok_dev, kv_local, per_kv, head_size)
    start_max = jnp.full((ch_dev, tok_dev, kv_local, per_kv), -1e30, jnp.float32)
    start_tot = jnp.zeros((ch_dev, tok_dev, kv_local, per_kv), jnp.float32)
    start_acc = jnp.zeros((ch_dev, tok_dev, kv_local, per_kv, head_size), jnp.float32)
    span_rows = (
        lax.all_gather(key_states, "seq", axis=1, tiled=True),
        lax.all_gather(value_states, "seq", axis=1, tiled=True),
    )
    key_piece = lax.all_gather(span_rows[0], "span", axis=0, tiled=True)
    value_piece = lax.all_gather(span_rows[1], "span", axis=0, tiled=True)
    new_max = []
    new_tot = []
    new_acc = []
    for q_span in range(ch_dev):
        inner_state = (start_max[q_span], start_tot[q_span], start_acc[q_span])
        for k_span in range(span_count):

            def update(inner, q_span=q_span, k_span=k_span):
                return fold_block(
                    inner, grouped[q_span], key_piece[k_span], value_piece[k_span], factor
                )

            inner_state = lax.cond(
                k_span <= first_span + q_span, update, lambda inner: inner, inner_state
            )
        new_max.append(inner_state[0])
        new_tot.append(inner_state[1])
        new_acc.append(inner_state[2])
    attn = (
        (jnp.stack(new_acc) / jnp.stack(new_tot)[..., None])
        .reshape(ch_dev, tok_dev, heads_local * head_size)
        .astype(jnp.bfloat16)
    )
    columns = jnp.einsum(
        "ctf,fo->cto",
        lax.all_gather(attn, "seq", axis=1, tiled=True),
        out_weight,
        preferred_element_type=jnp.float32,
    )
    partial_out = lax.all_to_all(
        columns.astype(jnp.bfloat16), "seq", split_axis=1, concat_axis=2, tiled=True
    ).astype(columns.dtype)
    summed = lax.psum_scatter(
        partial_out.astype(jnp.bfloat16), "tp", scatter_dimension=2, tiled=True
    ).astype(jnp.float32)
    levels = lax.dynamic_slice_in_dim(plan, first_span, ch_dev)
    picks = (levels[:, None] == jnp.arange(noise_table.shape[0], dtype=jnp.int32)[None, :]).astype(
        jnp.float32
    )
    gates = jnp.dot(picks, noise_table, precision=lax.Precision.HIGHEST)
    return (summed * gates[:, None, :]).astype(jnp.bfloat16)


def choose_parts(cols):
    for parts in (6, 3, 2, 1):
        if cols % (parts * 128) == 0:
            return parts
    return 0


def dispatch(queries, key_states, value_states, out_weight, noise_table, plan):
    depth, cols = out_weight.shape
    copies = lax.axis_size("rep") * lax.axis_size("span")
    parts = choose_parts(cols)
    pairs = all(lax.axis_size(name) == 2 for name in ("rep", "span", "tp"))
    args = (queries, key_states, value_states, out_weight, noise_table, plan)
    line = lax.axis_size("seq") == 2 * lax.axis_size("tp")
    if pairs and parts and depth % (copies * 16) == 0 and line:
        return fused(parts, *args)
    return per_device(*args)


def solution(mesh):
    placed = (
        P(("rep", "span"), "seq", "tp", None),
        P(("rep", "span"), "seq", "tp", None),
        P(("rep", "span"), "seq", "tp", None),
        P("tp", "seq"),
        P(None, "tp"),
        P("rep"),
    )
    return jax.shard_map(
        dispatch,
        mesh=mesh,
        in_specs=placed,
        out_specs=P(("rep", "span"), "seq", "tp"),
        check_vma=False,
    )
```

```python
import functools
import math

import jax
import jax.numpy as jnp
from jax import lax
from jax.experimental import pallas as pl
from jax.experimental.pallas import tpu as pltpu
from jax.sharding import PartitionSpec as P

MESH = pl.DeviceIdType.MESH


def fused_kernel(
    parts, keep, late, ahead, plan_ref, q_ref, kv_ref, noise_ref, w_ref, out_ref,
    kvbuf, wbuf, abuf, pbuf, xsend, xbuf, csend, cbuf,
    kv_send, kv_recv, kvc_send, kvc_recv, loc, wz_send, wz_recv, wf_send, wf_recv,
    wc_send, wc_recv, wy_send, wy_recv, x_send, x_recv, a_send, a_recv, c_send, c_recv,
):
    y, c = lax.axis_index("rep"), lax.axis_index("span")
    z, t = lax.axis_index("seq"), lax.axis_index("tp")
    n = lax.axis_size("seq")
    cores, tps = lax.axis_size("span"), lax.axis_size("tp")
    spans, heads, tok, hd = q_ref.shape
    kvh = kv_ref.shape[1]
    per_kv = heads // kvh
    depth, cols = w_ref.shape
    quarter = depth // (cores * lax.axis_size("rep"))
    sub = cols // parts
    owned = n // tps
    rows_own = spans * tok
    first = c * spans
    last = n - 1
    steps = last * parts
    scale = hd ** (-0.5) * math.log2(math.e)
    both = jnp.logical_and

    is_end = jnp.logical_or(z == 0, z == last)
    inward = jnp.where(2 * z < n, 1, -1)
    is_host = jnp.logical_or(z == 1, z == n - 2)
    guest = z - inward

    def place(r, s, j):
        return (jnp.abs(s - r) - 1) * parts + j - keep

    def wanted(r, s, j):
        far = place(r, s, j) >= 0
        return jnp.logical_not(both(jnp.logical_or(r == 0, r == last), far))

    def whole(s, j):
        return both(is_host, both(s == guest, j >= late))

    def rows(yy, cc):
        return pl.ds(pl.multiple_of((yy * cores + cc) * quarter, quarter), quarter)

    def columns(j):
        return pl.ds(pl.multiple_of(j * sub, sub), sub)

    def remote(src, dst, send, recv, where):
        return pltpu.make_async_remote_copy(
            src_ref=src, dst_ref=dst, send_sem=send, recv_sem=recv,
            device_id=where, device_id_type=MESH,
        )

    def z_copy(s, j, way, own):
        dst = wbuf.at[s, j, rows(y, c)]
        src = w_ref.at[rows(y, c), columns(j)] if own else dst
        to = z + 2 * way - 1
        return remote(src, dst, wz_send.at[way, s, j], wz_recv.at[s, j], {"seq": to})

    def rest_copy(s, j):
        src = w_ref.at[rows(1 - y, c), columns(j)]
        return remote(
            src, wbuf.at[s, j, rows(1 - y, c)], wf_send.at[j], wf_recv.at[j], {"seq": z + inward}
        )

    def core_copy(s, j, kind):
        part = wbuf.at[s, j, rows(y if kind == 0 else 1 - y, c)]
        return remote(part, part, wc_send.at[kind, s, j], wc_recv.at[kind, s, j], {"span": 1 - c})

    def y_copy(s, j):
        part = wbuf.at[s, j, rows(y, c)]
        return remote(part, part, wy_send.at[s, j], wy_recv.at[s, j], {"rep": 1 - y})

    def x_copy(s, j, src):
        at = lax.rem(s, owned)
        return remote(
            src, xbuf.at[at, j], x_send.at[at, j], x_recv.at[at, j], {"tp": 1 - t}
        )

    def a_copy(i):
        src = abuf.at[pl.ds(pl.multiple_of(i * tok, tok), tok)]
        dst = abuf.at[pl.ds(pl.multiple_of(rows_own + i * tok, tok), tok)]
        return remote(src, dst, a_send.at[i], a_recv.at[i], {"seq": z + inward})

    def c_copy(f):
        return remote(
            csend.at[f], cbuf.at[f], c_send.at[f], c_recv.at[f], {"seq": z - inward}
        )

    def kv_copy(s, g, way, own):
        dst = kvbuf.at[pl.ds(first, spans), g, :, s]
        src = kv_ref.at[:, g] if own else dst
        to = z - 1 if way == 0 else z + 1
        return remote(src, dst, kv_send.at[way, s, g], kv_recv.at[s, g], {"seq": to})

    def kv_core(s, g):
        part = kvbuf.at[pl.ds(0, spans), g, :, s]
        return remote(part, part, kvc_send.at[s, g], kvc_recv.at[s, g], {"span": 1 - c})

    def local_w(j):
        return pltpu.make_async_copy(w_ref.at[:, columns(j)], wbuf.at[z, j], loc.at[j])

    def local_kv():
        return pltpu.make_async_copy(
            kv_ref, kvbuf.at[pl.ds(first, spans), :, :, z], loc.at[parts]
        )

    reach = ((0, z > 0), (1, z < last))

    barrier = pltpu.get_barrier_semaphore()
    for way, ok in reach:
        @pl.when(ok)
        def _(way=way):
            to = z - 1 if way == 0 else z + 1
            pl.semaphore_signal(barrier, inc=1, device_id={"seq": to}, device_id_type=MESH)
    pl.semaphore_signal(barrier, inc=1, device_id={"rep": 1 - y}, device_id_type=MESH)
    pl.semaphore_signal(barrier, inc=1, device_id={"span": 1 - c}, device_id_type=MESH)
    pl.semaphore_signal(barrier, inc=1, device_id={"tp": 1 - t}, device_id_type=MESH)
    pl.semaphore_wait(barrier, jnp.where(is_end, 4, 5))

    for g in range(kvh):
        for way, ok in reach:
            @pl.when(ok)
            def _(g=g, way=way):
                kv_copy(z, g, way, True).start()
    local_kv().start()

    def own_weights(way, low, high, ok):
        for j in range(low, high):
            @pl.when(both(ok, wanted(z + 2 * way - 1, z, j)))
            def _(j=j):
                z_copy(z, j, way, True).start()

    for d in range(n):
        for g in range(kvh):
            if d == 0:
                if g == 0:
                    local_kv().wait()

                @pl.when(c == 0)
                def _(g=g):
                    kv_core(z, g).start()

                continue
            for sign in (-1, 1):
                s = z + sign * d

                @pl.when(both(s >= 0, s < n))
                def _(s=s, sign=sign, g=g):
                    way = 0 if sign > 0 else 1
                    kv_copy(s, g, way, False).wait_recv()

                    @pl.when(reach[way][1])
                    def _():
                        kv_copy(s, g, way, False).start()

                    @pl.when(c == 0)
                    def _():
                        kv_core(s, g).start()
        if d == 0:
            own_weights(0, 0, ahead, z == last)
            own_weights(1, 0, ahead, z == 0)
            for j in range(parts):
                local_w(j).start()
        else:
            own_weights(0, 0, parts, both(z > 0, last - z == d))
            own_weights(1, 0, parts, both(z < last, z == d))

    @pl.when(c != 0)
    def _():
        for s in range(n):
            for g in range(kvh):
                kv_core(s, g).wait_recv()

    def each(e, low, do):
        ok = both(e >= low, e < steps)
        d, j = e // parts + 1, e % parts
        for sign in (-1, 1):
            s = z + sign * d

            @pl.when(both(ok, both(s >= 0, s < n)))
            def _(s=s, sign=sign):
                do(s, j, sign)

    def arrive(s, j, sign):
        way = (1 - sign) // 2
        onward = z - sign

        @pl.when(wanted(z, s, j))
        def _():
            z_copy(s, j, way, False).wait_recv()

            @pl.when(both(both(onward >= 0, onward < n), wanted(onward, s, j)))
            def _():
                z_copy(s, j, way, False).start()

            @pl.when(jnp.logical_not(whole(s, j)))
            def _():
                y_copy(s, j).start()

            core_copy(s, j, 0).start()

    def arrive_in_line(s, j, sign):
        @pl.when(jnp.logical_not(both(is_host, both(s == guest, j >= ahead))))
        def _():
            arrive(s, j, sign)

    def pass_on(s, j, sign):
        @pl.when(both(wanted(z, s, j), jnp.logical_not(whole(s, j))))
        def _():
            y_copy(s, j).wait_recv()
            core_copy(s, j, 1).start()

    def project(s, j):
        part = jnp.dot(
            abuf[pl.ds(0, rows_own)], wbuf[s, j], preferred_element_type=jnp.float32
        )
        at = lax.rem(s, owned)

        @pl.when(s // owned == t)
        def _():
            pbuf[at, j] = part

        @pl.when(s // owned != t)
        def _():
            xsend[at, j] = part.astype(jnp.bfloat16)
            x_copy(s, j, xsend.at[at, j]).start()

    def project_guest(s, j):
        part = jnp.dot(
            abuf[pl.ds(rows_own, rows_own)], wbuf[s, j], preferred_element_type=jnp.float32
        )
        f = place(guest, s, j)
        csend[f] = part.astype(jnp.bfloat16)
        c_copy(f).start()

    def gathered(s, j):
        core_copy(s, j, 0).wait_recv()
        core_copy(s, j, 1).wait_recv()
        project(s, j)

    def gather_project(s, j, sign):
        @pl.when(both(wanted(z, s, j), jnp.logical_not(whole(s, j))))
        def _():
            gathered(s, j)

        @pl.when(jnp.logical_not(wanted(z, s, j)))
        def _():
            f = place(z, s, j)
            c_copy(f).wait_recv()

            @pl.when(s // owned != t)
            def _():
                x_copy(s, j, cbuf.at[f]).start()

    mine = t * owned
    near = z // owned == t
    front = jnp.where(near, z, jnp.where(inward > 0, mine, mine + owned - 1))
    rear = 2 * mine + owned - 1 - front

    def finish(q):
        s, j = jnp.where(q < parts, front, rear), lax.rem(q, parts)
        at = lax.rem(s, owned)
        x_copy(s, j, xsend.at[at, j]).wait_recv()
        where = pl.ds(pl.multiple_of(at * cols + j * sub, 128), sub)

        def put(own):
            for i in range(spans):
                level = plan_ref[first + i]
                gate = noise_ref[pl.ds(level, 1), where]
                span = pl.ds(i * tok, tok)
                total = own(span) + xbuf[at, j, span, :].astype(jnp.float32)
                out_ref[span, where] = (total * gate).astype(out_ref.dtype)

        @pl.when(wanted(z, s, j))
        def _():
            put(lambda span: pbuf[at, j, span, :])

        @pl.when(jnp.logical_not(wanted(z, s, j)))
        def _():
            put(lambda span: cbuf[place(z, s, j), span, :].astype(jnp.float32))

    units = spans * kvh
    lag = 2
    lead = per_kv * tok

    def attend(u, carry):
        i, g = u // kvh, u % kvh
        query = q_ref[i, pl.ds(g * per_kv, per_kv)].reshape(lead, hd)

        def fold(k, state):
            top, total, mixed = state
            keys = kvbuf[k, g, 0].reshape(n * tok, hd)
            values = kvbuf[k, g, 1].reshape(n * tok, hd)
            scores = lax.dot_general(
                query, keys, (((1,), (1,)), ((), ())), preferred_element_type=jnp.float32
            )
            high = jnp.maximum(top, jnp.max(scores, axis=1, keepdims=True))
            shrink = jnp.exp2((top - high) * scale)
            weights = jnp.exp2((scores - high) * scale)
            total = total * shrink + jnp.sum(weights, axis=1, keepdims=True)
            mixed = mixed * shrink + jnp.dot(
                weights.astype(jnp.bfloat16), values, preferred_element_type=jnp.float32
            )
            return high, total, mixed

        start = (
            jnp.full((lead, 1), -1e30, jnp.float32),
            jnp.zeros((lead, 1), jnp.float32),
            jnp.zeros((lead, hd), jnp.float32),
        )
        _, total, mixed = lax.fori_loop(0, first + i + 1, fold, start)
        result = (mixed / total).astype(jnp.bfloat16).reshape(per_kv, tok, hd)
        for h in range(per_kv):
            abuf[
                pl.ds(pl.multiple_of(i * tok, tok), tok),
                pl.ds(pl.multiple_of((g * per_kv + h) * hd, hd), hd),
            ] = result[h]

        @pl.when(both(is_end, g == kvh - 1))
        def _():
            a_copy(i).start()

        each(u, 0, arrive_in_line)
        return carry

    lax.fori_loop(0, units, attend, 0)

    own_weights(0, ahead, parts, z == last)
    own_weights(1, ahead, parts, z == 0)

    @pl.when(is_end)
    def _():
        for j in range(late, parts):
            rest_copy(z, j).start()

    def own(j, carry):
        local_w(j).wait()
        project(z, j)
        return carry

    lax.fori_loop(0, parts, own, 0)

    turn = jnp.where(c == 0, 4, 6)
    shift, due, sums = 4, 2 * parts, 2 * parts

    def run(e, carry):
        each(e, units, arrive_in_line)
        k = e - shift

        @pl.when(both(is_host, both(k >= ahead, k < parts)))
        def _():
            arrive(guest, k, -inward)

        each(e - lag, 0, pass_on)

        @pl.when(both(is_host, e == turn))
        def _():
            for i in range(spans):
                a_copy(i).wait_recv()

            def catch_up(f, carry):
                project_guest(z + inward * (f // parts), f % parts)
                return carry

            lax.fori_loop(keep, turn - lag - 1 + parts, catch_up, 0)

        each(e - lag - 1, 0, gather_project)
        f = e - lag - 1 + parts

        @pl.when(both(both(is_host, e >= turn), f < (n - 1) * parts))
        def _():
            project_guest(z + inward * (f // parts), f % parts)

        k = e - due + late

        @pl.when(both(is_host, both(k >= late, k < parts)))
        def _():
            rest_copy(guest, k).wait_recv()
            core_copy(guest, k, 1).start()

        @pl.when(both(is_host, both(k - 1 >= late, k - 1 < parts)))
        def _():
            gathered(guest, k - 1)

        q = e - sums

        @pl.when(both(q >= 0, q < owned * parts))
        def _():
            finish(q)

        return carry

    lax.fori_loop(lag, max(steps + lag + 1, due + parts - late + 1, sums + owned * parts), run, 0)

    for s in range(n):
        for way, ok in reach:
            @pl.when(both(ok, (z <= s) if way == 0 else (z >= s)))
            def _(s=s, way=way):
                for g in range(kvh):
                    kv_copy(s, g, way, False).wait_send()

        @pl.when(c == 0)
        def _(s=s):
            for g in range(kvh):
                kv_core(s, g).wait_send()

    @pl.when(is_end)
    def _():
        for i in range(spans):
            a_copy(i).wait_send()
        for j in range(late, parts):
            rest_copy(z, j).wait_send()

    def drain(f, carry):
        s, j = f // parts, f % parts

        @pl.when(both(both(z > 0, s >= z), wanted(z - 1, s, j)))
        def _():
            z_copy(s, j, 0, False).wait_send()

        @pl.when(both(both(z < last, s <= z), wanted(z + 1, s, j)))
        def _():
            z_copy(s, j, 1, False).wait_send()

        @pl.when(both(s != z, wanted(z, s, j)))
        def _():
            core_copy(s, j, 0).wait_send()
            core_copy(s, j, 1).wait_send()

            @pl.when(jnp.logical_not(whole(s, j)))
            def _():
                y_copy(s, j).wait_send()

        @pl.when(s // owned != t)
        def _():
            x_copy(s, j, xsend.at[lax.rem(s, owned), j]).wait_send()

        @pl.when(both(is_host, jnp.logical_not(wanted(guest, s, j))))
        def _():
            c_copy(place(guest, s, j)).wait_send()

        return carry

    lax.fori_loop(0, n * parts, drain, 0)


def fused(parts, queries, key_states, value_states, out_weight, noise_table, plan):
    spans, tok, heads, hd = queries.shape
    kvh = key_states.shape[2]
    depth, cols = out_weight.shape
    n, tps, cores = lax.axis_size("seq"), lax.axis_size("tp"), lax.axis_size("span")
    sub, owned, wide = cols // parts, n // tps, noise_table.shape[1]
    keep, late, ahead = parts // 2, parts // 3, parts - parts // 3
    extra = (n - 1) * parts - keep
    q = jnp.transpose(queries, (0, 2, 1, 3))
    kv = jnp.stack([key_states, value_states], axis=0).transpose(1, 3, 0, 2, 4)
    vmem = pl.BlockSpec(memory_space=pltpu.VMEM)
    dma = pltpu.SemaphoreType.DMA
    tile = (owned, parts, spans * tok, sub)
    out = pl.pallas_call(
        functools.partial(fused_kernel, parts, keep, late, ahead),
        out_shape=jax.ShapeDtypeStruct((spans * tok, wide), jnp.bfloat16),
        in_specs=[
            pl.BlockSpec(memory_space=pltpu.SMEM), vmem, vmem, vmem,
            pl.BlockSpec(memory_space=pl.ANY),
        ],
        out_specs=vmem,
        scratch_shapes=[
            pltpu.VMEM((spans * cores, kvh, 2, n, tok, hd), jnp.bfloat16),
            pltpu.VMEM((n, parts, depth, sub), jnp.bfloat16),
            pltpu.VMEM((2 * spans * tok, depth), jnp.bfloat16),
            pltpu.VMEM(tile, jnp.float32),
            pltpu.VMEM(tile, jnp.bfloat16),
            pltpu.VMEM(tile, jnp.bfloat16),
            pltpu.VMEM((extra, spans * tok, sub), jnp.bfloat16),
            pltpu.VMEM((extra, spans * tok, sub), jnp.bfloat16),
            dma((2, n, kvh)), dma((n, kvh)), dma((n, kvh)), dma((n, kvh)), dma((parts + 1,)),
            dma((2, n, parts)), dma((n, parts)), dma((parts,)), dma((parts,)),
            dma((2, n, parts)), dma((2, n, parts)), dma((n, parts)), dma((n, parts)),
            dma((owned, parts)), dma((owned, parts)), dma((spans,)), dma((spans,)),
            dma((extra,)), dma((extra,)),
        ],
        compiler_params=pltpu.CompilerParams(
            collective_id=0, has_side_effects=True, vmem_limit_bytes=60 * 1024 * 1024
        ),
        name="relay_attention",
    )(plan, q, kv, noise_table, out_weight)
    return out.reshape(spans, tok, wide)


def fold_block(carried, query_rows, key_rows, value_rows, factor):
    maxima, totals, weighted = carried
    scores = (
        jnp.einsum("tkgd,skd->tkgs", query_rows, key_rows, preferred_element_type=jnp.float32)
        * factor
    )
    highest = jnp.maximum(maxima, jnp.max(scores, axis=-1))
    shrink = jnp.exp(maxima - highest)
    weights = jnp.exp(scores - highest[..., None])
    totals = totals * shrink + jnp.sum(weights, axis=-1)
    weighted = weighted * shrink[..., None] + jnp.einsum(
        "tkgs,skd->tkgd",
        weights.astype(jnp.bfloat16),
        value_rows,
        preferred_element_type=jnp.float32,
    )
    return (maxima * 0.0 + highest, totals, weighted)


def per_device(queries, key_states, value_states, out_weight, noise_table, plan):
    ch_dev, tok_dev, heads_local, head_size = queries.shape
    kv_local = key_states.shape[2]
    per_kv = heads_local // kv_local
    span_count = ch_dev * lax.axis_size("span")
    first_span = lax.axis_index("span") * ch_dev
    factor = head_size ** (-0.5)
    grouped = queries.reshape(ch_dev, tok_dev, kv_local, per_kv, head_size)
    start_max = jnp.full((ch_dev, tok_dev, kv_local, per_kv), -1e30, jnp.float32)
    start_tot = jnp.zeros((ch_dev, tok_dev, kv_local, per_kv), jnp.float32)
    start_acc = jnp.zeros((ch_dev, tok_dev, kv_local, per_kv, head_size), jnp.float32)
    span_rows = (
        lax.all_gather(key_states, "seq", axis=1, tiled=True),
        lax.all_gather(value_states, "seq", axis=1, tiled=True),
    )
    key_piece = lax.all_gather(span_rows[0], "span", axis=0, tiled=True)
    value_piece = lax.all_gather(span_rows[1], "span", axis=0, tiled=True)
    new_max = []
    new_tot = []
    new_acc = []
    for q_span in range(ch_dev):
        inner_state = (start_max[q_span], start_tot[q_span], start_acc[q_span])
        for k_span in range(span_count):

            def update(inner, q_span=q_span, k_span=k_span):
                return fold_block(
                    inner, grouped[q_span], key_piece[k_span], value_piece[k_span], factor
                )

            inner_state = lax.cond(
                k_span <= first_span + q_span, update, lambda inner: inner, inner_state
            )
        new_max.append(inner_state[0])
        new_tot.append(inner_state[1])
        new_acc.append(inner_state[2])
    attn = (
        (jnp.stack(new_acc) / jnp.stack(new_tot)[..., None])
        .reshape(ch_dev, tok_dev, heads_local * head_size)
        .astype(jnp.bfloat16)
    )
    columns = jnp.einsum(
        "ctf,fo->cto",
        lax.all_gather(attn, "seq", axis=1, tiled=True),
        out_weight,
        preferred_element_type=jnp.float32,
    )
    partial_out = lax.all_to_all(
        columns.astype(jnp.bfloat16), "seq", split_axis=1, concat_axis=2, tiled=True
    ).astype(columns.dtype)
    summed = lax.psum_scatter(
        partial_out.astype(jnp.bfloat16), "tp", scatter_dimension=2, tiled=True
    ).astype(jnp.float32)
    levels = lax.dynamic_slice_in_dim(plan, first_span, ch_dev)
    picks = (levels[:, None] == jnp.arange(noise_table.shape[0], dtype=jnp.int32)[None, :]).astype(
        jnp.float32
    )
    gates = jnp.dot(picks, noise_table, precision=lax.Precision.HIGHEST)
    return (summed * gates[:, None, :]).astype(jnp.bfloat16)


def choose_parts(cols):
    for parts in (6, 3, 2, 1):
        if cols % (parts * 128) == 0:
            return parts
    return 0


def dispatch(queries, key_states, value_states, out_weight, noise_table, plan):
    depth, cols = out_weight.shape
    copies = lax.axis_size("rep") * lax.axis_size("span")
    parts = choose_parts(cols)
    pairs = all(lax.axis_size(name) == 2 for name in ("rep", "span", "tp"))
    args = (queries, key_states, value_states, out_weight, noise_table, plan)
    line = lax.axis_size("seq") == 2 * lax.axis_size("tp")
    if pairs and parts and depth % (copies * 16) == 0 and line:
        return fused(parts, *args)
    return per_device(*args)


def solution(mesh):
    placed = (
        P(("rep", "span"), "seq", "tp", None),
        P(("rep", "span"), "seq", "tp", None),
        P(("rep", "span"), "seq", "tp", None),
        P("tp", "seq"),
        P(None, "tp"),
        P("rep"),
    )
    return jax.shard_map(
        dispatch,
        mesh=mesh,
        in_specs=placed,
        out_specs=P(("rep", "span"), "seq", "tp"),
        check_vma=False,
    )
```

```python
import functools
import math

import jax
import jax.numpy as jnp
from jax import lax
from jax.experimental import pallas as pl
from jax.experimental.pallas import tpu as pltpu
from jax.sharding import PartitionSpec as P

MESH = pl.DeviceIdType.MESH


def fused_kernel(
    parts, keep, late, ahead, plan_ref, q_ref, kv_ref, noise_ref, w_ref, out_ref,
    kvbuf, wbuf, abuf, pbuf, xsend, xbuf, csend, cbuf,
    kv_send, kv_recv, kvc_send, kvc_recv, loc, wz_send, wz_recv, wf_send, wf_recv,
    wc_send, wc_recv, wy_send, wy_recv, x_send, x_recv, a_send, a_recv, c_send, c_recv,
):
    y, c = lax.axis_index("rep"), lax.axis_index("span")
    z, t = lax.axis_index("seq"), lax.axis_index("tp")
    n = lax.axis_size("seq")
    cores, tps = lax.axis_size("span"), lax.axis_size("tp")
    spans, heads, tok, hd = q_ref.shape
    kvh = kv_ref.shape[0]
    per_kv = heads // kvh
    depth, cols = w_ref.shape
    quarter = depth // (cores * lax.axis_size("rep"))
    sub = cols // parts
    owned = n // tps
    rows_own = spans * tok
    first = c * spans
    last = n - 1
    scale = hd ** (-0.5) * math.log2(math.e)
    both = jnp.logical_and

    is_end = jnp.logical_or(z == 0, z == last)
    is_host = jnp.logical_not(is_end)
    inward = jnp.where(2 * z < n, 1, -1)
    way_in = (1 + inward) // 2
    way_out = 1 - way_in
    guest = z - inward
    length = jnp.where(is_end, last, last - 1) * parts

    def source(e):
        return z + inward * (e // parts + 1), e % parts

    def place(r, s, j):
        return (jnp.abs(s - r) - 1) * parts + j - keep

    def wanted(r, s, j):
        far = place(r, s, j) >= 0
        return jnp.logical_not(both(jnp.logical_or(r == 0, r == last), far))

    def whole(s, j):
        return both(is_host, both(s == guest, j >= late))

    def rows(yy, cc):
        return pl.ds(pl.multiple_of((yy * cores + cc) * quarter, quarter), quarter)

    def columns(j):
        return pl.ds(pl.multiple_of(j * sub, sub), sub)

    def remote(src, dst, send, recv, where):
        return pltpu.make_async_remote_copy(
            src_ref=src, dst_ref=dst, send_sem=send, recv_sem=recv,
            device_id=where, device_id_type=MESH,
        )

    def z_copy(s, j, way, own):
        dst = wbuf.at[s, j, rows(y, c)]
        src = w_ref.at[rows(y, c), columns(j)] if own else dst
        to = z + 2 * way - 1
        return remote(src, dst, wz_send.at[way, s, j], wz_recv.at[s, j], {"seq": to})

    def rest_copy(s, j):
        src = w_ref.at[rows(1 - y, c), columns(j)]
        return remote(
            src, wbuf.at[s, j, rows(1 - y, c)], wf_send.at[j], wf_recv.at[j], {"seq": z + inward}
        )

    def core_copy(s, j, kind):
        part = wbuf.at[s, j, rows(y if kind == 0 else 1 - y, c)]
        return remote(part, part, wc_send.at[kind, s, j], wc_recv.at[kind, s, j], {"span": 1 - c})

    def y_copy(s, j):
        part = wbuf.at[s, j, rows(y, c)]
        return remote(part, part, wy_send.at[s, j], wy_recv.at[s, j], {"rep": 1 - y})

    def x_copy(s, j, src):
        at = lax.rem(s, owned)
        return remote(
            src, xbuf.at[at, j], x_send.at[at, j], x_recv.at[at, j], {"tp": 1 - t}
        )

    def a_copy(i):
        src = abuf.at[pl.ds(pl.multiple_of(i * tok, tok), tok)]
        dst = abuf.at[pl.ds(pl.multiple_of(rows_own + i * tok, tok), tok)]
        return remote(src, dst, a_send.at[i], a_recv.at[i], {"seq": z + inward})

    def c_copy(f):
        return remote(
            csend.at[f], cbuf.at[f], c_send.at[f], c_recv.at[f], {"seq": z - inward}
        )

    def kv_copy(s, g, way, own):
        dst = kvbuf.at[s, g, :, pl.ds(first, spans)]
        src = kv_ref.at[g] if own else dst
        to = z + 2 * way - 1
        return remote(src, dst, kv_send.at[way, s, g], kv_recv.at[s, g], {"seq": to})

    def kv_core(s, g):
        part = kvbuf.at[s, g, :, pl.ds(0, spans)]
        return remote(part, part, kvc_send.at[s, g], kvc_recv.at[s, g], {"span": 1 - c})

    def local_w(j):
        return pltpu.make_async_copy(w_ref.at[:, columns(j)], wbuf.at[z, j], loc.at[j])

    def local_kv():
        return pltpu.make_async_copy(
            kv_ref, kvbuf.at[z, :, :, pl.ds(first, spans)], loc.at[parts]
        )

    reach = ((0, z > 0), (1, z < last))

    barrier = pltpu.get_barrier_semaphore()
    for way, ok in reach:
        @pl.when(ok)
        def _(way=way):
            to = z - 1 if way == 0 else z + 1
            pl.semaphore_signal(barrier, inc=1, device_id={"seq": to}, device_id_type=MESH)
    pl.semaphore_signal(barrier, inc=1, device_id={"rep": 1 - y}, device_id_type=MESH)
    pl.semaphore_signal(barrier, inc=1, device_id={"span": 1 - c}, device_id_type=MESH)
    pl.semaphore_signal(barrier, inc=1, device_id={"tp": 1 - t}, device_id_type=MESH)
    pl.semaphore_wait(barrier, jnp.where(is_end, 4, 5))

    for g in range(kvh):
        for way, ok in reach:
            @pl.when(ok)
            def _(g=g, way=way):
                kv_copy(z, g, way, True).start()
    local_kv().start()

    def own_weights(way, low, high):
        for j in range(low, high):
            z_copy(z, j, way, True).start()

    for j in range(parts):
        local_w(j).start()

    @pl.when(is_end)
    def _():
        own_weights(way_in, 0, ahead)

    local_kv().wait()

    @pl.when(c == 0)
    def _():
        for g in range(kvh):
            kv_core(z, g).start()

    def receive(s, g, way):
        kv_copy(s, g, way, False).wait_recv()
        to = z + 2 * way - 1

        @pl.when(both(to >= 0, to < n))
        def _():
            kv_copy(s, g, way, False).start()

        @pl.when(c == 0)
        def _():
            kv_core(s, g).start()

    def arrive(s, j, sign):
        way = (1 - sign) // 2
        onward = z - sign

        @pl.when(wanted(z, s, j))
        def _():
            z_copy(s, j, way, False).wait_recv()

            @pl.when(both(both(onward >= 0, onward < n), wanted(onward, s, j)))
            def _():
                z_copy(s, j, way, False).start()

            @pl.when(jnp.logical_not(whole(s, j)))
            def _():
                y_copy(s, j).start()

            core_copy(s, j, 0).start()

    def pass_on(s, j):
        @pl.when(wanted(z, s, j))
        def _():
            y_copy(s, j).wait_recv()
            core_copy(s, j, 1).start()

    def project(s, j):
        part = jnp.dot(
            abuf[pl.ds(0, rows_own)], wbuf[s, j], preferred_element_type=jnp.float32
        )
        at = lax.rem(s, owned)

        @pl.when(s // owned == t)
        def _():
            pbuf[at, j] = part

        @pl.when(s // owned != t)
        def _():
            xsend[at, j] = part.astype(jnp.bfloat16)
            x_copy(s, j, xsend.at[at, j]).start()

    def project_guest(s, j):
        part = jnp.dot(
            abuf[pl.ds(rows_own, rows_own)], wbuf[s, j], preferred_element_type=jnp.float32
        )
        f = place(guest, s, j)
        csend[f] = part.astype(jnp.bfloat16)
        c_copy(f).start()

    def gathered(s, j):
        core_copy(s, j, 0).wait_recv()
        core_copy(s, j, 1).wait_recv()
        project(s, j)

    def gather_project(s, j):
        @pl.when(wanted(z, s, j))
        def _():
            gathered(s, j)

        @pl.when(jnp.logical_not(wanted(z, s, j)))
        def _():
            f = place(z, s, j)
            c_copy(f).wait_recv()

            @pl.when(s // owned != t)
            def _():
                x_copy(s, j, cbuf.at[f]).start()

    mine = t * owned
    near = z // owned == t
    front = jnp.where(near, z, jnp.where(inward > 0, mine, mine + owned - 1))
    rear = 2 * mine + owned - 1 - front

    def finish(q):
        s, j = jnp.where(q < parts, front, rear), lax.rem(q, parts)
        at = lax.rem(s, owned)
        x_copy(s, j, xsend.at[at, j]).wait_recv()
        where = pl.ds(pl.multiple_of(at * cols + j * sub, 128), sub)

        def put(own):
            for i in range(spans):
                level = plan_ref[first + i]
                gate = noise_ref[pl.ds(level, 1), where]
                span = pl.ds(i * tok, tok)
                total = own(span) + xbuf[at, j, span, :].astype(jnp.float32)
                out_ref[span, where] = (total * gate).astype(out_ref.dtype)

        @pl.when(wanted(z, s, j))
        def _():
            put(lambda span: pbuf[at, j, span, :])

        @pl.when(jnp.logical_not(wanted(z, s, j)))
        def _():
            put(lambda span: cbuf[place(z, s, j), span, :].astype(jnp.float32))

    lag = 2
    lead = per_kv * tok
    units = spans * kvh
    pace = max(parts // 6, 1)

    def inner(e):
        s, j = source(e)

        @pl.when(both(e >= 0, e < length))
        def _():
            arrive(s, j, inward)

    def outer(e):
        @pl.when(both(e >= 0, e < ahead))
        def _():
            arrive(guest, e, -inward)

    @pl.when(is_end)
    def _():
        for d in range(1, n):
            for g in range(kvh):
                receive(z + inward * d, g, way_out)

    @pl.when(is_host)
    def _():
        for g in range(kvh):
            receive(guest, g, way_in)
            receive(z + inward, g, way_out)
        own_weights(way_in, 0, parts)
        for g in range(kvh):
            receive(z + 2 * inward, g, way_out)
        own_weights(way_out, 0, keep)
        for k in range(pace):
            outer(k)

    @pl.when(c != 0)
    def _():
        for s in range(n):
            for g in range(kvh):
                kv_core(s, g).wait_recv()

    def attend(u, carry):
        i, g = u // kvh, u % kvh
        query = q_ref[i, pl.ds(g * per_kv, per_kv)].reshape(lead, hd)

        def fold(k, state):
            top, total, mixed = state
            keys = kvbuf[:, g, 0, k].reshape(n * tok, hd)
            values = kvbuf[:, g, 1, k].reshape(n * tok, hd)
            scores = lax.dot_general(
                query, keys, (((1,), (1,)), ((), ())), preferred_element_type=jnp.float32
            )
            high = jnp.maximum(top, jnp.max(scores, axis=1, keepdims=True))
            shrink = jnp.exp2((top - high) * scale)
            weights = jnp.exp2((scores - high) * scale)
            total = total * shrink + jnp.sum(weights, axis=1, keepdims=True)
            mixed = mixed * shrink + jnp.dot(
                weights.astype(jnp.bfloat16), values, preferred_element_type=jnp.float32
            )
            return high, total, mixed

        start = (
            jnp.full((lead, 1), -1e30, jnp.float32),
            jnp.zeros((lead, 1), jnp.float32),
            jnp.zeros((lead, hd), jnp.float32),
        )
        _, total, mixed = lax.fori_loop(0, first + i + 1, fold, start)
        result = (mixed / total).astype(jnp.bfloat16).reshape(per_kv, tok, hd)
        for h in range(per_kv):
            abuf[
                pl.ds(pl.multiple_of(i * tok, tok), tok),
                pl.ds(pl.multiple_of((g * per_kv + h) * hd, hd), hd),
            ] = result[h]

        @pl.when(both(is_end, g == kvh - 1))
        def _():
            a_copy(i).start()

        @pl.when(is_host)
        def _():
            for k in range(pace):
                outer((u + 1) * pace + k)
                inner(u * pace + k)

        @pl.when(both(is_end, c != 0))
        def _():
            for k in range(pace):
                inner((u - 1) * pace + k)

        return carry

    lax.fori_loop(0, units, attend, 0)

    @pl.when(is_end)
    def _():
        done = jnp.where(c == 0, 0, min((units - 1) * pace, keep))
        lax.fori_loop(done, keep, lambda e, carry: (inner(e), carry)[1], 0)

    def own(j, carry):
        local_w(j).wait()
        project(z, j)
        return carry

    lax.fori_loop(0, parts, own, 0)

    turn = jnp.where(c == 0, 3 * pace, 6 * pace)
    shift, due, sums, go = 4 * pace, 9 * pace, 2 * parts, 3 * pace

    def run(e, carry):
        @pl.when(both(is_end, e == go))
        def _():
            own_weights(way_in, ahead, parts)
            for j in range(late, parts):
                rest_copy(z, j).start()

        @pl.when(is_host)
        def _():
            @pl.when(e >= units * pace)
            def _():
                inner(e)

            k = e - shift

            @pl.when(both(k >= ahead, k < parts))
            def _():
                arrive(guest, k, -inward)

        f = e - lag

        @pl.when(both(f >= 0, f < length))
        def _():
            pass_on(*source(f))

        @pl.when(both(is_host, both(f >= 0, f < late)))
        def _():
            pass_on(guest, f)

        @pl.when(both(is_host, e == turn))
        def _():
            for i in range(spans):
                a_copy(i).wait_recv()

            def catch_up(f, carry):
                project_guest(*source(f - parts))
                return carry

            lax.fori_loop(keep, turn - lag - 1 + parts, catch_up, 0)

        f = e - lag - 1

        @pl.when(both(f >= 0, f < length))
        def _():
            gather_project(*source(f))

            @pl.when(both(is_host, e >= turn))
            def _():
                project_guest(*source(f))

        k = e - due + late

        @pl.when(both(is_host, both(k >= late, k < parts)))
        def _():
            rest_copy(guest, k).wait_recv()
            core_copy(guest, k, 1).start()

        k = jnp.where(f < late, f, k - 1)

        @pl.when(both(is_host, both(k >= 0, jnp.logical_or(f < late, both(k >= late, k < parts)))))
        def _():
            gathered(guest, k)

        q = e - sums

        @pl.when(both(q >= 0, q < owned * parts))
        def _():
            finish(q)

        return carry

    lax.fori_loop(
        lag, max(last * parts + lag + 1, due + parts - late + 1, sums + owned * parts), run, 0
    )

    for s in range(n):
        for way, ok in reach:
            @pl.when(both(ok, (z <= s) if way == 0 else (z >= s)))
            def _(s=s, way=way):
                for g in range(kvh):
                    kv_copy(s, g, way, False).wait_send()

        @pl.when(c == 0)
        def _(s=s):
            for g in range(kvh):
                kv_core(s, g).wait_send()

    @pl.when(is_end)
    def _():
        for i in range(spans):
            a_copy(i).wait_send()
        for j in range(late, parts):
            rest_copy(z, j).wait_send()

    def drain(f, carry):
        s, j = f // parts, f % parts

        @pl.when(both(both(z > 0, s >= z), wanted(z - 1, s, j)))
        def _():
            z_copy(s, j, 0, False).wait_send()

        @pl.when(both(both(z < last, s <= z), wanted(z + 1, s, j)))
        def _():
            z_copy(s, j, 1, False).wait_send()

        @pl.when(both(s != z, wanted(z, s, j)))
        def _():
            core_copy(s, j, 0).wait_send()
            core_copy(s, j, 1).wait_send()

            @pl.when(jnp.logical_not(whole(s, j)))
            def _():
                y_copy(s, j).wait_send()

        @pl.when(s // owned != t)
        def _():
            x_copy(s, j, xsend.at[lax.rem(s, owned), j]).wait_send()

        @pl.when(both(is_host, jnp.logical_not(wanted(guest, s, j))))
        def _():
            c_copy(place(guest, s, j)).wait_send()

        return carry

    lax.fori_loop(0, n * parts, drain, 0)


def fused(parts, queries, key_states, value_states, out_weight, noise_table, plan):
    spans, tok, heads, hd = queries.shape
    kvh = key_states.shape[2]
    depth, cols = out_weight.shape
    n, tps, cores = lax.axis_size("seq"), lax.axis_size("tp"), lax.axis_size("span")
    sub, owned, wide = cols // parts, n // tps, noise_table.shape[1]
    keep, late, ahead = 4 * parts // 6, parts // 6, 4 * parts // 6
    extra = (n - 1) * parts - keep
    q = jnp.transpose(queries, (0, 2, 1, 3))
    kv = jnp.stack([key_states, value_states], axis=0).transpose(3, 0, 1, 2, 4)
    vmem = pl.BlockSpec(memory_space=pltpu.VMEM)
    dma = pltpu.SemaphoreType.DMA
    tile = (owned, parts, spans * tok, sub)
    out = pl.pallas_call(
        functools.partial(fused_kernel, parts, keep, late, ahead),
        out_shape=jax.ShapeDtypeStruct((spans * tok, wide), jnp.bfloat16),
        in_specs=[
            pl.BlockSpec(memory_space=pltpu.SMEM), vmem, vmem, vmem,
            pl.BlockSpec(memory_space=pl.ANY),
        ],
        out_specs=vmem,
        scratch_shapes=[
            pltpu.VMEM((n, kvh, 2, spans * cores, tok, hd), jnp.bfloat16),
            pltpu.VMEM((n, parts, depth, sub), jnp.bfloat16),
            pltpu.VMEM((2 * spans * tok, depth), jnp.bfloat16),
            pltpu.VMEM(tile, jnp.float32),
            pltpu.VMEM(tile, jnp.bfloat16),
            pltpu.VMEM(tile, jnp.bfloat16),
            pltpu.VMEM((extra, spans * tok, sub), jnp.bfloat16),
            pltpu.VMEM((extra, spans * tok, sub), jnp.bfloat16),
            dma((2, n, kvh)), dma((n, kvh)), dma((n, kvh)), dma((n, kvh)), dma((parts + 1,)),
            dma((2, n, parts)), dma((n, parts)), dma((parts,)), dma((parts,)),
            dma((2, n, parts)), dma((2, n, parts)), dma((n, parts)), dma((n, parts)),
            dma((owned, parts)), dma((owned, parts)), dma((spans,)), dma((spans,)),
            dma((extra,)), dma((extra,)),
        ],
        compiler_params=pltpu.CompilerParams(
            collective_id=0, has_side_effects=True, vmem_limit_bytes=60 * 1024 * 1024
        ),
        name="relay_attention",
    )(plan, q, kv, noise_table, out_weight)
    return out.reshape(spans, tok, wide)


def fold_block(carried, query_rows, key_rows, value_rows, factor):
    maxima, totals, weighted = carried
    scores = (
        jnp.einsum("tkgd,skd->tkgs", query_rows, key_rows, preferred_element_type=jnp.float32)
        * factor
    )
    highest = jnp.maximum(maxima, jnp.max(scores, axis=-1))
    shrink = jnp.exp(maxima - highest)
    weights = jnp.exp(scores - highest[..., None])
    totals = totals * shrink + jnp.sum(weights, axis=-1)
    weighted = weighted * shrink[..., None] + jnp.einsum(
        "tkgs,skd->tkgd",
        weights.astype(jnp.bfloat16),
        value_rows,
        preferred_element_type=jnp.float32,
    )
    return (maxima * 0.0 + highest, totals, weighted)


def per_device(queries, key_states, value_states, out_weight, noise_table, plan):
    ch_dev, tok_dev, heads_local, head_size = queries.shape
    kv_local = key_states.shape[2]
    per_kv = heads_local // kv_local
    span_count = ch_dev * lax.axis_size("span")
    first_span = lax.axis_index("span") * ch_dev
    factor = head_size ** (-0.5)
    grouped = queries.reshape(ch_dev, tok_dev, kv_local, per_kv, head_size)
    start_max = jnp.full((ch_dev, tok_dev, kv_local, per_kv), -1e30, jnp.float32)
    start_tot = jnp.zeros((ch_dev, tok_dev, kv_local, per_kv), jnp.float32)
    start_acc = jnp.zeros((ch_dev, tok_dev, kv_local, per_kv, head_size), jnp.float32)
    span_rows = (
        lax.all_gather(key_states, "seq", axis=1, tiled=True),
        lax.all_gather(value_states, "seq", axis=1, tiled=True),
    )
    key_piece = lax.all_gather(span_rows[0], "span", axis=0, tiled=True)
    value_piece = lax.all_gather(span_rows[1], "span", axis=0, tiled=True)
    new_max = []
    new_tot = []
    new_acc = []
    for q_span in range(ch_dev):
        inner_state = (start_max[q_span], start_tot[q_span], start_acc[q_span])
        for k_span in range(span_count):

            def update(inner, q_span=q_span, k_span=k_span):
                return fold_block(
                    inner, grouped[q_span], key_piece[k_span], value_piece[k_span], factor
                )

            inner_state = lax.cond(
                k_span <= first_span + q_span, update, lambda inner: inner, inner_state
            )
        new_max.append(inner_state[0])
        new_tot.append(inner_state[1])
        new_acc.append(inner_state[2])
    attn = (
        (jnp.stack(new_acc) / jnp.stack(new_tot)[..., None])
        .reshape(ch_dev, tok_dev, heads_local * head_size)
        .astype(jnp.bfloat16)
    )
    columns = jnp.einsum(
        "ctf,fo->cto",
        lax.all_gather(attn, "seq", axis=1, tiled=True),
        out_weight,
        preferred_element_type=jnp.float32,
    )
    partial_out = lax.all_to_all(
        columns.astype(jnp.bfloat16), "seq", split_axis=1, concat_axis=2, tiled=True
    ).astype(columns.dtype)
    summed = lax.psum_scatter(
        partial_out.astype(jnp.bfloat16), "tp", scatter_dimension=2, tiled=True
    ).astype(jnp.float32)
    levels = lax.dynamic_slice_in_dim(plan, first_span, ch_dev)
    picks = (levels[:, None] == jnp.arange(noise_table.shape[0], dtype=jnp.int32)[None, :]).astype(
        jnp.float32
    )
    gates = jnp.dot(picks, noise_table, precision=lax.Precision.HIGHEST)
    return (summed * gates[:, None, :]).astype(jnp.bfloat16)


def choose_parts(cols):
    for parts in (6, 3, 2, 1):
        if cols % (parts * 128) == 0:
            return parts
    return 0


def dispatch(queries, key_states, value_states, out_weight, noise_table, plan):
    depth, cols = out_weight.shape
    copies = lax.axis_size("rep") * lax.axis_size("span")
    parts = choose_parts(cols)
    pairs = all(lax.axis_size(name) == 2 for name in ("rep", "span", "tp"))
    args = (queries, key_states, value_states, out_weight, noise_table, plan)
    line = lax.axis_size("seq") == 2 * lax.axis_size("tp")
    if pairs and parts and depth % (copies * 16) == 0 and line:
        return fused(parts, *args)
    return per_device(*args)


def solution(mesh):
    placed = (
        P(("rep", "span"), "seq", "tp", None),
        P(("rep", "span"), "seq", "tp", None),
        P(("rep", "span"), "seq", "tp", None),
        P("tp", "seq"),
        P(None, "tp"),
        P("rep"),
    )
    return jax.shard_map(
        dispatch,
        mesh=mesh,
        in_specs=placed,
        out_specs=P(("rep", "span"), "seq", "tp"),
        check_vma=False,
    )
```

```python
import functools
import math

import jax
import jax.numpy as jnp
from jax import lax
from jax.experimental import pallas as pl
from jax.experimental.pallas import tpu as pltpu
from jax.sharding import PartitionSpec as P

MESH = pl.DeviceIdType.MESH


def fused_kernel(
    parts, keep, late, ahead, plan_ref, q_hbm, kv_ref, noise_hbm, w_ref, out_hbm,
    kvbuf, wbuf, abuf, pbuf, xsend, xbuf, csend, cbuf,
    kv_send, kv_recv, kvc_send, kvc_recv, loc, wz_send, wz_recv, wf_send, wf_recv,
    wc_send, wc_recv, wy_send, wy_recv, x_send, x_recv, a_send, a_recv, c_send, c_recv, gates,
    q_ref, noise_ref, out_ref, out_sem,
):
    y, c = lax.axis_index("rep"), lax.axis_index("span")
    z, t = lax.axis_index("seq"), lax.axis_index("tp")
    n = lax.axis_size("seq")
    cores, tps = lax.axis_size("span"), lax.axis_size("tp")
    spans, heads, tok, hd = q_hbm.shape
    kvh = kv_ref.shape[0]
    per_kv = heads // kvh
    depth, cols = w_ref.shape
    quarter = depth // (cores * lax.axis_size("rep"))
    sub = cols // parts
    owned = n // tps
    rows_own = spans * tok
    first = c * spans
    last = n - 1
    scale = hd ** (-0.5) * math.log2(math.e)
    both = jnp.logical_and

    is_end = jnp.logical_or(z == 0, z == last)
    is_host = jnp.logical_not(is_end)
    inward = jnp.where(2 * z < n, 1, -1)
    way_in = (1 + inward) // 2
    way_out = 1 - way_in
    guest = z - inward
    length = jnp.where(is_end, last, last - 1) * parts

    def source(e):
        return z + inward * (e // parts + 1), e % parts

    def place(r, s, j):
        return (jnp.abs(s - r) - 1) * parts + j - keep

    def wanted(r, s, j):
        far = place(r, s, j) >= 0
        return jnp.logical_not(both(jnp.logical_or(r == 0, r == last), far))

    def whole(s, j):
        return both(is_host, both(s == guest, j >= late))

    def rows(yy, cc):
        return pl.ds(pl.multiple_of((yy * cores + cc) * quarter, quarter), quarter)

    def columns(j):
        return pl.ds(pl.multiple_of(j * sub, sub), sub)

    def remote(src, dst, send, recv, where):
        return pltpu.make_async_remote_copy(
            src_ref=src, dst_ref=dst, send_sem=send, recv_sem=recv,
            device_id=where, device_id_type=MESH,
        )

    def z_copy(s, j, way, own):
        dst = wbuf.at[s, j, rows(y, c)]
        src = w_ref.at[rows(y, c), columns(j)] if own else dst
        to = z + 2 * way - 1
        return remote(src, dst, wz_send.at[way, s, j], wz_recv.at[s, j], {"seq": to})

    def rest_copy(s, j):
        src = w_ref.at[rows(1 - y, c), columns(j)]
        return remote(
            src, wbuf.at[s, j, rows(1 - y, c)], wf_send.at[j], wf_recv.at[j], {"seq": z + inward}
        )

    def core_copy(s, j, kind):
        part = wbuf.at[s, j, rows(y if kind == 0 else 1 - y, c)]
        return remote(part, part, wc_send.at[kind, s, j], wc_recv.at[kind, s, j], {"span": 1 - c})

    def y_copy(s, j):
        part = wbuf.at[s, j, rows(y, c)]
        return remote(part, part, wy_send.at[s, j], wy_recv.at[s, j], {"rep": 1 - y})

    def x_copy(s, j, src):
        at = lax.rem(s, owned)
        return remote(
            src, xbuf.at[at, j], x_send.at[at, j], x_recv.at[at, j], {"tp": 1 - t}
        )

    def a_copy(i):
        src = abuf.at[pl.ds(pl.multiple_of(i * tok, tok), tok)]
        dst = abuf.at[pl.ds(pl.multiple_of(rows_own + i * tok, tok), tok)]
        return remote(src, dst, a_send.at[i], a_recv.at[i], {"seq": z + inward})

    def c_copy(f):
        return remote(
            csend.at[f], cbuf.at[f], c_send.at[f], c_recv.at[f], {"seq": z - inward}
        )

    def kv_copy(s, g, way, own):
        dst = kvbuf.at[s, g, :, pl.ds(first, spans)]
        src = kv_ref.at[g] if own else dst
        to = z + 2 * way - 1
        return remote(src, dst, kv_send.at[way, s, g], kv_recv.at[s, g], {"seq": to})

    def kv_core(s, g):
        part = kvbuf.at[s, g, :, pl.ds(0, spans)]
        return remote(part, part, kvc_send.at[s, g], kvc_recv.at[s, g], {"span": 1 - c})

    def local_w(j):
        return pltpu.make_async_copy(w_ref.at[:, columns(j)], wbuf.at[z, j], loc.at[j])

    def local_q():
        return pltpu.make_async_copy(q_hbm, q_ref, loc.at[parts + 1])

    def local_noise():
        return pltpu.make_async_copy(noise_hbm, noise_ref, loc.at[parts + 2])

    def put_copy(s, j):
        at = pl.ds(pl.multiple_of(lax.rem(s, owned) * cols + j * sub, 128), sub)
        return pltpu.make_async_copy(
            out_ref.at[:, at], out_hbm.at[:, at], out_sem.at[lax.rem(s, owned), j]
        )

    def local_kv():
        return pltpu.make_async_copy(
            kv_ref, kvbuf.at[z, :, :, pl.ds(first, spans)], loc.at[parts]
        )

    reach = ((0, z > 0), (1, z < last))

    barrier = pltpu.get_barrier_semaphore()
    for way, ok in reach:
        @pl.when(ok)
        def _(way=way):
            to = z - 1 if way == 0 else z + 1
            pl.semaphore_signal(barrier, inc=1, device_id={"seq": to}, device_id_type=MESH)
    pl.semaphore_signal(barrier, inc=1, device_id={"rep": 1 - y}, device_id_type=MESH)
    pl.semaphore_signal(barrier, inc=1, device_id={"span": 1 - c}, device_id_type=MESH)
    pl.semaphore_signal(barrier, inc=1, device_id={"tp": 1 - t}, device_id_type=MESH)
    pl.semaphore_wait(barrier, jnp.where(is_end, 4, 5))

    for g in range(kvh):
        for way, ok in reach:
            @pl.when(ok)
            def _(g=g, way=way):
                kv_copy(z, g, way, True).start()
    local_kv().start()

    def own_weights(way, low, high):
        for j in range(low, high):
            z_copy(z, j, way, True).start()

    local_q().start()
    local_noise().start()
    for j in range(parts):
        local_w(j).start()

    @pl.when(is_end)
    def _():
        own_weights(way_in, 0, ahead)

    local_kv().wait()

    @pl.when(c == 0)
    def _():
        for g in range(kvh):
            kv_core(z, g).start()

    def receive(s, g, way):
        kv_copy(s, g, way, False).wait_recv()
        to = z + 2 * way - 1

        @pl.when(both(to >= 0, to < n))
        def _():
            kv_copy(s, g, way, False).start()

        @pl.when(c == 0)
        def _():
            kv_core(s, g).start()

    def arrive(s, j, sign):
        way = (1 - sign) // 2
        onward = z - sign

        @pl.when(wanted(z, s, j))
        def _():
            z_copy(s, j, way, False).wait_recv()

            @pl.when(both(both(onward >= 0, onward < n), wanted(onward, s, j)))
            def _():
                z_copy(s, j, way, False).start()

            @pl.when(jnp.logical_not(whole(s, j)))
            def _():
                y_copy(s, j).start()

            core_copy(s, j, 0).start()

    def pass_on(s, j):
        @pl.when(wanted(z, s, j))
        def _():
            y_copy(s, j).wait_recv()
            core_copy(s, j, 1).start()

    def project(s, j):
        part = jnp.dot(
            abuf[pl.ds(0, rows_own)], wbuf[s, j], preferred_element_type=jnp.float32
        )
        at = lax.rem(s, owned)

        @pl.when(s // owned == t)
        def _():
            pbuf[at, j] = part

        @pl.when(s // owned != t)
        def _():
            xsend[at, j] = part.astype(jnp.bfloat16)
            x_copy(s, j, xsend.at[at, j]).start()

    def project_guest(s, j):
        part = jnp.dot(
            abuf[pl.ds(rows_own, rows_own)], wbuf[s, j], preferred_element_type=jnp.float32
        )
        f = place(guest, s, j)
        csend[f] = part.astype(jnp.bfloat16)
        c_copy(f).start()

    def gathered(s, j):
        core_copy(s, j, 0).wait_recv()
        core_copy(s, j, 1).wait_recv()
        project(s, j)

    def gather_project(s, j):
        @pl.when(wanted(z, s, j))
        def _():
            gathered(s, j)

        @pl.when(jnp.logical_not(wanted(z, s, j)))
        def _():
            f = place(z, s, j)
            c_copy(f).wait_recv()

            @pl.when(s // owned != t)
            def _():
                x_copy(s, j, cbuf.at[f]).start()

    mine = t * owned
    near = z // owned == t
    front = jnp.where(near, z, jnp.where(inward > 0, mine, mine + owned - 1))
    rear = 2 * mine + owned - 1 - front

    def finish(q):
        s, j = jnp.where(q < parts, front, rear), lax.rem(q, parts)
        at = lax.rem(s, owned)
        x_copy(s, j, xsend.at[at, j]).wait_recv()
        where = pl.ds(pl.multiple_of(at * cols + j * sub, 128), sub)

        def put(own):
            for i in range(spans):
                gate = gates[i, :, where]
                span = pl.ds(i * tok, tok)
                total = own(span) + xbuf[at, j, span, :].astype(jnp.float32)
                out_ref[span, where] = (total * gate).astype(out_ref.dtype)

        @pl.when(wanted(z, s, j))
        def _():
            put(lambda span: pbuf[at, j, span, :])

        @pl.when(jnp.logical_not(wanted(z, s, j)))
        def _():
            put(lambda span: cbuf[place(z, s, j), span, :].astype(jnp.float32))

        put_copy(s, j).start()

    lag = 3
    lead = per_kv * tok
    units = spans * kvh
    pace = max(parts // 6, 1)

    def inner(e):
        s, j = source(e)

        @pl.when(both(e >= 0, e < length))
        def _():
            arrive(s, j, inward)

    def outer(e):
        @pl.when(both(e >= 0, e < ahead))
        def _():
            arrive(guest, e, -inward)

    @pl.when(is_end)
    def _():
        for d in range(1, n):
            for g in range(kvh):
                receive(z + inward * d, g, way_out)

    @pl.when(is_host)
    def _():
        for g in range(kvh):
            receive(guest, g, way_in)
            receive(z + inward, g, way_out)
        own_weights(way_in, 0, parts)
        for g in range(kvh):
            receive(z + 2 * inward, g, way_out)
        own_weights(way_out, 0, keep)
        for k in range(pace):
            outer(k)
            inner(k)

    local_q().wait()
    local_noise().wait()
    for i in range(spans):
        gates[i] = noise_ref[pl.ds(plan_ref[first + i], 1), :]

    @pl.when(c != 0)
    def _():
        for s in range(n):
            for g in range(kvh):
                kv_core(s, g).wait_recv()

    def attend(u, carry):
        i, g = u // kvh, u % kvh
        query = q_ref[i, pl.ds(g * per_kv, per_kv)].reshape(lead, hd)

        def fold(k, state):
            top, total, mixed = state
            keys = kvbuf[:, g, 0, k].reshape(n * tok, hd)
            values = kvbuf[:, g, 1, k].reshape(n * tok, hd)
            scores = lax.dot_general(
                query, keys, (((1,), (1,)), ((), ())), preferred_element_type=jnp.float32
            )
            high = jnp.maximum(top, jnp.max(scores, axis=1, keepdims=True))
            shrink = jnp.exp2((top - high) * scale)
            weights = jnp.exp2((scores - high) * scale)
            total = total * shrink + jnp.sum(weights, axis=1, keepdims=True)
            mixed = mixed * shrink + jnp.dot(
                weights.astype(jnp.bfloat16), values, preferred_element_type=jnp.float32
            )
            return high, total, mixed

        start = (
            jnp.full((lead, 1), -1e30, jnp.float32),
            jnp.zeros((lead, 1), jnp.float32),
            jnp.zeros((lead, hd), jnp.float32),
        )
        _, total, mixed = lax.fori_loop(0, first + i + 1, fold, start)
        result = (mixed / total).astype(jnp.bfloat16).reshape(per_kv, tok, hd)
        for h in range(per_kv):
            abuf[
                pl.ds(pl.multiple_of(i * tok, tok), tok),
                pl.ds(pl.multiple_of((g * per_kv + h) * hd, hd), hd),
            ] = result[h]

        @pl.when(both(is_end, g == kvh - 1))
        def _():
            a_copy(i).start()

        @pl.when(is_host)
        def _():
            for k in range(pace):
                outer((u + 1) * pace + k)
                inner((u + 1) * pace + k)

        @pl.when(both(is_end, c != 0))
        def _():
            for k in range(pace):
                inner((u - 1) * pace + k)

        return carry

    lax.fori_loop(0, units, attend, 0)

    @pl.when(is_end)
    def _():
        done = jnp.where(c == 0, 0, min((units - 1) * pace, keep))
        lax.fori_loop(done, keep, lambda e, carry: (inner(e), carry)[1], 0)

    def own(j, carry):
        local_w(j).wait()
        project(z, j)
        return carry

    lax.fori_loop(0, parts, own, 0)

    def drain(f, carry):
        s, j = source(f - parts)
        s = jnp.where(s == z + inward * (length // parts + 1), guest, s)

        @pl.when(both(both(z > 0, s >= z), wanted(z - 1, s, j)))
        def _():
            z_copy(s, j, 0, False).wait_send()

        @pl.when(both(both(z < last, s <= z), wanted(z + 1, s, j)))
        def _():
            z_copy(s, j, 1, False).wait_send()

        @pl.when(both(s != z, wanted(z, s, j)))
        def _():
            core_copy(s, j, 0).wait_send()
            core_copy(s, j, 1).wait_send()

            @pl.when(jnp.logical_not(whole(s, j)))
            def _():
                y_copy(s, j).wait_send()

        @pl.when(s // owned != t)
        def _():
            x_copy(s, j, xsend.at[lax.rem(s, owned), j]).wait_send()

        @pl.when(both(is_host, jnp.logical_not(wanted(guest, s, j))))
        def _():
            c_copy(place(guest, s, j)).wait_send()

        return carry

    turn = jnp.where(c == 0, 4 * pace, 6 * pace)
    shift, due, sums, go = 4 * pace, 9 * pace, 2 * parts, 3 * pace

    def run(e, carry):
        @pl.when(both(is_end, e == go))
        def _():
            own_weights(way_in, ahead, parts)
            for j in range(late, parts):
                rest_copy(z, j).start()

        @pl.when(is_host)
        def _():
            @pl.when(e > units * pace)
            def _():
                inner(e)

            k = e - shift

            @pl.when(both(k >= ahead, k < parts))
            def _():
                arrive(guest, k, -inward)

        f = e - lag

        @pl.when(both(f >= 0, f < length))
        def _():
            pass_on(*source(f))

        @pl.when(both(is_host, both(f >= 0, f < late)))
        def _():
            pass_on(guest, f)

        @pl.when(both(is_host, e == turn))
        def _():
            for i in range(spans):
                a_copy(i).wait_recv()

            def catch_up(f, carry):
                project_guest(*source(f - parts))
                return carry

            lax.fori_loop(keep, turn - lag - 1 + parts, catch_up, 0)

        f = e - lag - 1

        @pl.when(both(f >= 0, f < length))
        def _():
            gather_project(*source(f))

            @pl.when(both(is_host, e >= turn))
            def _():
                project_guest(*source(f))

        k = e - due + late

        @pl.when(both(is_host, both(k >= late, k < parts)))
        def _():
            rest_copy(guest, k).wait_recv()
            core_copy(guest, k, 1).start()

        k = jnp.where(f < late, f, k - 1)

        @pl.when(both(is_host, both(k >= 0, jnp.logical_or(f < late, both(k >= late, k < parts)))))
        def _():
            gathered(guest, k)

        q = e - sums

        @pl.when(both(q >= 0, q < owned * parts))
        def _():
            finish(q)
            lax.fori_loop(q * tps, (q + 1) * tps, drain, 0)

        return carry

    lax.fori_loop(
        lag, max(last * parts + lag + 1, due + parts - late + 1, sums + owned * parts), run, 0
    )

    for s in range(n):
        for way, ok in reach:
            @pl.when(both(ok, (z <= s) if way == 0 else (z >= s)))
            def _(s=s, way=way):
                for g in range(kvh):
                    kv_copy(s, g, way, False).wait_send()

        @pl.when(c == 0)
        def _(s=s):
            for g in range(kvh):
                kv_core(s, g).wait_send()

    @pl.when(is_end)
    def _():
        for i in range(spans):
            a_copy(i).wait_send()
        for j in range(late, parts):
            rest_copy(z, j).wait_send()

    for q in range(owned * parts):
        put_copy(mine + q // parts, q % parts).wait()


def fused(parts, queries, key_states, value_states, out_weight, noise_table, plan):
    spans, tok, heads, hd = queries.shape
    kvh = key_states.shape[2]
    depth, cols = out_weight.shape
    n, tps, cores = lax.axis_size("seq"), lax.axis_size("tp"), lax.axis_size("span")
    sub, owned, wide = cols // parts, n // tps, noise_table.shape[1]
    keep, late, ahead = 4 * parts // 6, parts // 6, 4 * parts // 6
    extra = (n - 1) * parts - keep
    q = jnp.transpose(queries, (0, 2, 1, 3))
    kv = jnp.stack([key_states, value_states], axis=0).transpose(3, 0, 1, 2, 4)
    where_it_is = pl.BlockSpec(memory_space=pl.ANY)
    dma = pltpu.SemaphoreType.DMA
    tile = (owned, parts, spans * tok, sub)
    out = pl.pallas_call(
        functools.partial(fused_kernel, parts, keep, late, ahead),
        out_shape=jax.ShapeDtypeStruct((spans * tok, wide), jnp.bfloat16),
        in_specs=[
            pl.BlockSpec(memory_space=pltpu.SMEM), where_it_is, where_it_is, where_it_is, where_it_is,
        ],
        out_specs=where_it_is,
        scratch_shapes=[
            pltpu.VMEM((n, kvh, 2, spans * cores, tok, hd), jnp.bfloat16),
            pltpu.VMEM((n, parts, depth, sub), jnp.bfloat16),
            pltpu.VMEM((2 * spans * tok, depth), jnp.bfloat16),
            pltpu.VMEM(tile, jnp.float32),
            pltpu.VMEM(tile, jnp.bfloat16),
            pltpu.VMEM(tile, jnp.bfloat16),
            pltpu.VMEM((extra, spans * tok, sub), jnp.bfloat16),
            pltpu.VMEM((extra, spans * tok, sub), jnp.bfloat16),
            dma((2, n, kvh)), dma((n, kvh)), dma((n, kvh)), dma((n, kvh)), dma((parts + 3,)),
            dma((2, n, parts)), dma((n, parts)), dma((parts,)), dma((parts,)),
            dma((2, n, parts)), dma((2, n, parts)), dma((n, parts)), dma((n, parts)),
            dma((owned, parts)), dma((owned, parts)), dma((spans,)), dma((spans,)),
            dma((extra,)), dma((extra,)),
            pltpu.VMEM((spans, 1, wide), jnp.float32),
            pltpu.VMEM(q.shape, q.dtype),
            pltpu.VMEM(noise_table.shape, noise_table.dtype),
            pltpu.VMEM((spans * tok, wide), jnp.bfloat16),
            dma((owned, parts)),
        ],
        compiler_params=pltpu.CompilerParams(
            collective_id=0, has_side_effects=True, vmem_limit_bytes=60 * 1024 * 1024
        ),
        name="relay_attention",
    )(plan, q, kv, noise_table, out_weight)
    return out.reshape(spans, tok, wide)


def fold_block(carried, query_rows, key_rows, value_rows, factor):
    maxima, totals, weighted = carried
    scores = (
        jnp.einsum("tkgd,skd->tkgs", query_rows, key_rows, preferred_element_type=jnp.float32)
        * factor
    )
    highest = jnp.maximum(maxima, jnp.max(scores, axis=-1))
    shrink = jnp.exp(maxima - highest)
    weights = jnp.exp(scores - highest[..., None])
    totals = totals * shrink + jnp.sum(weights, axis=-1)
    weighted = weighted * shrink[..., None] + jnp.einsum(
        "tkgs,skd->tkgd",
        weights.astype(jnp.bfloat16),
        value_rows,
        preferred_element_type=jnp.float32,
    )
    return (maxima * 0.0 + highest, totals, weighted)


def per_device(queries, key_states, value_states, out_weight, noise_table, plan):
    ch_dev, tok_dev, heads_local, head_size = queries.shape
    kv_local = key_states.shape[2]
    per_kv = heads_local // kv_local
    span_count = ch_dev * lax.axis_size("span")
    first_span = lax.axis_index("span") * ch_dev
    factor = head_size ** (-0.5)
    grouped = queries.reshape(ch_dev, tok_dev, kv_local, per_kv, head_size)
    start_max = jnp.full((ch_dev, tok_dev, kv_local, per_kv), -1e30, jnp.float32)
    start_tot = jnp.zeros((ch_dev, tok_dev, kv_local, per_kv), jnp.float32)
    start_acc = jnp.zeros((ch_dev, tok_dev, kv_local, per_kv, head_size), jnp.float32)
    span_rows = (
        lax.all_gather(key_states, "seq", axis=1, tiled=True),
        lax.all_gather(value_states, "seq", axis=1, tiled=True),
    )
    key_piece = lax.all_gather(span_rows[0], "span", axis=0, tiled=True)
    value_piece = lax.all_gather(span_rows[1], "span", axis=0, tiled=True)
    new_max = []
    new_tot = []
    new_acc = []
    for q_span in range(ch_dev):
        inner_state = (start_max[q_span], start_tot[q_span], start_acc[q_span])
        for k_span in range(span_count):

            def update(inner, q_span=q_span, k_span=k_span):
                return fold_block(
                    inner, grouped[q_span], key_piece[k_span], value_piece[k_span], factor
                )

            inner_state = lax.cond(
                k_span <= first_span + q_span, update, lambda inner: inner, inner_state
            )
        new_max.append(inner_state[0])
        new_tot.append(inner_state[1])
        new_acc.append(inner_state[2])
    attn = (
        (jnp.stack(new_acc) / jnp.stack(new_tot)[..., None])
        .reshape(ch_dev, tok_dev, heads_local * head_size)
        .astype(jnp.bfloat16)
    )
    columns = jnp.einsum(
        "ctf,fo->cto",
        lax.all_gather(attn, "seq", axis=1, tiled=True),
        out_weight,
        preferred_element_type=jnp.float32,
    )
    partial_out = lax.all_to_all(
        columns.astype(jnp.bfloat16), "seq", split_axis=1, concat_axis=2, tiled=True
    ).astype(columns.dtype)
    summed = lax.psum_scatter(
        partial_out.astype(jnp.bfloat16), "tp", scatter_dimension=2, tiled=True
    ).astype(jnp.float32)
    levels = lax.dynamic_slice_in_dim(plan, first_span, ch_dev)
    picks = (levels[:, None] == jnp.arange(noise_table.shape[0], dtype=jnp.int32)[None, :]).astype(
        jnp.float32
    )
    gates = jnp.dot(picks, noise_table, precision=lax.Precision.HIGHEST)
    return (summed * gates[:, None, :]).astype(jnp.bfloat16)


def choose_parts(cols):
    for parts in (6, 3, 2, 1):
        if cols % (parts * 128) == 0:
            return parts
    return 0


def dispatch(queries, key_states, value_states, out_weight, noise_table, plan):
    depth, cols = out_weight.shape
    copies = lax.axis_size("rep") * lax.axis_size("span")
    parts = choose_parts(cols)
    pairs = all(lax.axis_size(name) == 2 for name in ("rep", "span", "tp"))
    args = (queries, key_states, value_states, out_weight, noise_table, plan)
    line = lax.axis_size("seq") == 2 * lax.axis_size("tp")
    if pairs and parts and depth % (copies * 16) == 0 and line:
        return fused(parts, *args)
    return per_device(*args)


def solution(mesh):
    placed = (
        P(("rep", "span"), "seq", "tp", None),
        P(("rep", "span"), "seq", "tp", None),
        P(("rep", "span"), "seq", "tp", None),
        P("tp", "seq"),
        P(None, "tp"),
        P("rep"),
    )
    return jax.shard_map(
        dispatch,
        mesh=mesh,
        in_specs=placed,
        out_specs=P(("rep", "span"), "seq", "tp"),
        check_vma=False,
    )
```

```python
import functools
import math

import jax
import jax.numpy as jnp
from jax import lax
from jax.experimental import pallas as pl
from jax.experimental.pallas import tpu as pltpu
from jax.sharding import PartitionSpec as P

MESH = pl.DeviceIdType.MESH


def fused_kernel(
    parts, keep, late, ahead, plan_ref, q_hbm, kv_ref, noise_hbm, w_ref, out_hbm,
    kvbuf, wbuf, abuf, pbuf, xsend, xbuf, csend, cbuf,
    kv_send, kv_recv, kvc_send, kvc_recv, loc, wz_send, wz_recv, wf_send, wf_recv,
    wc_send, wc_recv, wy_send, wy_recv, x_send, x_recv, a_send, a_recv, c_send, c_recv, gates,
    q_ref, noise_ref, out_ref, out_sem,
):
    y, c = lax.axis_index("rep"), lax.axis_index("span")
    z, t = lax.axis_index("seq"), lax.axis_index("tp")
    n = lax.axis_size("seq")
    cores, tps = lax.axis_size("span"), lax.axis_size("tp")
    spans, heads, tok, hd = q_hbm.shape
    kvh = kv_ref.shape[0]
    per_kv = heads // kvh
    depth, cols = w_ref.shape
    quarter = depth // (cores * lax.axis_size("rep"))
    sub = cols // parts
    owned = n // tps
    rows_own = spans * tok
    first = c * spans
    last = n - 1
    scale = hd ** (-0.5) * math.log2(math.e)
    both = jnp.logical_and

    is_end = jnp.logical_or(z == 0, z == last)
    is_host = jnp.logical_not(is_end)
    inward = jnp.where(2 * z < n, 1, -1)
    way_in = (1 + inward) // 2
    way_out = 1 - way_in
    guest = z - inward
    length = jnp.where(is_end, last, last - 1) * parts

    def source(e):
        return z + inward * (e // parts + 1), e % parts

    def place(r, s, j):
        return (jnp.abs(s - r) - 1) * parts + j - keep

    def wanted(r, s, j):
        far = place(r, s, j) >= 0
        return jnp.logical_not(both(jnp.logical_or(r == 0, r == last), far))

    def whole(s, j):
        return both(is_host, both(s == guest, j >= late))

    def rows(yy, cc):
        return pl.ds(pl.multiple_of((yy * cores + cc) * quarter, quarter), quarter)

    def columns(j):
        return pl.ds(pl.multiple_of(j * sub, sub), sub)

    def remote(src, dst, send, recv, where):
        return pltpu.make_async_remote_copy(
            src_ref=src, dst_ref=dst, send_sem=send, recv_sem=recv,
            device_id=where, device_id_type=MESH,
        )

    def turn_of(r, s, j):
        inside = (s - r) * jnp.where(2 * r < n, 1, -1) > 0
        return jnp.where(inside, (jnp.abs(s - r) - 1) * parts, (n - 2) * parts) + j

    def sent(part, sem):
        remote(part, part, sem, sem, {"span": 1 - c}).wait_send()

    def z_copy(s, j, way, own):
        dst = wbuf.at[s, j, rows(y, c)]
        src = w_ref.at[rows(y, c), columns(j)] if own else dst
        to = z + 2 * way - 1
        group = jnp.where(way == way_in, 0, 1) if own else 2
        return remote(src, dst, wz_send.at[group], wz_recv.at[turn_of(to, s, j)], {"seq": to})

    def z_arrival(s, j):
        dst = wbuf.at[s, j, rows(y, c)]
        return remote(dst, dst, wz_send.at[2], wz_recv.at[turn_of(z, s, j)], {"seq": z + inward})

    def rest_copy(s, j):
        src = w_ref.at[rows(1 - y, c), columns(j)]
        return remote(
            src, wbuf.at[s, j, rows(1 - y, c)], wf_send, wf_recv.at[j], {"seq": z + inward}
        )

    def core_copy(s, j, kind):
        part = wbuf.at[s, j, rows(y if kind == 0 else 1 - y, c)]
        return remote(part, part, wc_send, wc_recv.at[turn_of(z, s, j)], {"span": 1 - c})

    def core_arrival(s, j):
        part = wbuf.at[s, j, pl.ds(0, 2 * quarter)]
        return remote(part, part, wc_send, wc_recv.at[turn_of(z, s, j)], {"span": 1 - c})

    def y_copy(s, j):
        part = wbuf.at[s, j, rows(y, c)]
        group = jnp.where(both(is_host, s == guest), 1, 0)
        return remote(
            part, part, wy_send.at[group], wy_recv.at[turn_of(z, s, j)], {"rep": 1 - y}
        )

    def x_copy(s, j, src):
        at = lax.rem(s, owned)
        return remote(
            src, xbuf.at[at, j], x_send, x_recv.at[at, j], {"tp": 1 - t}
        )

    def a_copy(i):
        src = abuf.at[pl.ds(pl.multiple_of(i * tok, tok), tok)]
        dst = abuf.at[pl.ds(pl.multiple_of(rows_own + i * tok, tok), tok)]
        return remote(src, dst, a_send, a_recv, {"seq": z + inward})

    def c_copy(f):
        return remote(
            csend.at[f], cbuf.at[f], c_send, c_recv.at[f], {"seq": z - inward}
        )

    def kv_copy(s, g, way, own):
        dst = kvbuf.at[s, g, :, pl.ds(first, spans)]
        src = kv_ref.at[g] if own else dst
        to = z + 2 * way - 1
        group = jnp.where(way == way_in, 0, 1)
        return remote(src, dst, kv_send.at[group], kv_recv.at[s, g], {"seq": to})

    def kv_core(s, g):
        part = kvbuf.at[s, g, :, pl.ds(0, spans)]
        return remote(part, part, kvc_send, kvc_recv, {"span": 1 - c})

    def local_w(j):
        return pltpu.make_async_copy(w_ref.at[:, columns(j)], wbuf.at[z, j], loc.at[3])

    def all_w():
        return pltpu.make_async_copy(wbuf.at[z], wbuf.at[z], loc.at[3])

    def local_q():
        return pltpu.make_async_copy(q_hbm, q_ref, loc.at[1])

    def local_noise():
        return pltpu.make_async_copy(noise_hbm, noise_ref, loc.at[2])

    def put_copy(s, j):
        at = pl.ds(pl.multiple_of(lax.rem(s, owned) * cols + j * sub, 128), sub)
        return pltpu.make_async_copy(
            out_ref.at[:, at], out_hbm.at[:, at], out_sem
        )

    def local_kv():
        return pltpu.make_async_copy(
            kv_ref, kvbuf.at[z, :, :, pl.ds(first, spans)], loc.at[0]
        )

    reach = ((0, z > 0), (1, z < last))

    barrier = pltpu.get_barrier_semaphore()
    for way, ok in reach:
        @pl.when(ok)
        def _(way=way):
            to = z - 1 if way == 0 else z + 1
            pl.semaphore_signal(barrier, inc=1, device_id={"seq": to}, device_id_type=MESH)
    pl.semaphore_signal(barrier, inc=1, device_id={"rep": 1 - y}, device_id_type=MESH)
    pl.semaphore_signal(barrier, inc=1, device_id={"span": 1 - c}, device_id_type=MESH)
    pl.semaphore_signal(barrier, inc=1, device_id={"tp": 1 - t}, device_id_type=MESH)
    pl.semaphore_wait(barrier, jnp.where(is_end, 4, 5))

    for g in range(kvh):
        for way, ok in reach:
            @pl.when(ok)
            def _(g=g, way=way):
                kv_copy(z, g, way, True).start()
    local_kv().start()

    def own_weights(way, low, high):
        for j in range(low, high):
            z_copy(z, j, way, True).start()

    local_q().start()
    local_noise().start()
    for j in range(parts):
        local_w(j).start()

    @pl.when(is_end)
    def _():
        own_weights(way_in, 0, ahead)

    local_kv().wait()

    @pl.when(c == 0)
    def _():
        for g in range(kvh):
            kv_core(z, g).start()

    def receive(s, g, way):
        kv_copy(s, g, way, False).wait_recv()
        to = z + 2 * way - 1

        @pl.when(both(to >= 0, to < n))
        def _():
            kv_copy(s, g, way, False).start()

        @pl.when(c == 0)
        def _():
            kv_core(s, g).start()

    def arrive(s, j, sign):
        way = (1 - sign) // 2
        onward = z - sign

        @pl.when(wanted(z, s, j))
        def _():
            z_arrival(s, j).wait_recv()

            @pl.when(both(both(onward >= 0, onward < n), wanted(onward, s, j)))
            def _():
                z_copy(s, j, way, False).start()

            @pl.when(jnp.logical_not(whole(s, j)))
            def _():
                y_copy(s, j).start()

            core_copy(s, j, 0).start()

    def pass_on(s, j):
        @pl.when(wanted(z, s, j))
        def _():
            y_copy(s, j).wait_recv()
            core_copy(s, j, 1).start()

    def project(s, j):
        part = jnp.dot(
            abuf[pl.ds(0, rows_own)], wbuf[s, j], preferred_element_type=jnp.float32
        )
        at = lax.rem(s, owned)

        @pl.when(s // owned == t)
        def _():
            pbuf[at, j] = part

        @pl.when(s // owned != t)
        def _():
            xsend[at, j] = part.astype(jnp.bfloat16)
            x_copy(s, j, xsend.at[at, j]).start()

    def project_guest(s, j):
        part = jnp.dot(
            abuf[pl.ds(rows_own, rows_own)], wbuf[s, j], preferred_element_type=jnp.float32
        )
        f = place(guest, s, j)
        csend[f] = part.astype(jnp.bfloat16)
        c_copy(f).start()

    def gathered(s, j):
        core_arrival(s, j).wait_recv()
        project(s, j)

    def gather_project(s, j):
        @pl.when(wanted(z, s, j))
        def _():
            gathered(s, j)

        @pl.when(jnp.logical_not(wanted(z, s, j)))
        def _():
            f = place(z, s, j)
            c_copy(f).wait_recv()

            @pl.when(s // owned != t)
            def _():
                x_copy(s, j, cbuf.at[f]).start()

    mine = t * owned
    near = z // owned == t
    front = jnp.where(near, z, jnp.where(inward > 0, mine, mine + owned - 1))
    rear = 2 * mine + owned - 1 - front

    def finish(q):
        s, j = jnp.where(q < parts, front, rear), lax.rem(q, parts)
        at = lax.rem(s, owned)
        x_copy(s, j, xsend.at[at, j]).wait_recv()
        where = pl.ds(pl.multiple_of(at * cols + j * sub, 128), sub)

        def put(own):
            for i in range(spans):
                gate = gates[i, :, where]
                span = pl.ds(i * tok, tok)
                total = own(span) + xbuf[at, j, span, :].astype(jnp.float32)
                out_ref[span, where] = (total * gate).astype(out_ref.dtype)

        @pl.when(wanted(z, s, j))
        def _():
            put(lambda span: pbuf[at, j, span, :])

        @pl.when(jnp.logical_not(wanted(z, s, j)))
        def _():
            put(lambda span: cbuf[place(z, s, j), span, :].astype(jnp.float32))

        put_copy(s, j).start()

    lag = 3
    lead = per_kv * tok
    units = spans * kvh
    pace = max(parts // 6, 1)

    def inner(e):
        s, j = source(e)

        @pl.when(both(e >= 0, e < length))
        def _():
            arrive(s, j, inward)

    def outer(e):
        @pl.when(both(e >= 0, e < ahead))
        def _():
            arrive(guest, e, -inward)

    @pl.when(is_end)
    def _():
        for d in range(1, n):
            for g in range(kvh):
                receive(z + inward * d, g, way_out)

    @pl.when(is_host)
    def _():
        for g in range(kvh):
            receive(guest, g, way_in)
            receive(z + inward, g, way_out)
        own_weights(way_in, 0, parts)
        for g in range(kvh):
            receive(z + 2 * inward, g, way_out)
        own_weights(way_out, 0, keep)
        for k in range(pace):
            outer(k)
            inner(k)

    local_q().wait()
    local_noise().wait()
    for i in range(spans):
        gates[i] = noise_ref[pl.ds(plan_ref[first + i], 1), :]

    @pl.when(c != 0)
    def _():
        kv_all = kvbuf.at[:, :, :, pl.ds(0, spans)]
        remote(kv_all, kv_all, kvc_send, kvc_recv, {"span": 1 - c}).wait_recv()

    def attend(u, carry):
        i, g = u // kvh, u % kvh
        query = q_ref[i, pl.ds(g * per_kv, per_kv)].reshape(lead, hd)

        def fold(k, state):
            top, total, mixed = state
            keys = kvbuf[:, g, 0, k].reshape(n * tok, hd)
            values = kvbuf[:, g, 1, k].reshape(n * tok, hd)
            scores = lax.dot_general(
                query, keys, (((1,), (1,)), ((), ())), preferred_element_type=jnp.float32
            )
            high = jnp.maximum(top, jnp.max(scores, axis=1, keepdims=True))
            shrink = jnp.exp2((top - high) * scale)
            weights = jnp.exp2((scores - high) * scale)
            total = total * shrink + jnp.sum(weights, axis=1, keepdims=True)
            mixed = mixed * shrink + jnp.dot(
                weights.astype(jnp.bfloat16), values, preferred_element_type=jnp.float32
            )
            return high, total, mixed

        start = (
            jnp.full((lead, 1), -1e30, jnp.float32),
            jnp.zeros((lead, 1), jnp.float32),
            jnp.zeros((lead, hd), jnp.float32),
        )
        _, total, mixed = lax.fori_loop(0, first + i + 1, fold, start)
        result = (mixed / total).astype(jnp.bfloat16).reshape(per_kv, tok, hd)
        for h in range(per_kv):
            abuf[
                pl.ds(pl.multiple_of(i * tok, tok), tok),
                pl.ds(pl.multiple_of((g * per_kv + h) * hd, hd), hd),
            ] = result[h]

        @pl.when(both(is_end, g == kvh - 1))
        def _():
            a_copy(i).start()

        @pl.when(is_host)
        def _():
            for k in range(pace):
                outer((u + 1) * pace + k)
                inner((u + 1) * pace + k)

        @pl.when(both(is_end, c != 0))
        def _():
            for k in range(pace):
                inner((u - 1) * pace + k)

        return carry

    lax.fori_loop(0, units, attend, 0)

    @pl.when(is_end)
    def _():
        done = jnp.where(c == 0, 0, min((units - 1) * pace, keep))
        lax.fori_loop(done, keep, lambda e, carry: (inner(e), carry)[1], 0)

    def own(j, carry):
        project(z, j)
        return carry

    all_w().wait()
    lax.fori_loop(0, parts, own, 0)

    turn = jnp.where(c == 0, 4 * pace, 6 * pace)
    shift, due, sums, go = 4 * pace, 9 * pace, 2 * parts, 3 * pace

    def run(e, carry):
        @pl.when(both(is_end, e == go))
        def _():
            own_weights(way_in, ahead, parts)
            for j in range(late, parts):
                rest_copy(z, j).start()

        @pl.when(is_host)
        def _():
            @pl.when(e > units * pace)
            def _():
                inner(e)

            k = e - shift

            @pl.when(both(k >= ahead, k < parts))
            def _():
                arrive(guest, k, -inward)

        f = e - lag

        @pl.when(both(f >= 0, f < length))
        def _():
            pass_on(*source(f))

        @pl.when(both(is_host, both(f >= 0, f < late)))
        def _():
            pass_on(guest, f)

        @pl.when(both(is_host, e == turn))
        def _():
            rows_in = abuf.at[pl.ds(rows_own, rows_own)]
            remote(rows_in, rows_in, a_send, a_recv, {"seq": guest}).wait_recv()

            def catch_up(f, carry):
                project_guest(*source(f - parts))
                return carry

            lax.fori_loop(keep, turn - lag - 1 + parts, catch_up, 0)

        f = e - lag - 1

        @pl.when(both(f >= 0, f < length))
        def _():
            gather_project(*source(f))

            @pl.when(both(is_host, e >= turn))
            def _():
                project_guest(*source(f))

        k = e - due + late

        @pl.when(both(is_host, both(k >= late, k < parts)))
        def _():
            rest_copy(guest, k).wait_recv()
            core_copy(guest, k, 1).start()

        k = jnp.where(f < late, f, k - 1)

        @pl.when(both(is_host, both(k >= 0, jnp.logical_or(f < late, both(k >= late, k < parts)))))
        def _():
            gathered(guest, k)

        q = e - sums

        @pl.when(both(q >= 0, q < owned * parts))
        def _():
            finish(q)

        return carry

    lax.fori_loop(
        lag, max(last * parts + lag + 1, due + parts - late + 1, sums + owned * parts), run, 0
    )

    piece = pl.ds(0, quarter)
    pair = pl.ds(0, 2 * quarter)

    @pl.when(is_end)
    def _():
        sent(kv_ref, kv_send.at[0])
        sent(w_ref.at[piece], wz_send.at[0])
        sent(w_ref.at[piece, pl.ds(0, (parts - late) * sub)], wf_send)
        sent(wbuf.at[0, pl.ds(0, keep), pair], wc_send)
        sent(wbuf.at[0, pl.ds(0, keep), piece], wy_send.at[0])
        sent(abuf.at[pl.ds(0, rows_own)], a_send)

    @pl.when(is_host)
    def _():
        sent(kvbuf.at[pl.ds(0, 2), :, :, pl.ds(0, spans)], kv_send.at[0])
        sent(kvbuf.at[pl.ds(0, n - 1), :, :, pl.ds(0, spans)], kv_send.at[1])
        sent(w_ref.at[piece], wz_send.at[0])
        sent(w_ref.at[piece, pl.ds(0, keep * sub)], wz_send.at[1])
        sent(wbuf.at[0, :, piece], wz_send.at[2])
        sent(wbuf.at[pl.ds(0, n - 1), :, pair], wc_send)
        sent(wbuf.at[pl.ds(0, n - 2), :, piece], wy_send.at[0])
        sent(w_ref.at[piece, pl.ds(0, late * sub)], wy_send.at[1])
        sent(csend, c_send)

    @pl.when(c == 0)
    def _():
        sent(kvbuf.at[:, :, :, pl.ds(0, spans)], kvc_send)

    sent(xsend, x_send)
    pltpu.make_async_copy(out_ref, out_hbm, out_sem).wait()


def fused(parts, queries, key_states, value_states, out_weight, noise_table, plan):
    spans, tok, heads, hd = queries.shape
    kvh = key_states.shape[2]
    depth, cols = out_weight.shape
    n, tps, cores = lax.axis_size("seq"), lax.axis_size("tp"), lax.axis_size("span")
    sub, owned, wide = cols // parts, n // tps, noise_table.shape[1]
    keep, late, ahead = 4 * parts // 6, parts // 6, 4 * parts // 6
    extra, taken = (n - 1) * parts - keep, (n - 1) * parts
    q = jnp.transpose(queries, (0, 2, 1, 3))
    kv = jnp.stack([key_states, value_states], axis=0).transpose(3, 0, 1, 2, 4)
    where_it_is = pl.BlockSpec(memory_space=pl.ANY)
    dma = pltpu.SemaphoreType.DMA
    tile = (owned, parts, spans * tok, sub)
    out = pl.pallas_call(
        functools.partial(fused_kernel, parts, keep, late, ahead),
        out_shape=jax.ShapeDtypeStruct((spans * tok, wide), jnp.bfloat16),
        in_specs=[
            pl.BlockSpec(memory_space=pltpu.SMEM), where_it_is, where_it_is, where_it_is, where_it_is,
        ],
        out_specs=where_it_is,
        scratch_shapes=[
            pltpu.VMEM((n, kvh, 2, spans * cores, tok, hd), jnp.bfloat16),
            pltpu.VMEM((n, parts, depth, sub), jnp.bfloat16),
            pltpu.VMEM((2 * spans * tok, depth), jnp.bfloat16),
            pltpu.VMEM(tile, jnp.float32),
            pltpu.VMEM(tile, jnp.bfloat16),
            pltpu.VMEM(tile, jnp.bfloat16),
            pltpu.VMEM((extra, spans * tok, sub), jnp.bfloat16),
            pltpu.VMEM((extra, spans * tok, sub), jnp.bfloat16),
            dma((2,)), dma((n, kvh)), dma, dma, dma((4,)),
            dma((3,)), dma((taken,)), dma, dma((parts,)),
            dma, dma((taken,)), dma((2,)), dma((taken,)),
            dma, dma((owned, parts)), dma, dma, dma, dma((extra,)),
            pltpu.VMEM((spans, 1, wide), jnp.float32),
            pltpu.VMEM(q.shape, q.dtype),
            pltpu.VMEM(noise_table.shape, noise_table.dtype),
            pltpu.VMEM((spans * tok, wide), jnp.bfloat16),
            dma,
        ],
        compiler_params=pltpu.CompilerParams(
            collective_id=0, has_side_effects=True, vmem_limit_bytes=60 * 1024 * 1024
        ),
        name="relay_attention",
    )(plan, q, kv, noise_table, out_weight)
    return out.reshape(spans, tok, wide)


def fold_block(carried, query_rows, key_rows, value_rows, factor):
    maxima, totals, weighted = carried
    scores = (
        jnp.einsum("tkgd,skd->tkgs", query_rows, key_rows, preferred_element_type=jnp.float32)
        * factor
    )
    highest = jnp.maximum(maxima, jnp.max(scores, axis=-1))
    shrink = jnp.exp(maxima - highest)
    weights = jnp.exp(scores - highest[..., None])
    totals = totals * shrink + jnp.sum(weights, axis=-1)
    weighted = weighted * shrink[..., None] + jnp.einsum(
        "tkgs,skd->tkgd",
        weights.astype(jnp.bfloat16),
        value_rows,
        preferred_element_type=jnp.float32,
    )
    return (maxima * 0.0 + highest, totals, weighted)


def per_device(queries, key_states, value_states, out_weight, noise_table, plan):
    ch_dev, tok_dev, heads_local, head_size = queries.shape
    kv_local = key_states.shape[2]
    per_kv = heads_local // kv_local
    span_count = ch_dev * lax.axis_size("span")
    first_span = lax.axis_index("span") * ch_dev
    factor = head_size ** (-0.5)
    grouped = queries.reshape(ch_dev, tok_dev, kv_local, per_kv, head_size)
    start_max = jnp.full((ch_dev, tok_dev, kv_local, per_kv), -1e30, jnp.float32)
    start_tot = jnp.zeros((ch_dev, tok_dev, kv_local, per_kv), jnp.float32)
    start_acc = jnp.zeros((ch_dev, tok_dev, kv_local, per_kv, head_size), jnp.float32)
    span_rows = (
        lax.all_gather(key_states, "seq", axis=1, tiled=True),
        lax.all_gather(value_states, "seq", axis=1, tiled=True),
    )
    key_piece = lax.all_gather(span_rows[0], "span", axis=0, tiled=True)
    value_piece = lax.all_gather(span_rows[1], "span", axis=0, tiled=True)
    new_max = []
    new_tot = []
    new_acc = []
    for q_span in range(ch_dev):
        inner_state = (start_max[q_span], start_tot[q_span], start_acc[q_span])
        for k_span in range(span_count):

            def update(inner, q_span=q_span, k_span=k_span):
                return fold_block(
                    inner, grouped[q_span], key_piece[k_span], value_piece[k_span], factor
                )

            inner_state = lax.cond(
                k_span <= first_span + q_span, update, lambda inner: inner, inner_state
            )
        new_max.append(inner_state[0])
        new_tot.append(inner_state[1])
        new_acc.append(inner_state[2])
    attn = (
        (jnp.stack(new_acc) / jnp.stack(new_tot)[..., None])
        .reshape(ch_dev, tok_dev, heads_local * head_size)
        .astype(jnp.bfloat16)
    )
    columns = jnp.einsum(
        "ctf,fo->cto",
        lax.all_gather(attn, "seq", axis=1, tiled=True),
        out_weight,
        preferred_element_type=jnp.float32,
    )
    partial_out = lax.all_to_all(
        columns.astype(jnp.bfloat16), "seq", split_axis=1, concat_axis=2, tiled=True
    ).astype(columns.dtype)
    summed = lax.psum_scatter(
        partial_out.astype(jnp.bfloat16), "tp", scatter_dimension=2, tiled=True
    ).astype(jnp.float32)
    levels = lax.dynamic_slice_in_dim(plan, first_span, ch_dev)
    picks = (levels[:, None] == jnp.arange(noise_table.shape[0], dtype=jnp.int32)[None, :]).astype(
        jnp.float32
    )
    gates = jnp.dot(picks, noise_table, precision=lax.Precision.HIGHEST)
    return (summed * gates[:, None, :]).astype(jnp.bfloat16)


def choose_parts(cols):
    for parts in (6, 3, 2, 1):
        if cols % (parts * 128) == 0:
            return parts
    return 0


def dispatch(queries, key_states, value_states, out_weight, noise_table, plan):
    depth, cols = out_weight.shape
    copies = lax.axis_size("rep") * lax.axis_size("span")
    parts = choose_parts(cols)
    pairs = all(lax.axis_size(name) == 2 for name in ("rep", "span", "tp"))
    args = (queries, key_states, value_states, out_weight, noise_table, plan)
    line = lax.axis_size("seq") == 2 * lax.axis_size("tp")
    if pairs and parts and depth % (copies * 16) == 0 and line:
        return fused(parts, *args)
    return per_device(*args)


def solution(mesh):
    placed = (
        P(("rep", "span"), "seq", "tp", None),
        P(("rep", "span"), "seq", "tp", None),
        P(("rep", "span"), "seq", "tp", None),
        P("tp", "seq"),
        P(None, "tp"),
        P("rep"),
    )
    return jax.shard_map(
        dispatch,
        mesh=mesh,
        in_specs=placed,
        out_specs=P(("rep", "span"), "seq", "tp"),
        check_vma=False,
    )
```

```python
import functools
import math

import jax
import jax.numpy as jnp
from jax import lax
from jax.experimental import pallas as pl
from jax.experimental.pallas import tpu as pltpu
from jax.sharding import PartitionSpec as P

MESH = pl.DeviceIdType.MESH


def fused_kernel(
    parts, keep, late, ahead, pick, plan_ref, q_hbm, kv_ref, noise_hbm, w_ref, out_hbm,
    kvbuf, wbuf, abuf, pbuf, xsend, xbuf, csend, cbuf,
    kv_send, kv_recv, kvc_send, kvc_recv, loc, wz_send, wz_recv, wf_send, wf_recv,
    wc_send, wc_recv, wy_send, wy_recv, x_send, x_recv, a_send, a_recv, c_send, c_recv, gates,
    q_ref, noise_ref, out_ref, out_sem,
    gsend, grecv, gpart, g_send, g_recv,
):
    y, c = lax.axis_index("rep"), lax.axis_index("span")
    z, t = lax.axis_index("seq"), lax.axis_index("tp")
    n = lax.axis_size("seq")
    cores, tps = lax.axis_size("span"), lax.axis_size("tp")
    spans, heads, tok, hd = q_hbm.shape
    kvh = kv_ref.shape[0]
    per_kv = heads // kvh
    depth, cols = w_ref.shape
    quarter = depth // (cores * lax.axis_size("rep"))
    sub = cols // parts
    owned = n // tps
    rows_own = spans * tok
    first = c * spans
    last = n - 1
    scale = hd ** (-0.5) * math.log2(math.e)
    both = jnp.logical_and

    is_end = jnp.logical_or(z == 0, z == last)
    is_host = jnp.logical_not(is_end)
    inward = jnp.where(2 * z < n, 1, -1)
    way_in = (1 + inward) // 2
    way_out = 1 - way_in
    guest = z - inward
    length = jnp.where(is_end, last, last - 1) * parts

    def source(e):
        return z + inward * (e // parts + 1), e % parts

    def place(r, s, j):
        return (jnp.abs(s - r) - 1) * parts + j - keep

    def wanted(r, s, j):
        far = place(r, s, j) >= 0
        return jnp.logical_not(both(jnp.logical_or(r == 0, r == last), far))

    shared = parts - keep

    def summed(r, s, j):
        f = place(r, s, j) + keep
        k = f - parts - pick
        return jnp.logical_or(both(f >= keep, f < parts), both(k >= 0, k < shared))

    def sum_at(r, s, j):
        f = place(r, s, j) + keep
        return jnp.where(f < parts, f - keep, f - parts - pick)

    def whole(s, j):
        return both(is_host, both(s == guest, j >= late))

    def rows(yy, cc):
        return pl.ds(pl.multiple_of((yy * cores + cc) * quarter, quarter), quarter)

    def columns(j):
        return pl.ds(pl.multiple_of(j * sub, sub), sub)

    def remote(src, dst, send, recv, where):
        return pltpu.make_async_remote_copy(
            src_ref=src, dst_ref=dst, send_sem=send, recv_sem=recv,
            device_id=where, device_id_type=MESH,
        )

    def turn_of(r, s, j):
        inside = (s - r) * jnp.where(2 * r < n, 1, -1) > 0
        return jnp.where(inside, (jnp.abs(s - r) - 1) * parts, (n - 2) * parts) + j

    def sent(part, sem):
        remote(part, part, sem, sem, {"span": 1 - c}).wait_send()

    def z_copy(s, j, way, own):
        dst = wbuf.at[s, j, rows(y, c)]
        src = w_ref.at[rows(y, c), columns(j)] if own else dst
        to = z + 2 * way - 1
        group = jnp.where(way == way_in, 0, 1) if own else 2
        return remote(src, dst, wz_send.at[group], wz_recv.at[turn_of(to, s, j)], {"seq": to})

    def z_arrival(s, j):
        dst = wbuf.at[s, j, rows(y, c)]
        return remote(dst, dst, wz_send.at[2], wz_recv.at[turn_of(z, s, j)], {"seq": z + inward})

    def rest_copy(s, j):
        src = w_ref.at[rows(1 - y, c), columns(j)]
        return remote(
            src, wbuf.at[s, j, rows(1 - y, c)], wf_send, wf_recv.at[j], {"seq": z + inward}
        )

    def core_copy(s, j, kind):
        part = wbuf.at[s, j, rows(y if kind == 0 else 1 - y, c)]
        return remote(part, part, wc_send, wc_recv.at[turn_of(z, s, j)], {"span": 1 - c})

    def core_arrival(s, j):
        part = wbuf.at[s, j, pl.ds(0, 2 * quarter)]
        return remote(part, part, wc_send, wc_recv.at[turn_of(z, s, j)], {"span": 1 - c})

    def y_copy(s, j):
        part = wbuf.at[s, j, rows(y, c)]
        group = jnp.where(both(is_host, s == guest), 1, 0)
        return remote(
            part, part, wy_send.at[group], wy_recv.at[turn_of(z, s, j)], {"rep": 1 - y}
        )

    def x_copy(s, j, src):
        at = lax.rem(s, owned)
        return remote(
            src, xbuf.at[at, j], x_send, x_recv.at[at, j], {"tp": 1 - t}
        )

    def a_copy(i):
        src = abuf.at[pl.ds(pl.multiple_of(i * tok, tok), tok)]
        dst = abuf.at[pl.ds(pl.multiple_of(rows_own + i * tok, tok), tok)]
        return remote(src, dst, a_send, a_recv, {"seq": z + inward})

    def c_copy(f):
        return remote(
            csend.at[f], cbuf.at[f], c_send, c_recv.at[f], {"seq": z - inward}
        )

    def g_copy(k):
        return remote(gsend.at[k], grecv.at[k], g_send, g_recv.at[k], {"tp": 1 - t})

    def kv_copy(s, g, way, own):
        dst = kvbuf.at[s, g, :, pl.ds(first, spans)]
        src = kv_ref.at[g] if own else dst
        to = z + 2 * way - 1
        group = jnp.where(way == way_in, 0, 1)
        return remote(src, dst, kv_send.at[group], kv_recv.at[s, g], {"seq": to})

    def kv_core(s, g):
        part = kvbuf.at[s, g, :, pl.ds(0, spans)]
        return remote(part, part, kvc_send, kvc_recv, {"span": 1 - c})

    def local_w(j):
        return pltpu.make_async_copy(w_ref.at[:, columns(j)], wbuf.at[z, j], loc.at[3])

    def all_w():
        return pltpu.make_async_copy(wbuf.at[z], wbuf.at[z], loc.at[3])

    def local_q():
        return pltpu.make_async_copy(q_hbm, q_ref, loc.at[1])

    def local_noise():
        return pltpu.make_async_copy(noise_hbm, noise_ref, loc.at[2])

    def put_copy(s, j):
        at = pl.ds(pl.multiple_of(lax.rem(s, owned) * cols + j * sub, 128), sub)
        return pltpu.make_async_copy(
            out_ref.at[:, at], out_hbm.at[:, at], out_sem
        )

    def local_kv():
        return pltpu.make_async_copy(
            kv_ref, kvbuf.at[z, :, :, pl.ds(first, spans)], loc.at[0]
        )

    reach = ((0, z > 0), (1, z < last))

    barrier = pltpu.get_barrier_semaphore()
    for way, ok in reach:
        @pl.when(ok)
        def _(way=way):
            to = z - 1 if way == 0 else z + 1
            pl.semaphore_signal(barrier, inc=1, device_id={"seq": to}, device_id_type=MESH)
    pl.semaphore_signal(barrier, inc=1, device_id={"rep": 1 - y}, device_id_type=MESH)
    pl.semaphore_signal(barrier, inc=1, device_id={"span": 1 - c}, device_id_type=MESH)
    pl.semaphore_signal(barrier, inc=1, device_id={"tp": 1 - t}, device_id_type=MESH)
    pl.semaphore_wait(barrier, jnp.where(is_end, 4, 5))

    for g in range(kvh):
        for way, ok in reach:
            @pl.when(ok)
            def _(g=g, way=way):
                kv_copy(z, g, way, True).start()
    local_kv().start()

    def own_weights(way, low, high):
        for j in range(low, high):
            z_copy(z, j, way, True).start()

    local_q().start()
    local_noise().start()
    for j in range(parts):
        local_w(j).start()

    @pl.when(is_end)
    def _():
        own_weights(way_in, 0, ahead)

    local_kv().wait()

    @pl.when(c == 0)
    def _():
        for g in range(kvh):
            kv_core(z, g).start()

    def receive(s, g, way):
        kv_copy(s, g, way, False).wait_recv()
        to = z + 2 * way - 1

        @pl.when(both(to >= 0, to < n))
        def _():
            kv_copy(s, g, way, False).start()

        @pl.when(c == 0)
        def _():
            kv_core(s, g).start()

    def arrive(s, j, sign):
        way = (1 - sign) // 2
        onward = z - sign

        @pl.when(wanted(z, s, j))
        def _():
            z_arrival(s, j).wait_recv()

            @pl.when(both(both(onward >= 0, onward < n), wanted(onward, s, j)))
            def _():
                z_copy(s, j, way, False).start()

            @pl.when(jnp.logical_not(whole(s, j)))
            def _():
                y_copy(s, j).start()

            core_copy(s, j, 0).start()

    def pass_on(s, j):
        @pl.when(wanted(z, s, j))
        def _():
            y_copy(s, j).wait_recv()
            core_copy(s, j, 1).start()

    def project(s, j):
        part = jnp.dot(
            abuf[pl.ds(0, rows_own)], wbuf[s, j], preferred_element_type=jnp.float32
        )
        at = lax.rem(s, owned)

        @pl.when(s // owned == t)
        def _():
            pbuf[at, j] = part

        @pl.when(s // owned != t)
        def _():
            xsend[at, j] = part.astype(jnp.bfloat16)
            x_copy(s, j, xsend.at[at, j]).start()

    def project_guest(s, j):
        part = jnp.dot(
            abuf[pl.ds(rows_own, rows_own)], wbuf[s, j], preferred_element_type=jnp.float32
        )
        f = place(guest, s, j)
        k = sum_at(guest, s, j)
        add = summed(guest, s, j)
        mine = s // owned == t

        @pl.when(jnp.logical_not(add))
        def _():
            csend[f] = part.astype(jnp.bfloat16)
            c_copy(f).start()

        @pl.when(both(add, mine))
        def _():
            gpart[k] = part

        @pl.when(both(add, jnp.logical_not(mine)))
        def _():
            gsend[k] = part.astype(jnp.bfloat16)
            g_copy(k).start()

    def pass_sum(f):
        s, j = source(f - parts)

        @pl.when(s // owned == t)
        def _():
            f = place(guest, s, j)
            k = sum_at(guest, s, j)
            g_copy(k).wait_recv()
            csend[f] = (gpart[k] + grecv[k].astype(jnp.float32)).astype(jnp.bfloat16)
            c_copy(f).start()

    def gathered(s, j):
        core_arrival(s, j).wait_recv()
        project(s, j)

    def gather_project(s, j):
        @pl.when(wanted(z, s, j))
        def _():
            gathered(s, j)

        @pl.when(jnp.logical_not(jnp.logical_or(wanted(z, s, j), summed(z, s, j))))
        def _():
            f = place(z, s, j)
            c_copy(f).wait_recv()

            @pl.when(s // owned != t)
            def _():
                x_copy(s, j, cbuf.at[f]).start()

    mine = t * owned
    near = z // owned == t
    front = jnp.where(near, z, jnp.where(inward > 0, mine, mine + owned - 1))
    rear = 2 * mine + owned - 1 - front

    def finish(q):
        s, j = jnp.where(q < parts, front, rear), lax.rem(q, parts)
        at = lax.rem(s, owned)
        whole_sum = both(is_end, summed(z, s, j))

        @pl.when(whole_sum)
        def _():
            c_copy(place(z, s, j)).wait_recv()

        @pl.when(jnp.logical_not(whole_sum))
        def _():
            x_copy(s, j, xsend.at[at, j]).wait_recv()

        where = pl.ds(pl.multiple_of(at * cols + j * sub, 128), sub)

        def put(total):
            for i in range(spans):
                span = pl.ds(i * tok, tok)
                out_ref[span, where] = (total(span) * gates[i, :, where]).astype(out_ref.dtype)

        def other(span):
            return xbuf[at, j, span, :].astype(jnp.float32)

        def guests(span):
            return cbuf[place(z, s, j), span, :].astype(jnp.float32)

        @pl.when(wanted(z, s, j))
        def _():
            put(lambda span: pbuf[at, j, span, :] + other(span))

        @pl.when(whole_sum)
        def _():
            put(guests)

        @pl.when(jnp.logical_not(jnp.logical_or(wanted(z, s, j), whole_sum)))
        def _():
            put(lambda span: guests(span) + other(span))

        put_copy(s, j).start()

    lag, most = 2, 3
    gap = jnp.where(c == 0, 2, 3)
    lead = per_kv * tok
    units = spans * kvh
    pace = max(parts // 6, 1)

    def inner(e):
        s, j = source(e)

        @pl.when(both(e >= 0, e < length))
        def _():
            arrive(s, j, inward)

    def outer(e):
        @pl.when(both(e >= 0, e < ahead))
        def _():
            arrive(guest, e, -inward)

    @pl.when(is_end)
    def _():
        for d in range(1, n):
            for g in range(kvh):
                receive(z + inward * d, g, way_out)

    @pl.when(is_host)
    def _():
        for g in range(kvh):
            receive(guest, g, way_in)
            receive(z + inward, g, way_out)
        own_weights(way_in, 0, parts)
        for g in range(kvh):
            receive(z + 2 * inward, g, way_out)
        own_weights(way_out, 0, keep)
        for k in range(pace):
            outer(k)
            inner(k)

    local_q().wait()
    local_noise().wait()
    for i in range(spans):
        gates[i] = noise_ref[pl.ds(plan_ref[first + i], 1), :]

    @pl.when(c != 0)
    def _():
        kv_all = kvbuf.at[:, :, :, pl.ds(0, spans)]
        remote(kv_all, kv_all, kvc_send, kvc_recv, {"span": 1 - c}).wait_recv()

    def relay_in(e):
        @pl.when(both(e >= 0, e < length))
        def _():
            pass_on(*source(e))

        @pl.when(both(is_host, both(e >= 0, e < late)))
        def _():
            pass_on(guest, e)

    def attend(u, carry):
        i, g = u // kvh, u % kvh
        query = q_ref[i, pl.ds(g * per_kv, per_kv)].reshape(lead, hd)

        def fold(k, state):
            top, total, mixed = state
            keys = kvbuf[:, g, 0, k].reshape(n * tok, hd)
            values = kvbuf[:, g, 1, k].reshape(n * tok, hd)
            scores = lax.dot_general(
                query, keys, (((1,), (1,)), ((), ())), preferred_element_type=jnp.float32
            )
            high = jnp.maximum(top, jnp.max(scores, axis=1, keepdims=True))
            shrink = jnp.exp2((top - high) * scale)
            weights = jnp.exp2((scores - high) * scale)
            total = total * shrink + jnp.sum(weights, axis=1, keepdims=True)
            mixed = mixed * shrink + jnp.dot(
                weights.astype(jnp.bfloat16), values, preferred_element_type=jnp.float32
            )
            return high, total, mixed

        start = (
            jnp.full((lead, 1), -1e30, jnp.float32),
            jnp.zeros((lead, 1), jnp.float32),
            jnp.zeros((lead, hd), jnp.float32),
        )
        _, total, mixed = lax.fori_loop(0, first + i + 1, fold, start)
        result = (mixed / total).astype(jnp.bfloat16).reshape(per_kv, tok, hd)
        for h in range(per_kv):
            abuf[
                pl.ds(pl.multiple_of(i * tok, tok), tok),
                pl.ds(pl.multiple_of((g * per_kv + h) * hd, hd), hd),
            ] = result[h]

        @pl.when(both(is_end, g == kvh - 1))
        def _():
            a_copy(i).start()

        @pl.when(is_host)
        def _():
            for k in range(pace):
                outer((u + 1) * pace + k)
                inner((u + 1) * pace + k)
                relay_in((u + 1) * pace + k - lag)

        @pl.when(both(is_end, c != 0))
        def _():
            for k in range(pace):
                inner((u - 1) * pace + k)

        return carry

    lax.fori_loop(0, units, attend, 0)

    @pl.when(is_end)
    def _():
        done = jnp.where(c == 0, 0, min((units - 1) * pace, keep))
        lax.fori_loop(done, keep, lambda e, carry: (inner(e), carry)[1], 0)

    def own(j, carry):
        project(z, j)
        return carry

    all_w().wait()
    lax.fori_loop(0, jnp.where(is_end, parts, 0), own, 0)

    turn = jnp.where(c == 0, 4 * pace, 6 * pace)
    shift, due, sums, go, own_at = 4 * pace, 9 * pace, 2 * parts, 3 * pace, 5 * pace

    def run(e, carry):
        @pl.when(both(is_end, e == go))
        def _():
            own_weights(way_in, ahead, parts)
            for j in range(late, parts):
                rest_copy(z, j).start()

        @pl.when(is_host)
        def _():
            @pl.when(e > units * pace)
            def _():
                inner(e)

            k = e - shift

            @pl.when(both(k >= ahead, k < parts))
            def _():
                arrive(guest, k, -inward)

        @pl.when(jnp.logical_or(is_end, e > units * pace))
        def _():
            relay_in(e - lag)

        @pl.when(both(is_host, e == turn))
        def _():
            rows_in = abuf.at[pl.ds(rows_own, rows_own)]
            remote(rows_in, rows_in, a_send, a_recv, {"seq": guest}).wait_recv()

            def catch_up(f, carry):
                project_guest(*source(f - parts))
                return carry

            lax.fori_loop(keep, turn - gap + parts, catch_up, 0)

        f = e - gap

        @pl.when(both(f >= 0, f < length))
        def _():
            gather_project(*source(f))

            @pl.when(both(is_host, e >= turn))
            def _():
                project_guest(*source(f))

        @pl.when(both(is_host, e == turn + 2 * pace))
        def _():
            lax.fori_loop(keep, parts, lambda f, carry: (pass_sum(f), carry)[1], 0)

        k = e - gap - 2 * pace - pick

        @pl.when(both(is_host, both(k >= 0, k < shared)))
        def _():
            pass_sum(parts + pick + k)

        k = e - own_at

        @pl.when(both(is_host, both(k >= 0, k < parts)))
        def _():
            project(z, k)

        k = e - due + late

        @pl.when(both(is_host, both(k >= late, k < parts)))
        def _():
            rest_copy(guest, k).wait_recv()
            core_copy(guest, k, 1).start()

        k = jnp.where(f < late, f, k - 1)

        @pl.when(both(is_host, both(k >= 0, jnp.logical_or(f < late, both(k >= late, k < parts)))))
        def _():
            gathered(guest, k)

        q = e - sums

        @pl.when(both(q >= 0, q < owned * parts))
        def _():
            finish(q)

        return carry

    lax.fori_loop(
        2, max(last * parts + most, due + parts - late + 1, sums + owned * parts), run, 0
    )

    piece = pl.ds(0, quarter)
    pair = pl.ds(0, 2 * quarter)

    @pl.when(is_end)
    def _():
        sent(kv_ref, kv_send.at[0])
        sent(w_ref.at[piece], wz_send.at[0])
        sent(w_ref.at[piece, pl.ds(0, (parts - late) * sub)], wf_send)
        sent(wbuf.at[0, pl.ds(0, keep), pair], wc_send)
        sent(wbuf.at[0, pl.ds(0, keep), piece], wy_send.at[0])
        sent(abuf.at[pl.ds(0, rows_own)], a_send)
        sent(csend.at[pl.ds(0, owned * parts - shared)], x_send)

    @pl.when(is_host)
    def _():
        sent(kvbuf.at[pl.ds(0, 2), :, :, pl.ds(0, spans)], kv_send.at[0])
        sent(kvbuf.at[pl.ds(0, n - 1), :, :, pl.ds(0, spans)], kv_send.at[1])
        sent(w_ref.at[piece], wz_send.at[0])
        sent(w_ref.at[piece, pl.ds(0, keep * sub)], wz_send.at[1])
        sent(wbuf.at[0, :, piece], wz_send.at[2])
        sent(wbuf.at[pl.ds(0, n - 1), :, pair], wc_send)
        sent(wbuf.at[pl.ds(0, n - 2), :, piece], wy_send.at[0])
        sent(w_ref.at[piece, pl.ds(0, late * sub)], wy_send.at[1])
        sent(csend.at[pl.ds(0, csend.shape[0] - shared)], c_send)
        sent(gsend, g_send)
        sent(xsend, x_send)

    @pl.when(c == 0)
    def _():
        sent(kvbuf.at[:, :, :, pl.ds(0, spans)], kvc_send)

    pltpu.make_async_copy(out_ref, out_hbm, out_sem).wait()


def fused(parts, queries, key_states, value_states, out_weight, noise_table, plan):
    spans, tok, heads, hd = queries.shape
    kvh = key_states.shape[2]
    depth, cols = out_weight.shape
    n, tps, cores = lax.axis_size("seq"), lax.axis_size("tp"), lax.axis_size("span")
    sub, owned, wide = cols // parts, n // tps, noise_table.shape[1]
    keep, late, ahead = 4 * parts // 6, parts // 6, 4 * parts // 6
    pick, shared = keep, parts - keep
    extra, taken = (n - 1) * parts - keep, (n - 1) * parts
    q = jnp.transpose(queries, (0, 2, 1, 3))
    kv = jnp.stack([key_states, value_states], axis=0).transpose(3, 0, 1, 2, 4)
    where_it_is = pl.BlockSpec(memory_space=pl.ANY)
    far = pl.BlockSpec(memory_space=pltpu.HBM)
    dma = pltpu.SemaphoreType.DMA
    tile = (owned, parts, spans * tok, sub)
    out = pl.pallas_call(
        functools.partial(fused_kernel, parts, keep, late, ahead, pick),
        out_shape=jax.ShapeDtypeStruct((spans * tok, wide), jnp.bfloat16),
        in_specs=[
            pl.BlockSpec(memory_space=pltpu.SMEM), far, where_it_is, far, far,
        ],
        out_specs=where_it_is,
        scratch_shapes=[
            pltpu.VMEM((n, kvh, 2, spans * cores, tok, hd), jnp.bfloat16),
            pltpu.VMEM((n, parts, depth, sub), jnp.bfloat16),
            pltpu.VMEM((2 * spans * tok, depth), jnp.bfloat16),
            pltpu.VMEM(tile, jnp.float32),
            pltpu.VMEM(tile, jnp.bfloat16),
            pltpu.VMEM(tile, jnp.bfloat16),
            pltpu.VMEM((extra, spans * tok, sub), jnp.bfloat16),
            pltpu.VMEM((extra, spans * tok, sub), jnp.bfloat16),
            dma((2,)), dma((n, kvh)), dma, dma, dma((4,)),
            dma((3,)), dma((taken,)), dma, dma((parts,)),
            dma, dma((taken,)), dma((2,)), dma((taken,)),
            dma, dma((owned, parts)), dma, dma, dma, dma((extra,)),
            pltpu.VMEM((spans, 1, wide), jnp.float32),
            pltpu.VMEM(q.shape, q.dtype),
            pltpu.VMEM(noise_table.shape, noise_table.dtype),
            pltpu.VMEM((spans * tok, wide), jnp.bfloat16),
            dma,
            pltpu.VMEM((shared, spans * tok, sub), jnp.bfloat16),
            pltpu.VMEM((shared, spans * tok, sub), jnp.bfloat16),
            pltpu.VMEM((shared, spans * tok, sub), jnp.float32),
            dma, dma((shared,)),
        ],
        compiler_params=pltpu.CompilerParams(
            collective_id=0, has_side_effects=True, vmem_limit_bytes=48 * 1024 * 1024
        ),
        name="relay_attention",
    )(plan, q, kv, noise_table, out_weight)
    return out.reshape(spans, tok, wide)


def fold_block(carried, query_rows, key_rows, value_rows, factor):
    maxima, totals, weighted = carried
    scores = (
        jnp.einsum("tkgd,skd->tkgs", query_rows, key_rows, preferred_element_type=jnp.float32)
        * factor
    )
    highest = jnp.maximum(maxima, jnp.max(scores, axis=-1))
    shrink = jnp.exp(maxima - highest)
    weights = jnp.exp(scores - highest[..., None])
    totals = totals * shrink + jnp.sum(weights, axis=-1)
    weighted = weighted * shrink[..., None] + jnp.einsum(
        "tkgs,skd->tkgd",
        weights.astype(jnp.bfloat16),
        value_rows,
        preferred_element_type=jnp.float32,
    )
    return (maxima * 0.0 + highest, totals, weighted)


def per_device(queries, key_states, value_states, out_weight, noise_table, plan):
    ch_dev, tok_dev, heads_local, head_size = queries.shape
    kv_local = key_states.shape[2]
    per_kv = heads_local // kv_local
    span_count = ch_dev * lax.axis_size("span")
    first_span = lax.axis_index("span") * ch_dev
    factor = head_size ** (-0.5)
    grouped = queries.reshape(ch_dev, tok_dev, kv_local, per_kv, head_size)
    start_max = jnp.full((ch_dev, tok_dev, kv_local, per_kv), -1e30, jnp.float32)
    start_tot = jnp.zeros((ch_dev, tok_dev, kv_local, per_kv), jnp.float32)
    start_acc = jnp.zeros((ch_dev, tok_dev, kv_local, per_kv, head_size), jnp.float32)
    span_rows = (
        lax.all_gather(key_states, "seq", axis=1, tiled=True),
        lax.all_gather(value_states, "seq", axis=1, tiled=True),
    )
    key_piece = lax.all_gather(span_rows[0], "span", axis=0, tiled=True)
    value_piece = lax.all_gather(span_rows[1], "span", axis=0, tiled=True)
    new_max = []
    new_tot = []
    new_acc = []
    for q_span in range(ch_dev):
        inner_state = (start_max[q_span], start_tot[q_span], start_acc[q_span])
        for k_span in range(span_count):

            def update(inner, q_span=q_span, k_span=k_span):
                return fold_block(
                    inner, grouped[q_span], key_piece[k_span], value_piece[k_span], factor
                )

            inner_state = lax.cond(
                k_span <= first_span + q_span, update, lambda inner: inner, inner_state
            )
        new_max.append(inner_state[0])
        new_tot.append(inner_state[1])
        new_acc.append(inner_state[2])
    attn = (
        (jnp.stack(new_acc) / jnp.stack(new_tot)[..., None])
        .reshape(ch_dev, tok_dev, heads_local * head_size)
        .astype(jnp.bfloat16)
    )
    columns = jnp.einsum(
        "ctf,fo->cto",
        lax.all_gather(attn, "seq", axis=1, tiled=True),
        out_weight,
        preferred_element_type=jnp.float32,
    )
    partial_out = lax.all_to_all(
        columns.astype(jnp.bfloat16), "seq", split_axis=1, concat_axis=2, tiled=True
    ).astype(columns.dtype)
    summed = lax.psum_scatter(
        partial_out.astype(jnp.bfloat16), "tp", scatter_dimension=2, tiled=True
    ).astype(jnp.float32)
    levels = lax.dynamic_slice_in_dim(plan, first_span, ch_dev)
    picks = (levels[:, None] == jnp.arange(noise_table.shape[0], dtype=jnp.int32)[None, :]).astype(
        jnp.float32
    )
    gates = jnp.dot(picks, noise_table, precision=lax.Precision.HIGHEST)
    return (summed * gates[:, None, :]).astype(jnp.bfloat16)


def choose_parts(cols):
    for parts in (6, 3, 2, 1):
        if cols % (parts * 128) == 0:
            return parts
    return 0


def dispatch(queries, key_states, value_states, out_weight, noise_table, plan):
    depth, cols = out_weight.shape
    copies = lax.axis_size("rep") * lax.axis_size("span")
    parts = choose_parts(cols)
    pairs = all(lax.axis_size(name) == 2 for name in ("rep", "span", "tp"))
    args = (queries, key_states, value_states, out_weight, noise_table, plan)
    line = lax.axis_size("seq") == 2 * lax.axis_size("tp")
    if pairs and parts and depth % (copies * 16) == 0 and line:
        return fused(parts, *args)
    return per_device(*args)


def solution(mesh):
    placed = (
        P(("rep", "span"), "seq", "tp", None),
        P(("rep", "span"), "seq", "tp", None),
        P(("rep", "span"), "seq", "tp", None),
        P("tp", "seq"),
        P(None, "tp"),
        P("rep"),
    )
    return jax.shard_map(
        dispatch,
        mesh=mesh,
        in_specs=placed,
        out_specs=P(("rep", "span"), "seq", "tp"),
        check_vma=False,
    )
```

```python
import functools
import math

import jax
import jax.numpy as jnp
from jax import lax
from jax.experimental import pallas as pl
from jax.experimental.pallas import tpu as pltpu
from jax.sharding import PartitionSpec as P

MESH = pl.DeviceIdType.MESH


def fused_kernel(
    parts, keep, late, ahead, pick, plan_ref, q_hbm, kv_ref, noise_hbm, w_ref, out_hbm,
    kvbuf, wbuf, abuf, pbuf, xsend, xbuf, csend, cbuf,
    kv_send, kv_recv, kvc_send, kvc_recv, loc, wz_send, wz_recv, wf_send, wf_recv,
    wc_send, wc_recv, wy_send, wy_recv, x_send, x_recv, a_send, a_recv, c_send, c_recv, gates,
    q_ref, noise_ref, out_ref, out_sem,
    gsend, grecv, gpart, g_send, g_recv, wl_send, wl_recv, cs_recv, xs_recv,
):
    y, c = lax.axis_index("rep"), lax.axis_index("span")
    z, t = lax.axis_index("seq"), lax.axis_index("tp")
    n = lax.axis_size("seq")
    cores, tps = lax.axis_size("span"), lax.axis_size("tp")
    spans, heads, tok, hd = q_hbm.shape
    kvh = kv_ref.shape[0]
    per_kv = heads // kvh
    depth, cols = w_ref.shape
    quarter = depth // (cores * lax.axis_size("rep"))
    sub = cols // parts
    owned = n // tps
    rows_own = spans * tok
    first = c * spans
    last = n - 1
    scale = hd ** (-0.5) * math.log2(math.e)
    both = jnp.logical_and

    is_end = jnp.logical_or(z == 0, z == last)
    is_host = jnp.logical_not(is_end)
    inward = jnp.where(2 * z < n, 1, -1)
    way_in = (1 + inward) // 2
    way_out = 1 - way_in
    guest = z - inward
    length = jnp.where(is_end, last, last - 1) * parts

    base = jnp.where(is_end, z + inward, z)

    def order(k):
        behind = both(k >= parts - 1, k < 2 * parts - 1)
        j = jnp.where(behind, k - parts + 1, jnp.minimum(k, parts - 1))
        return behind, j

    def source(e):
        k = e - jnp.where(is_end, parts, 0)
        behind, j = order(k)
        step = jnp.where(k < 0, 0, jnp.where(behind, 2, 1))
        return base + inward * step, jnp.where(k < 0, k + parts, j)

    def place(r, s, j):
        return (jnp.abs(s - r) - 1) * parts + j - keep

    def wanted(r, s, j):
        far = place(r, s, j) >= 0
        return jnp.logical_not(both(jnp.logical_or(r == 0, r == last), far))

    shared = parts - keep

    def summed(r, s, j):
        f = place(r, s, j) + keep
        k = f - parts - pick
        return jnp.logical_or(both(f >= keep, f < parts), both(k >= 0, k < shared))

    def sum_at(r, s, j):
        f = place(r, s, j) + keep
        return jnp.where(f < parts, f - keep, f - parts - pick)

    def whole(s, j):
        final = both(s == z + inward, j == parts - 1)
        return both(is_host, jnp.logical_or(both(s == guest, j >= late), final))

    def rows(yy, cc):
        return pl.ds(pl.multiple_of((yy * cores + cc) * quarter, quarter), quarter)

    def columns(j):
        return pl.ds(pl.multiple_of(j * sub, sub), sub)

    def remote(src, dst, send, recv, where):
        return pltpu.make_async_remote_copy(
            src_ref=src, dst_ref=dst, send_sem=send, recv_sem=recv,
            device_id=where, device_id_type=MESH,
        )

    def turn_of(r, s, j):
        inside = (s - r) * jnp.where(2 * r < n, 1, -1) > 0
        return jnp.where(inside, (jnp.abs(s - r) - 1) * parts, (n - 2) * parts) + j

    def sent(part, sem):
        remote(part, part, sem, sem, {"span": 1 - c}).wait_send()

    def z_copy(s, j, way, own):
        dst = wbuf.at[s, j, rows(y, c)]
        src = w_ref.at[rows(y, c), columns(j)] if own else dst
        to = z + 2 * way - 1
        group = jnp.where(way == way_in, 0, 1) if own else 2
        return remote(src, dst, wz_send.at[group], wz_recv.at[turn_of(to, s, j)], {"seq": to})

    def z_arrival(s, j):
        dst = wbuf.at[s, j, rows(y, c)]
        return remote(dst, dst, wz_send.at[2], wz_recv.at[turn_of(z, s, j)], {"seq": z + inward})

    def rest_copy(s, j):
        src = w_ref.at[rows(1 - y, c), columns(j)]
        return remote(
            src, wbuf.at[s, j, rows(1 - y, c)], wf_send, wf_recv.at[j], {"seq": z + inward}
        )

    def final_copy():
        src = w_ref.at[rows(1 - y, c), columns(parts - 1)]
        return remote(
            src, wbuf.at[z, parts - 1, rows(1 - y, c)], wl_send, wl_recv, {"seq": z + inward}
        )

    def core_copy(s, j, kind):
        part = wbuf.at[s, j, rows(y if kind == 0 else 1 - y, c)]
        return remote(part, part, wc_send, wc_recv.at[turn_of(z, s, j)], {"span": 1 - c})

    def core_arrival(s, j):
        part = wbuf.at[s, j, pl.ds(0, 2 * quarter)]
        return remote(part, part, wc_send, wc_recv.at[turn_of(z, s, j)], {"span": 1 - c})

    def y_copy(s, j):
        part = wbuf.at[s, j, rows(y, c)]
        group = jnp.where(s == guest, 1, jnp.where(s == z + 2 * inward, 2, 0))
        return remote(
            part, part, wy_send.at[group], wy_recv.at[turn_of(z, s, j)], {"rep": 1 - y}
        )

    def x_copy(s, j, src):
        at = lax.rem(s, owned)
        return remote(
            src, xbuf.at[at, j], x_send, x_recv.at[at, j], {"tp": 1 - t}
        )

    def a_copy(i):
        src = abuf.at[pl.ds(pl.multiple_of(i * tok, tok), tok)]
        dst = abuf.at[pl.ds(pl.multiple_of(rows_own + i * tok, tok), tok)]
        return remote(src, dst, a_send, a_recv, {"seq": z + inward})

    def c_copy(f):
        return remote(
            csend.at[f], cbuf.at[f], c_send, c_recv.at[f], {"seq": z - inward}
        )

    def g_copy(k):
        return remote(gsend.at[k], grecv.at[k], g_send, g_recv.at[k], {"tp": 1 - t})

    end_place = 2 * parts - 1 - keep

    def c_part(i):
        at = pl.ds(i * tok, tok)
        return remote(
            csend.at[end_place, at], cbuf.at[end_place, at], c_send, cs_recv.at[i],
            {"seq": z - inward},
        )

    def x_part(i, at, j):
        mine = pl.ds(i * tok, tok)
        return remote(
            cbuf.at[end_place, mine], xbuf.at[at, j, mine], x_send, xs_recv.at[i], {"tp": 1 - t}
        )

    def kv_copy(s, g, way, own):
        dst = kvbuf.at[s, g, :, pl.ds(first, spans)]
        src = kv_ref.at[g] if own else dst
        to = z + 2 * way - 1
        group = jnp.where(way == way_in, 0, 1)
        return remote(src, dst, kv_send.at[group], kv_recv.at[s, g], {"seq": to})

    def kv_core(s, g):
        part = kvbuf.at[s, g, :, pl.ds(0, spans)]
        return remote(part, part, kvc_send, kvc_recv, {"span": 1 - c})

    def local_w(j):
        return pltpu.make_async_copy(w_ref.at[:, columns(j)], wbuf.at[z, j], loc.at[3])

    def all_w():
        return pltpu.make_async_copy(wbuf.at[z], wbuf.at[z], loc.at[3])

    def local_q():
        return pltpu.make_async_copy(q_hbm, q_ref, loc.at[1])

    def local_noise():
        return pltpu.make_async_copy(noise_hbm, noise_ref, loc.at[2])

    def put_copy(s, j):
        at = pl.ds(pl.multiple_of(lax.rem(s, owned) * cols + j * sub, 128), sub)
        return pltpu.make_async_copy(
            out_ref.at[:, at], out_hbm.at[:, at], out_sem
        )

    def local_kv():
        return pltpu.make_async_copy(
            kv_ref, kvbuf.at[z, :, :, pl.ds(first, spans)], loc.at[0]
        )

    reach = ((0, z > 0), (1, z < last))

    barrier = pltpu.get_barrier_semaphore()
    for way, ok in reach:
        @pl.when(ok)
        def _(way=way):
            to = z - 1 if way == 0 else z + 1
            pl.semaphore_signal(barrier, inc=1, device_id={"seq": to}, device_id_type=MESH)
    pl.semaphore_signal(barrier, inc=1, device_id={"rep": 1 - y}, device_id_type=MESH)
    pl.semaphore_signal(barrier, inc=1, device_id={"span": 1 - c}, device_id_type=MESH)
    pl.semaphore_signal(barrier, inc=1, device_id={"tp": 1 - t}, device_id_type=MESH)
    pl.semaphore_wait(barrier, jnp.where(is_end, 4, 5))

    for g in range(kvh):
        for way, ok in reach:
            @pl.when(ok)
            def _(g=g, way=way):
                kv_copy(z, g, way, True).start()
    local_kv().start()

    def own_weights(way, low, high):
        for j in range(low, high):
            z_copy(z, j, way, True).start()

    local_q().start()
    local_noise().start()
    for j in range(parts):
        local_w(j).start()

    @pl.when(is_end)
    def _():
        own_weights(way_in, 0, ahead)

    local_kv().wait()

    @pl.when(c == 0)
    def _():
        for g in range(kvh):
            kv_core(z, g).start()

    def receive(s, g, way):
        kv_copy(s, g, way, False).wait_recv()
        to = z + 2 * way - 1

        @pl.when(both(to >= 0, to < n))
        def _():
            kv_copy(s, g, way, False).start()

        @pl.when(c == 0)
        def _():
            kv_core(s, g).start()

    def arrive(s, j, sign):
        way = (1 - sign) // 2
        onward = z - sign

        @pl.when(wanted(z, s, j))
        def _():
            z_arrival(s, j).wait_recv()

            @pl.when(both(both(onward >= 0, onward < n), wanted(onward, s, j)))
            def _():
                z_copy(s, j, way, False).start()

            @pl.when(jnp.logical_not(whole(s, j)))
            def _():
                y_copy(s, j).start()

            core_copy(s, j, 0).start()

    def pass_on(s, j):
        @pl.when(wanted(z, s, j))
        def _():
            @pl.when(whole(s, j))
            def _():
                final_copy().wait_recv()

            @pl.when(jnp.logical_not(whole(s, j)))
            def _():
                y_copy(s, j).wait_recv()

            core_copy(s, j, 1).start()

    def project(s, j):
        part = jnp.dot(
            abuf[pl.ds(0, rows_own)], wbuf[s, j], preferred_element_type=jnp.float32
        )
        at = lax.rem(s, owned)

        @pl.when(s // owned == t)
        def _():
            pbuf[at, j] = part

        @pl.when(s // owned != t)
        def _():
            xsend[at, j] = part.astype(jnp.bfloat16)
            x_copy(s, j, xsend.at[at, j]).start()

    def project_guest(s, j):
        part = jnp.dot(
            abuf[pl.ds(rows_own, rows_own)], wbuf[s, j], preferred_element_type=jnp.float32
        )
        f = place(guest, s, j)
        k = sum_at(guest, s, j)
        add = summed(guest, s, j)
        mine = s // owned == t

        @pl.when(jnp.logical_not(add))
        def _():
            csend[f] = part.astype(jnp.bfloat16)

            @pl.when(f == end_place)
            def _():
                for i in range(spans):
                    c_part(i).start()

            @pl.when(f != end_place)
            def _():
                c_copy(f).start()

        @pl.when(both(add, mine))
        def _():
            gpart[k] = part

        @pl.when(both(add, jnp.logical_not(mine)))
        def _():
            gsend[k] = part.astype(jnp.bfloat16)
            g_copy(k).start()

    def pass_sum(f):
        s, j = source(f - parts)

        @pl.when(s // owned == t)
        def _():
            f = place(guest, s, j)
            k = sum_at(guest, s, j)
            g_copy(k).wait_recv()
            csend[f] = (gpart[k] + grecv[k].astype(jnp.float32)).astype(jnp.bfloat16)
            c_copy(f).start()

    def gathered(s, j):
        core_arrival(s, j).wait_recv()
        project(s, j)

    def gather_project(s, j):
        @pl.when(wanted(z, s, j))
        def _():
            gathered(s, j)

        @pl.when(jnp.logical_not(jnp.logical_or(wanted(z, s, j), summed(z, s, j))))
        def _():
            f = place(z, s, j)
            away = s // owned != t

            @pl.when(f == end_place)
            def _():
                for i in range(spans):
                    c_part(i).wait_recv()

                    @pl.when(away)
                    def _(i=i):
                        x_part(i, lax.rem(s, owned), j).start()

            @pl.when(f != end_place)
            def _():
                c_copy(f).wait_recv()

                @pl.when(away)
                def _():
                    x_copy(s, j, cbuf.at[f]).start()

    mine = t * owned
    near = z // owned == t
    front = jnp.where(near, z, jnp.where(inward > 0, mine, mine + owned - 1))
    rear = 2 * mine + owned - 1 - front

    def finish(q):
        behind, j = order(q)
        behind = jnp.logical_or(both(near, q >= parts), both(jnp.logical_not(near), behind))
        s, j = jnp.where(behind, rear, front), jnp.where(near, lax.rem(q, parts), j)
        at = lax.rem(s, owned)
        whole_sum = both(is_end, summed(z, s, j))

        @pl.when(whole_sum)
        def _():
            c_copy(place(z, s, j)).wait_recv()

        split = both(is_end, place(z, s, j) == end_place)

        @pl.when(split)
        def _():
            for i in range(spans):
                x_part(i, at, j).wait_recv()

        @pl.when(jnp.logical_not(jnp.logical_or(whole_sum, split)))
        def _():
            x_copy(s, j, xsend.at[at, j]).wait_recv()

        where = pl.ds(pl.multiple_of(at * cols + j * sub, 128), sub)

        def put(total):
            for i in range(spans):
                span = pl.ds(i * tok, tok)
                out_ref[span, where] = (total(span) * gates[i, :, where]).astype(out_ref.dtype)

        def other(span):
            return xbuf[at, j, span, :].astype(jnp.float32)

        def guests(span):
            return cbuf[place(z, s, j), span, :].astype(jnp.float32)

        @pl.when(wanted(z, s, j))
        def _():
            put(lambda span: pbuf[at, j, span, :] + other(span))

        @pl.when(whole_sum)
        def _():
            put(guests)

        @pl.when(jnp.logical_not(jnp.logical_or(wanted(z, s, j), whole_sum)))
        def _():
            put(lambda span: guests(span) + other(span))

        put_copy(s, j).start()

    lag, most = 2, 3
    gap = jnp.where(c == 0, 2, 3)
    lead = per_kv * tok
    units = spans * kvh
    pace = max(parts // 6, 1)

    def inner(e):
        s, j = source(e)

        @pl.when(both(e >= 0, e < length))
        def _():
            arrive(s, j, inward)

    def outer(e):
        @pl.when(both(e >= 0, e < ahead))
        def _():
            arrive(guest, e, -inward)

    @pl.when(is_end)
    def _():
        for d in range(1, n):
            for g in range(kvh):
                receive(z + inward * d, g, way_out)

    @pl.when(is_host)
    def _():
        for g in range(kvh):
            receive(guest, g, way_in)
            receive(z + inward, g, way_out)
        own_weights(way_in, 0, parts - 1)
        for g in range(kvh):
            receive(z + 2 * inward, g, way_out)
        own_weights(way_out, 0, keep)
        for k in range(pace):
            outer(k)
            inner(k)

    local_q().wait()
    local_noise().wait()
    for i in range(spans):
        gates[i] = noise_ref[pl.ds(plan_ref[first + i], 1), :]

    @pl.when(c != 0)
    def _():
        kv_all = kvbuf.at[:, :, :, pl.ds(0, spans)]
        remote(kv_all, kv_all, kvc_send, kvc_recv, {"span": 1 - c}).wait_recv()

    def relay_in(e):
        @pl.when(both(e >= 0, e < length))
        def _():
            pass_on(*source(e))

        @pl.when(both(is_host, both(e >= 0, e < late)))
        def _():
            pass_on(guest, e)

    def attend(u, carry):
        i, g = u // kvh, u % kvh
        query = q_ref[i, pl.ds(g * per_kv, per_kv)].reshape(lead, hd)

        def fold(k, state):
            top, total, mixed = state
            keys = kvbuf[:, g, 0, k].reshape(n * tok, hd)
            values = kvbuf[:, g, 1, k].reshape(n * tok, hd)
            scores = lax.dot_general(
                query, keys, (((1,), (1,)), ((), ())), preferred_element_type=jnp.float32
            )
            high = jnp.maximum(top, jnp.max(scores, axis=1, keepdims=True))
            shrink = jnp.exp2((top - high) * scale)
            weights = jnp.exp2((scores - high) * scale)
            total = total * shrink + jnp.sum(weights, axis=1, keepdims=True)
            mixed = mixed * shrink + jnp.dot(
                weights.astype(jnp.bfloat16), values, preferred_element_type=jnp.float32
            )
            return high, total, mixed

        start = (
            jnp.full((lead, 1), -1e30, jnp.float32),
            jnp.zeros((lead, 1), jnp.float32),
            jnp.zeros((lead, hd), jnp.float32),
        )
        _, total, mixed = lax.fori_loop(0, first + i + 1, fold, start)
        result = (mixed / total).astype(jnp.bfloat16).reshape(per_kv, tok, hd)
        for h in range(per_kv):
            abuf[
                pl.ds(pl.multiple_of(i * tok, tok), tok),
                pl.ds(pl.multiple_of((g * per_kv + h) * hd, hd), hd),
            ] = result[h]

        @pl.when(both(is_end, g == kvh - 1))
        def _():
            a_copy(i).start()

        @pl.when(is_host)
        def _():
            for k in range(pace):
                outer((u + 1) * pace + k)
                inner((u + 1) * pace + k)
                relay_in((u + 1) * pace + k - lag)

        @pl.when(both(is_end, c != 0))
        def _():
            for k in range(pace):
                inner((u - 1) * pace + k)

        return carry

    lax.fori_loop(0, units, attend, 0)

    @pl.when(is_end)
    def _():
        done = jnp.where(c == 0, 0, min((units - 1) * pace, keep))
        lax.fori_loop(done, keep, lambda e, carry: (inner(e), carry)[1], 0)

    def own(j, carry):
        project(z, j)
        return carry

    all_w().wait()
    lax.fori_loop(0, jnp.where(is_end, parts, 0), own, 0)

    turn = jnp.where(c == 0, 4 * pace, 6 * pace)
    shift, due, sums, go, own_at = 3 * pace, 9 * pace, 2 * parts, 3 * pace, jnp.where(c == 0, 5 * pace, 2 * pace)

    def run(e, carry):
        @pl.when(both(is_end, e == go))
        def _():
            own_weights(way_in, ahead, parts)
            for j in range(late, parts):
                rest_copy(z, j).start()

        @pl.when(is_host)
        def _():
            @pl.when(e > units * pace)
            def _():
                inner(e)

            k = e - shift

            @pl.when(both(k >= ahead, k < parts))
            def _():
                arrive(guest, k, -inward)

            @pl.when(k == parts - 1)
            def _():
                own_weights(way_in, parts - 1, parts)
                final_copy().start()

        @pl.when(jnp.logical_or(is_end, e > units * pace))
        def _():
            relay_in(e - lag)

        @pl.when(both(is_host, e == turn))
        def _():
            rows_in = abuf.at[pl.ds(rows_own, rows_own)]
            remote(rows_in, rows_in, a_send, a_recv, {"seq": guest}).wait_recv()

            def catch_up(f, carry):
                project_guest(*source(f - parts))
                return carry

            lax.fori_loop(keep, turn - gap + parts, catch_up, 0)

        f = e - gap

        @pl.when(both(f >= 0, f < length))
        def _():
            gather_project(*source(f))

            @pl.when(both(is_host, e >= turn))
            def _():
                project_guest(*source(f))

        @pl.when(both(is_host, e == turn + 2 * pace))
        def _():
            lax.fori_loop(keep, parts, lambda f, carry: (pass_sum(f), carry)[1], 0)

        k = e - gap - 2 * pace - pick

        @pl.when(both(is_host, both(k >= 0, k < shared)))
        def _():
            pass_sum(parts + pick + k)

        k = e - own_at

        @pl.when(both(is_host, both(k >= 0, k < parts)))
        def _():
            project(z, k)

        k = e - due + late

        @pl.when(both(is_host, both(k >= late, k < parts)))
        def _():
            rest_copy(guest, k).wait_recv()
            core_copy(guest, k, 1).start()

        k = jnp.where(f < late, f, k - 1)

        @pl.when(both(is_host, both(k >= 0, jnp.logical_or(f < late, both(k >= late, k < parts)))))
        def _():
            gathered(guest, k)

        q = e - sums

        @pl.when(both(q >= 0, q < owned * parts))
        def _():
            finish(q)

        return carry

    lax.fori_loop(
        2, max(last * parts + most, due + parts - late + 1, sums + owned * parts), run, 0
    )

    piece = pl.ds(0, quarter)
    pair = pl.ds(0, 2 * quarter)

    @pl.when(is_end)
    def _():
        sent(kv_ref, kv_send.at[0])
        sent(w_ref.at[piece], wz_send.at[0])
        sent(w_ref.at[piece, pl.ds(0, (parts - late) * sub)], wf_send)
        sent(wbuf.at[0, pl.ds(0, keep), pair], wc_send)
        sent(wbuf.at[0, pl.ds(0, keep), piece], wy_send.at[0])
        sent(abuf.at[pl.ds(0, rows_own)], a_send)
        sent(csend.at[pl.ds(0, owned * parts - shared)], x_send)

    @pl.when(is_host)
    def _():
        sent(kvbuf.at[pl.ds(0, 2), :, :, pl.ds(0, spans)], kv_send.at[0])
        sent(kvbuf.at[pl.ds(0, n - 1), :, :, pl.ds(0, spans)], kv_send.at[1])
        sent(w_ref.at[piece], wz_send.at[0])
        sent(w_ref.at[piece, pl.ds(0, keep * sub)], wz_send.at[1])
        sent(wbuf.at[0, :, piece], wz_send.at[2])
        sent(wbuf.at[pl.ds(0, n - 1), :, pair], wc_send)
        sent(wbuf.at[0, pl.ds(0, parts - 1), piece], wy_send.at[0])
        sent(wbuf.at[0, :, piece], wy_send.at[2])
        sent(wbuf.at[0, 0, piece], wl_send)
        sent(w_ref.at[piece, pl.ds(0, late * sub)], wy_send.at[1])
        sent(csend.at[pl.ds(0, csend.shape[0] - shared)], c_send)
        sent(gsend, g_send)
        sent(xsend, x_send)

    @pl.when(c == 0)
    def _():
        sent(kvbuf.at[:, :, :, pl.ds(0, spans)], kvc_send)

    pltpu.make_async_copy(out_ref, out_hbm, out_sem).wait()


def fused(parts, queries, key_states, value_states, out_weight, noise_table, plan):
    spans, tok, heads, hd = queries.shape
    kvh = key_states.shape[2]
    depth, cols = out_weight.shape
    n, tps, cores = lax.axis_size("seq"), lax.axis_size("tp"), lax.axis_size("span")
    sub, owned, wide = cols // parts, n // tps, noise_table.shape[1]
    keep, late, ahead = 4 * parts // 6, parts // 6, 4 * parts // 6
    pick, shared = 3 * parts // 6, parts - keep
    extra, taken = (n - 1) * parts - keep, (n - 1) * parts
    q = jnp.transpose(queries, (0, 2, 1, 3))
    kv = jnp.stack([key_states, value_states], axis=0).transpose(3, 0, 1, 2, 4)
    where_it_is = pl.BlockSpec(memory_space=pl.ANY)
    far = pl.BlockSpec(memory_space=pltpu.HBM)
    dma = pltpu.SemaphoreType.DMA
    tile = (owned, parts, spans * tok, sub)
    out = pl.pallas_call(
        functools.partial(fused_kernel, parts, keep, late, ahead, pick),
        out_shape=jax.ShapeDtypeStruct((spans * tok, wide), jnp.bfloat16),
        in_specs=[
            pl.BlockSpec(memory_space=pltpu.SMEM), far, where_it_is, far, far,
        ],
        out_specs=where_it_is,
        scratch_shapes=[
            pltpu.VMEM((n, kvh, 2, spans * cores, tok, hd), jnp.bfloat16),
            pltpu.VMEM((n, parts, depth, sub), jnp.bfloat16),
            pltpu.VMEM((2 * spans * tok, depth), jnp.bfloat16),
            pltpu.VMEM(tile, jnp.float32),
            pltpu.VMEM(tile, jnp.bfloat16),
            pltpu.VMEM(tile, jnp.bfloat16),
            pltpu.VMEM((extra, spans * tok, sub), jnp.bfloat16),
            pltpu.VMEM((extra, spans * tok, sub), jnp.bfloat16),
            dma((2,)), dma((n, kvh)), dma, dma, dma((4,)),
            dma((3,)), dma((taken,)), dma, dma((parts,)),
            dma, dma((taken,)), dma((3,)), dma((taken,)),
            dma, dma((owned, parts)), dma, dma, dma, dma((extra,)),
            pltpu.VMEM((spans, 1, wide), jnp.float32),
            pltpu.VMEM(q.shape, q.dtype),
            pltpu.VMEM(noise_table.shape, noise_table.dtype),
            pltpu.VMEM((spans * tok, wide), jnp.bfloat16),
            dma,
            pltpu.VMEM((shared, spans * tok, sub), jnp.bfloat16),
            pltpu.VMEM((shared, spans * tok, sub), jnp.bfloat16),
            pltpu.VMEM((shared, spans * tok, sub), jnp.float32),
            dma, dma((shared,)), dma, dma, dma((spans,)), dma((spans,)),
        ],
        compiler_params=pltpu.CompilerParams(
            collective_id=0, has_side_effects=True, vmem_limit_bytes=48 * 1024 * 1024
        ),
        name="relay_attention",
    )(plan, pltpu.with_memory_space_constraint(q, pltpu.HBM), kv, pltpu.with_memory_space_constraint(noise_table, pltpu.HBM), pltpu.with_memory_space_constraint(out_weight, pltpu.HBM))
    return out.reshape(spans, tok, wide)


def fold_block(carried, query_rows, key_rows, value_rows, factor):
    maxima, totals, weighted = carried
    scores = (
        jnp.einsum("tkgd,skd->tkgs", query_rows, key_rows, preferred_element_type=jnp.float32)
        * factor
    )
    highest = jnp.maximum(maxima, jnp.max(scores, axis=-1))
    shrink = jnp.exp(maxima - highest)
    weights = jnp.exp(scores - highest[..., None])
    totals = totals * shrink + jnp.sum(weights, axis=-1)
    weighted = weighted * shrink[..., None] + jnp.einsum(
        "tkgs,skd->tkgd",
        weights.astype(jnp.bfloat16),
        value_rows,
        preferred_element_type=jnp.float32,
    )
    return (maxima * 0.0 + highest, totals, weighted)


def per_device(queries, key_states, value_states, out_weight, noise_table, plan):
    ch_dev, tok_dev, heads_local, head_size = queries.shape
    kv_local = key_states.shape[2]
    per_kv = heads_local // kv_local
    span_count = ch_dev * lax.axis_size("span")
    first_span = lax.axis_index("span") * ch_dev
    factor = head_size ** (-0.5)
    grouped = queries.reshape(ch_dev, tok_dev, kv_local, per_kv, head_size)
    start_max = jnp.full((ch_dev, tok_dev, kv_local, per_kv), -1e30, jnp.float32)
    start_tot = jnp.zeros((ch_dev, tok_dev, kv_local, per_kv), jnp.float32)
    start_acc = jnp.zeros((ch_dev, tok_dev, kv_local, per_kv, head_size), jnp.float32)
    span_rows = (
        lax.all_gather(key_states, "seq", axis=1, tiled=True),
        lax.all_gather(value_states, "seq", axis=1, tiled=True),
    )
    key_piece = lax.all_gather(span_rows[0], "span", axis=0, tiled=True)
    value_piece = lax.all_gather(span_rows[1], "span", axis=0, tiled=True)
    new_max = []
    new_tot = []
    new_acc = []
    for q_span in range(ch_dev):
        inner_state = (start_max[q_span], start_tot[q_span], start_acc[q_span])
        for k_span in range(span_count):

            def update(inner, q_span=q_span, k_span=k_span):
                return fold_block(
                    inner, grouped[q_span], key_piece[k_span], value_piece[k_span], factor
                )

            inner_state = lax.cond(
                k_span <= first_span + q_span, update, lambda inner: inner, inner_state
            )
        new_max.append(inner_state[0])
        new_tot.append(inner_state[1])
        new_acc.append(inner_state[2])
    attn = (
        (jnp.stack(new_acc) / jnp.stack(new_tot)[..., None])
        .reshape(ch_dev, tok_dev, heads_local * head_size)
        .astype(jnp.bfloat16)
    )
    columns = jnp.einsum(
        "ctf,fo->cto",
        lax.all_gather(attn, "seq", axis=1, tiled=True),
        out_weight,
        preferred_element_type=jnp.float32,
    )
    partial_out = lax.all_to_all(
        columns.astype(jnp.bfloat16), "seq", split_axis=1, concat_axis=2, tiled=True
    ).astype(columns.dtype)
    summed = lax.psum_scatter(
        partial_out.astype(jnp.bfloat16), "tp", scatter_dimension=2, tiled=True
    ).astype(jnp.float32)
    levels = lax.dynamic_slice_in_dim(plan, first_span, ch_dev)
    picks = (levels[:, None] == jnp.arange(noise_table.shape[0], dtype=jnp.int32)[None, :]).astype(
        jnp.float32
    )
    gates = jnp.dot(picks, noise_table, precision=lax.Precision.HIGHEST)
    return (summed * gates[:, None, :]).astype(jnp.bfloat16)


def choose_parts(cols):
    for parts in (6, 3, 2, 1):
        if cols % (parts * 128) == 0:
            return parts
    return 0


def dispatch(queries, key_states, value_states, out_weight, noise_table, plan):
    depth, cols = out_weight.shape
    copies = lax.axis_size("rep") * lax.axis_size("span")
    parts = choose_parts(cols)
    pairs = all(lax.axis_size(name) == 2 for name in ("rep", "span", "tp"))
    args = (queries, key_states, value_states, out_weight, noise_table, plan)
    line = lax.axis_size("seq") == 2 * lax.axis_size("tp")
    if pairs and parts and depth % (copies * 16) == 0 and line:
        return fused(parts, *args)
    return per_device(*args)


def solution(mesh):
    placed = (
        P(("rep", "span"), "seq", "tp", None),
        P(("rep", "span"), "seq", "tp", None),
        P(("rep", "span"), "seq", "tp", None),
        P("tp", "seq"),
        P(None, "tp"),
        P("rep"),
    )
    return jax.shard_map(
        dispatch,
        mesh=mesh,
        in_specs=placed,
        out_specs=P(("rep", "span"), "seq", "tp"),
        check_vma=False,
    )
```

```python
import functools
import math

import jax
import jax.numpy as jnp
from jax import lax
from jax.experimental import pallas as pl
from jax.experimental.pallas import tpu as pltpu
from jax.sharding import PartitionSpec as P

MESH = pl.DeviceIdType.MESH


def fused_kernel(
    parts, keep, late, ahead, pick, plan_ref, q_hbm, kv_ref, noise_hbm, w_ref, out_hbm,
    kvbuf, wbuf, abuf, pbuf, xsend, xbuf, csend, cbuf,
    kv_send, kv_recv, kvc_send, kvc_recv, loc, wz_send, wz_recv, wf_send, wf_recv,
    wc_send, wc_recv, wy_send, wy_recv, x_send, x_recv, a_send, a_recv, c_send, c_recv, gates,
    q_ref, noise_ref, out_ref, out_sem,
    gsend, grecv, gpart, g_send, g_recv, wl_send, wl_recv, cs_recv, xs_recv,
):
    y, c = lax.axis_index("rep"), lax.axis_index("span")
    z, t = lax.axis_index("seq"), lax.axis_index("tp")
    n = lax.axis_size("seq")
    cores, tps = lax.axis_size("span"), lax.axis_size("tp")
    spans, heads, tok, hd = q_hbm.shape
    kvh = kv_ref.shape[0]
    per_kv = heads // kvh
    depth, cols = w_ref.shape
    quarter = depth // (cores * lax.axis_size("rep"))
    sub = cols // parts
    owned = n // tps
    rows_own = spans * tok
    first = c * spans
    last = n - 1
    scale = hd ** (-0.5) * math.log2(math.e)
    both = jnp.logical_and

    is_end = jnp.logical_or(z == 0, z == last)
    is_host = jnp.logical_not(is_end)
    inward = jnp.where(2 * z < n, 1, -1)
    way_in = (1 + inward) // 2
    way_out = 1 - way_in
    guest = z - inward
    length = jnp.where(is_end, last, last - 1) * parts

    base = jnp.where(is_end, z + inward, z)

    def order(k):
        behind = both(k >= parts - 1, k < 2 * parts - 1)
        j = jnp.where(behind, k - parts + 1, jnp.minimum(k, parts - 1))
        return behind, j

    def source(e):
        k = e - jnp.where(is_end, parts, 0)
        behind, j = order(k)
        step = jnp.where(k < 0, 0, jnp.where(behind, 2, 1))
        return base + inward * step, jnp.where(k < 0, k + parts, j)

    def place(r, s, j):
        return (jnp.abs(s - r) - 1) * parts + j - keep

    def wanted(r, s, j):
        far = place(r, s, j) >= 0
        return jnp.logical_not(both(jnp.logical_or(r == 0, r == last), far))

    shared = parts - keep

    def summed(r, s, j):
        f = place(r, s, j) + keep
        k = f - parts - pick
        return jnp.logical_or(both(f >= keep, f < parts), both(k >= 0, k < shared))

    def sum_at(r, s, j):
        f = place(r, s, j) + keep
        return jnp.where(f < parts, f - keep, f - parts - pick)

    def whole(s, j):
        final = both(s == z + inward, j == parts - 1)
        return both(is_host, jnp.logical_or(both(s == guest, j >= late), final))

    def rows(yy, cc):
        return pl.ds(pl.multiple_of((yy * cores + cc) * quarter, quarter), quarter)

    def columns(j):
        return pl.ds(pl.multiple_of(j * sub, sub), sub)

    def remote(src, dst, send, recv, where):
        return pltpu.make_async_remote_copy(
            src_ref=src, dst_ref=dst, send_sem=send, recv_sem=recv,
            device_id=where, device_id_type=MESH,
        )

    def turn_of(r, s, j):
        inside = (s - r) * jnp.where(2 * r < n, 1, -1) > 0
        return jnp.where(inside, (jnp.abs(s - r) - 1) * parts, (n - 2) * parts) + j

    def sent(part, sem):
        remote(part, part, sem, sem, {"span": 1 - c}).wait_send()

    def z_copy(s, j, way, own):
        dst = wbuf.at[s, j, rows(y, c)]
        src = w_ref.at[rows(y, c), columns(j)] if own else dst
        to = z + 2 * way - 1
        group = jnp.where(way == way_in, 0, 1) if own else 2
        return remote(src, dst, wz_send.at[group], wz_recv.at[turn_of(to, s, j)], {"seq": to})

    def z_arrival(s, j):
        dst = wbuf.at[s, j, rows(y, c)]
        return remote(dst, dst, wz_send.at[2], wz_recv.at[turn_of(z, s, j)], {"seq": z + inward})

    def rest_copy(s, j):
        src = w_ref.at[rows(1 - y, c), columns(j)]
        return remote(
            src, wbuf.at[s, j, rows(1 - y, c)], wf_send, wf_recv.at[j], {"seq": z + inward}
        )

    def final_copy():
        src = w_ref.at[rows(1 - y, c), columns(parts - 1)]
        return remote(
            src, wbuf.at[z, parts - 1, rows(1 - y, c)], wl_send, wl_recv, {"seq": z + inward}
        )

    def core_copy(s, j, kind):
        part = wbuf.at[s, j, rows(y if kind == 0 else 1 - y, c)]
        return remote(part, part, wc_send, wc_recv.at[turn_of(z, s, j)], {"span": 1 - c})

    def core_arrival(s, j):
        part = wbuf.at[s, j, pl.ds(0, 2 * quarter)]
        return remote(part, part, wc_send, wc_recv.at[turn_of(z, s, j)], {"span": 1 - c})

    def y_copy(s, j):
        part = wbuf.at[s, j, rows(y, c)]
        group = jnp.where(s == guest, 1, jnp.where(s == z + 2 * inward, 2, 0))
        return remote(
            part, part, wy_send.at[group], wy_recv.at[turn_of(z, s, j)], {"rep": 1 - y}
        )

    def x_copy(s, j, src):
        at = lax.rem(s, owned)
        return remote(
            src, xbuf.at[at, j], x_send, x_recv.at[at, j], {"tp": 1 - t}
        )

    def a_copy(i):
        src = abuf.at[pl.ds(pl.multiple_of(i * tok, tok), tok)]
        dst = abuf.at[pl.ds(pl.multiple_of(rows_own + i * tok, tok), tok)]
        return remote(src, dst, a_send, a_recv, {"seq": z + inward})

    def c_copy(f):
        return remote(
            csend.at[f], cbuf.at[f], c_send, c_recv.at[f], {"seq": z - inward}
        )

    def g_copy(k):
        return remote(gsend.at[k], grecv.at[k], g_send, g_recv.at[k], {"tp": 1 - t})

    end_place = 2 * parts - 1 - keep

    def c_part(i):
        at = pl.ds(i * tok, tok)
        return remote(
            csend.at[end_place, at], cbuf.at[end_place, at], c_send, cs_recv.at[i],
            {"seq": z - inward},
        )

    def x_part(i, at, j):
        mine = pl.ds(i * tok, tok)
        return remote(
            cbuf.at[end_place, mine], xbuf.at[at, j, mine], x_send, xs_recv.at[i], {"tp": 1 - t}
        )

    def kv_copy(s, g, way, own):
        dst = kvbuf.at[s, g, :, pl.ds(first, spans)]
        src = kv_ref.at[g] if own else dst
        to = z + 2 * way - 1
        group = jnp.where(way == way_in, 0, 1)
        return remote(src, dst, kv_send.at[group], kv_recv.at[s, g], {"seq": to})

    def kv_core(s, g):
        part = kvbuf.at[s, g, :, pl.ds(0, spans)]
        return remote(part, part, kvc_send, kvc_recv, {"span": 1 - c})

    def local_w(j):
        return pltpu.make_async_copy(w_ref.at[:, columns(j)], wbuf.at[z, j], loc.at[3])

    def all_w():
        return pltpu.make_async_copy(wbuf.at[z], wbuf.at[z], loc.at[3])

    def local_q():
        return pltpu.make_async_copy(q_hbm, q_ref, loc.at[1])

    def local_noise():
        return pltpu.make_async_copy(noise_hbm, noise_ref, loc.at[2])

    def put_copy(s, j):
        at = pl.ds(pl.multiple_of(lax.rem(s, owned) * cols + j * sub, 128), sub)
        return pltpu.make_async_copy(
            out_ref.at[:, at], out_hbm.at[:, at], out_sem
        )

    def local_kv():
        return pltpu.make_async_copy(
            kv_ref, kvbuf.at[z, :, :, pl.ds(first, spans)], loc.at[0]
        )

    reach = ((0, z > 0), (1, z < last))

    barrier = pltpu.get_barrier_semaphore()
    for way, ok in reach:
        @pl.when(ok)
        def _(way=way):
            to = z - 1 if way == 0 else z + 1
            pl.semaphore_signal(barrier, inc=1, device_id={"seq": to}, device_id_type=MESH)
    pl.semaphore_signal(barrier, inc=1, device_id={"rep": 1 - y}, device_id_type=MESH)
    pl.semaphore_signal(barrier, inc=1, device_id={"span": 1 - c}, device_id_type=MESH)
    pl.semaphore_signal(barrier, inc=1, device_id={"tp": 1 - t}, device_id_type=MESH)
    pl.semaphore_wait(barrier, jnp.where(is_end, 4, 5))

    for g in range(kvh):
        for way, ok in reach:
            @pl.when(ok)
            def _(g=g, way=way):
                kv_copy(z, g, way, True).start()
    local_kv().start()

    def own_weights(way, low, high):
        for j in range(low, high):
            z_copy(z, j, way, True).start()

    local_q().start()
    local_noise().start()
    for j in range(parts):
        local_w(j).start()

    @pl.when(is_end)
    def _():
        own_weights(way_in, 0, ahead)

    local_kv().wait()

    @pl.when(c == 0)
    def _():
        for g in range(kvh):
            kv_core(z, g).start()

    def receive(s, g, way):
        kv_copy(s, g, way, False).wait_recv()
        to = z + 2 * way - 1

        @pl.when(both(to >= 0, to < n))
        def _():
            kv_copy(s, g, way, False).start()

        @pl.when(c == 0)
        def _():
            kv_core(s, g).start()

    def arrive(s, j, sign):
        way = (1 - sign) // 2
        onward = z - sign

        @pl.when(wanted(z, s, j))
        def _():
            z_arrival(s, j).wait_recv()

            @pl.when(both(both(onward >= 0, onward < n), wanted(onward, s, j)))
            def _():
                z_copy(s, j, way, False).start()

            @pl.when(jnp.logical_not(whole(s, j)))
            def _():
                y_copy(s, j).start()

            core_copy(s, j, 0).start()

    def pass_on(s, j):
        @pl.when(wanted(z, s, j))
        def _():
            @pl.when(whole(s, j))
            def _():
                final_copy().wait_recv()

            @pl.when(jnp.logical_not(whole(s, j)))
            def _():
                y_copy(s, j).wait_recv()

            core_copy(s, j, 1).start()

    def project(s, j):
        part = jnp.dot(
            abuf[pl.ds(0, rows_own)], wbuf[s, j], preferred_element_type=jnp.float32
        )
        at = lax.rem(s, owned)

        @pl.when(s // owned == t)
        def _():
            pbuf[at, j] = part

        @pl.when(s // owned != t)
        def _():
            xsend[at, j] = part.astype(jnp.bfloat16)
            x_copy(s, j, xsend.at[at, j]).start()

    def project_guest(s, j):
        part = jnp.dot(
            abuf[pl.ds(rows_own, rows_own)], wbuf[s, j], preferred_element_type=jnp.float32
        )
        f = place(guest, s, j)
        k = sum_at(guest, s, j)
        add = summed(guest, s, j)
        mine = s // owned == t

        @pl.when(jnp.logical_not(add))
        def _():
            csend[f] = part.astype(jnp.bfloat16)

            @pl.when(f == end_place)
            def _():
                for i in range(spans):
                    c_part(i).start()

            @pl.when(f != end_place)
            def _():
                c_copy(f).start()

        @pl.when(both(add, mine))
        def _():
            gpart[k] = part

        @pl.when(both(add, jnp.logical_not(mine)))
        def _():
            gsend[k] = part.astype(jnp.bfloat16)
            g_copy(k).start()

    def pass_sum(f):
        s, j = source(f - parts)

        @pl.when(s // owned == t)
        def _():
            f = place(guest, s, j)
            k = sum_at(guest, s, j)
            g_copy(k).wait_recv()
            csend[f] = (gpart[k] + grecv[k].astype(jnp.float32)).astype(jnp.bfloat16)
            c_copy(f).start()

    def gathered(s, j):
        core_arrival(s, j).wait_recv()
        project(s, j)

    def gather_project(s, j):
        @pl.when(wanted(z, s, j))
        def _():
            gathered(s, j)

        @pl.when(jnp.logical_not(jnp.logical_or(wanted(z, s, j), summed(z, s, j))))
        def _():
            f = place(z, s, j)
            away = s // owned != t

            @pl.when(f == end_place)
            def _():
                for i in range(spans):
                    c_part(i).wait_recv()

                    @pl.when(away)
                    def _(i=i):
                        x_part(i, lax.rem(s, owned), j).start()

            @pl.when(f != end_place)
            def _():
                c_copy(f).wait_recv()

                @pl.when(away)
                def _():
                    x_copy(s, j, cbuf.at[f]).start()

    mine = t * owned
    near = z // owned == t
    front = jnp.where(near, z, jnp.where(inward > 0, mine, mine + owned - 1))
    rear = 2 * mine + owned - 1 - front

    def finish(q):
        behind, j = order(q)
        behind = jnp.logical_or(both(near, q >= parts), both(jnp.logical_not(near), behind))
        s, j = jnp.where(behind, rear, front), jnp.where(near, lax.rem(q, parts), j)
        at = lax.rem(s, owned)
        whole_sum = both(is_end, summed(z, s, j))

        @pl.when(whole_sum)
        def _():
            c_copy(place(z, s, j)).wait_recv()

        split = both(is_end, place(z, s, j) == end_place)

        @pl.when(split)
        def _():
            for i in range(spans):
                x_part(i, at, j).wait_recv()

        @pl.when(jnp.logical_not(jnp.logical_or(whole_sum, split)))
        def _():
            x_copy(s, j, xsend.at[at, j]).wait_recv()

        where = pl.ds(pl.multiple_of(at * cols + j * sub, 128), sub)

        def put(total):
            for i in range(spans):
                span = pl.ds(i * tok, tok)
                out_ref[span, where] = (total(span) * gates[i, :, where]).astype(out_ref.dtype)

        def other(span):
            return xbuf[at, j, span, :].astype(jnp.float32)

        def guests(span):
            return cbuf[place(z, s, j), span, :].astype(jnp.float32)

        @pl.when(wanted(z, s, j))
        def _():
            put(lambda span: pbuf[at, j, span, :] + other(span))

        @pl.when(whole_sum)
        def _():
            put(guests)

        @pl.when(jnp.logical_not(jnp.logical_or(wanted(z, s, j), whole_sum)))
        def _():
            put(lambda span: guests(span) + other(span))

        put_copy(s, j).start()

    lag, most = 2, 3
    gap = jnp.where(c == 0, 2, 3)
    lead = per_kv * tok
    units = spans * kvh
    pace = max(parts // 6, 1)

    def inner(e):
        s, j = source(e)

        @pl.when(both(e >= 0, e < length))
        def _():
            arrive(s, j, inward)

    def outer(e):
        @pl.when(both(e >= 0, e < ahead))
        def _():
            arrive(guest, e, -inward)

    @pl.when(is_end)
    def _():
        for d in range(1, n):
            for g in range(kvh):
                receive(z + inward * d, g, way_out)

    @pl.when(is_host)
    def _():
        for g in range(kvh):
            receive(guest, g, way_in)
            receive(z + inward, g, way_out)
        own_weights(way_in, 0, parts - 1)
        for g in range(kvh):
            receive(z + 2 * inward, g, way_out)
        own_weights(way_out, 0, keep)
        for k in range(pace):
            outer(k)
            inner(k)

    local_q().wait()
    local_noise().wait()
    for i in range(spans):
        gates[i] = noise_ref[pl.ds(plan_ref[first + i], 1), :]

    @pl.when(c != 0)
    def _():
        kv_all = kvbuf.at[:, :, :, pl.ds(0, spans)]
        remote(kv_all, kv_all, kvc_send, kvc_recv, {"span": 1 - c}).wait_recv()

    def relay_in(e):
        @pl.when(both(e >= 0, e < length))
        def _():
            pass_on(*source(e))

        @pl.when(both(is_host, both(e >= 0, e < late)))
        def _():
            pass_on(guest, e)

    def attend(u, carry):
        i, g = u // kvh, u % kvh
        query = q_ref[i, pl.ds(g * per_kv, per_kv)].reshape(lead, hd)

        def fold(k, state):
            top, total, mixed = state
            keys = kvbuf[:, g, 0, k].reshape(n * tok, hd)
            values = kvbuf[:, g, 1, k].reshape(n * tok, hd)
            scores = lax.dot_general(
                query, keys, (((1,), (1,)), ((), ())), preferred_element_type=jnp.float32
            )
            high = jnp.maximum(top, jnp.max(scores, axis=1, keepdims=True))
            shrink = jnp.exp2((top - high) * scale)
            weights = jnp.exp2((scores - high) * scale)
            total = total * shrink + jnp.sum(weights, axis=1, keepdims=True)
            mixed = mixed * shrink + jnp.dot(
                weights.astype(jnp.bfloat16), values, preferred_element_type=jnp.float32
            )
            return high, total, mixed

        start = (
            jnp.full((lead, 1), -1e30, jnp.float32),
            jnp.zeros((lead, 1), jnp.float32),
            jnp.zeros((lead, hd), jnp.float32),
        )
        _, total, mixed = lax.fori_loop(0, first + i + 1, fold, start)
        result = (mixed / total).astype(jnp.bfloat16).reshape(per_kv, tok, hd)
        for h in range(per_kv):
            abuf[
                pl.ds(pl.multiple_of(i * tok, tok), tok),
                pl.ds(pl.multiple_of((g * per_kv + h) * hd, hd), hd),
            ] = result[h]

        @pl.when(both(is_end, g == kvh - 1))
        def _():
            a_copy(i).start()

        @pl.when(is_host)
        def _():
            for k in range(pace):
                outer((u + 1) * pace + k)
                inner((u + 1) * pace + k)
                relay_in((u + 1) * pace + k - lag)

        @pl.when(both(is_end, c != 0))
        def _():
            for k in range(pace):
                inner((u - 1) * pace + k)

        return carry

    lax.fori_loop(0, units, attend, 0)

    @pl.when(is_end)
    def _():
        done = jnp.where(c == 0, 0, min((units - 1) * pace, keep))
        lax.fori_loop(done, keep, lambda e, carry: (inner(e), carry)[1], 0)

    def own(j, carry):
        project(z, j)
        return carry

    all_w().wait()
    lax.fori_loop(0, jnp.where(is_end, parts, 0), own, 0)

    turn = jnp.where(c == 0, 4 * pace, 6 * pace)
    shift, due, sums, go, own_at = 3 * pace, 9 * pace, 2 * parts, 3 * pace, jnp.where(c == 0, 6 * pace, 2 * pace)

    def run(e, carry):
        @pl.when(both(is_end, e == go))
        def _():
            own_weights(way_in, ahead, parts)
            for j in range(late, parts):
                rest_copy(z, j).start()

        @pl.when(is_host)
        def _():
            @pl.when(e > units * pace)
            def _():
                inner(e)

            k = e - shift

            @pl.when(both(k >= ahead, k < parts))
            def _():
                arrive(guest, k, -inward)

            @pl.when(k == parts - 1)
            def _():
                own_weights(way_in, parts - 1, parts)
                final_copy().start()

        @pl.when(jnp.logical_or(is_end, e > units * pace))
        def _():
            relay_in(e - lag)

        @pl.when(both(is_host, e == turn))
        def _():
            rows_in = abuf.at[pl.ds(rows_own, rows_own)]
            remote(rows_in, rows_in, a_send, a_recv, {"seq": guest}).wait_recv()

            def catch_up(f, carry):
                project_guest(*source(f - parts))
                return carry

            lax.fori_loop(keep, turn - gap + parts, catch_up, 0)

        f = e - gap

        @pl.when(both(f >= 0, f < length))
        def _():
            gather_project(*source(f))

            @pl.when(both(is_host, e >= turn))
            def _():
                project_guest(*source(f))

        @pl.when(both(is_host, e == turn + 2 * pace))
        def _():
            lax.fori_loop(keep, parts, lambda f, carry: (pass_sum(f), carry)[1], 0)

        k = e - gap - 2 * pace - pick

        @pl.when(both(is_host, both(k >= 0, k < shared)))
        def _():
            pass_sum(parts + pick + k)

        k = e - own_at

        @pl.when(both(is_host, both(k >= 0, k < parts)))
        def _():
            project(z, k)

        k = e - due + late

        @pl.when(both(is_host, both(k >= late, k < parts)))
        def _():
            rest_copy(guest, k).wait_recv()
            core_copy(guest, k, 1).start()

        k = jnp.where(f < late, f, k - 1)

        @pl.when(both(is_host, both(k >= 0, jnp.logical_or(f < late, both(k >= late, k < parts)))))
        def _():
            gathered(guest, k)

        q = e - sums

        @pl.when(both(q >= 0, q < owned * parts))
        def _():
            finish(q)

        return carry

    lax.fori_loop(
        2, max(last * parts + most, due + parts - late + 1, sums + owned * parts), run, 0
    )

    piece = pl.ds(0, quarter)
    pair = pl.ds(0, 2 * quarter)

    @pl.when(is_end)
    def _():
        sent(kv_ref, kv_send.at[0])
        sent(w_ref.at[piece], wz_send.at[0])
        sent(w_ref.at[piece, pl.ds(0, (parts - late) * sub)], wf_send)
        sent(wbuf.at[0, pl.ds(0, keep), pair], wc_send)
        sent(wbuf.at[0, pl.ds(0, keep), piece], wy_send.at[0])
        sent(abuf.at[pl.ds(0, rows_own)], a_send)
        sent(csend.at[pl.ds(0, owned * parts - shared)], x_send)

    @pl.when(is_host)
    def _():
        sent(kvbuf.at[pl.ds(0, 2), :, :, pl.ds(0, spans)], kv_send.at[0])
        sent(kvbuf.at[pl.ds(0, n - 1), :, :, pl.ds(0, spans)], kv_send.at[1])
        sent(w_ref.at[piece], wz_send.at[0])
        sent(w_ref.at[piece, pl.ds(0, keep * sub)], wz_send.at[1])
        sent(wbuf.at[0, :, piece], wz_send.at[2])
        sent(wbuf.at[pl.ds(0, n - 1), :, pair], wc_send)
        sent(wbuf.at[0, pl.ds(0, parts - 1), piece], wy_send.at[0])
        sent(wbuf.at[0, :, piece], wy_send.at[2])
        sent(wbuf.at[0, 0, piece], wl_send)
        sent(w_ref.at[piece, pl.ds(0, late * sub)], wy_send.at[1])
        sent(csend.at[pl.ds(0, csend.shape[0] - shared)], c_send)
        sent(gsend, g_send)
        sent(xsend, x_send)

    @pl.when(c == 0)
    def _():
        sent(kvbuf.at[:, :, :, pl.ds(0, spans)], kvc_send)

    pltpu.make_async_copy(out_ref, out_hbm, out_sem).wait()


def fused(parts, queries, key_states, value_states, out_weight, noise_table, plan):
    spans, tok, heads, hd = queries.shape
    kvh = key_states.shape[2]
    depth, cols = out_weight.shape
    n, tps, cores = lax.axis_size("seq"), lax.axis_size("tp"), lax.axis_size("span")
    sub, owned, wide = cols // parts, n // tps, noise_table.shape[1]
    keep, late, ahead = 4 * parts // 6, parts // 6, 4 * parts // 6
    pick, shared = 3 * parts // 6, parts - keep
    extra, taken = (n - 1) * parts - keep, (n - 1) * parts
    q = jnp.transpose(queries, (0, 2, 1, 3))
    kv = jnp.stack([key_states, value_states], axis=0).transpose(3, 0, 1, 2, 4)
    where_it_is = pl.BlockSpec(memory_space=pl.ANY)
    far = pl.BlockSpec(memory_space=pltpu.HBM)
    dma = pltpu.SemaphoreType.DMA
    tile = (owned, parts, spans * tok, sub)
    out = pl.pallas_call(
        functools.partial(fused_kernel, parts, keep, late, ahead, pick),
        out_shape=jax.ShapeDtypeStruct((spans * tok, wide), jnp.bfloat16),
        in_specs=[
            pl.BlockSpec(memory_space=pltpu.SMEM), far, where_it_is, far, far,
        ],
        out_specs=where_it_is,
        scratch_shapes=[
            pltpu.VMEM((n, kvh, 2, spans * cores, tok, hd), jnp.bfloat16),
            pltpu.VMEM((n, parts, depth, sub), jnp.bfloat16),
            pltpu.VMEM((2 * spans * tok, depth), jnp.bfloat16),
            pltpu.VMEM(tile, jnp.float32),
            pltpu.VMEM(tile, jnp.bfloat16),
            pltpu.VMEM(tile, jnp.bfloat16),
            pltpu.VMEM((extra, spans * tok, sub), jnp.bfloat16),
            pltpu.VMEM((extra, spans * tok, sub), jnp.bfloat16),
            dma((2,)), dma((n, kvh)), dma, dma, dma((4,)),
            dma((3,)), dma((taken,)), dma, dma((parts,)),
            dma, dma((taken,)), dma((3,)), dma((taken,)),
            dma, dma((owned, parts)), dma, dma, dma, dma((extra,)),
            pltpu.VMEM((spans, 1, wide), jnp.float32),
            pltpu.VMEM(q.shape, q.dtype),
            pltpu.VMEM(noise_table.shape, noise_table.dtype),
            pltpu.VMEM((spans * tok, wide), jnp.bfloat16),
            dma,
            pltpu.VMEM((shared, spans * tok, sub), jnp.bfloat16),
            pltpu.VMEM((shared, spans * tok, sub), jnp.bfloat16),
            pltpu.VMEM((shared, spans * tok, sub), jnp.float32),
            dma, dma((shared,)), dma, dma, dma((spans,)), dma((spans,)),
        ],
        compiler_params=pltpu.CompilerParams(
            collective_id=0, has_side_effects=True, vmem_limit_bytes=48 * 1024 * 1024
        ),
        name="relay_attention",
    )(plan, pltpu.with_memory_space_constraint(q, pltpu.HBM), kv, pltpu.with_memory_space_constraint(noise_table, pltpu.HBM), pltpu.with_memory_space_constraint(out_weight, pltpu.HBM))
    return out.reshape(spans, tok, wide)


def fold_block(carried, query_rows, key_rows, value_rows, factor):
    maxima, totals, weighted = carried
    scores = (
        jnp.einsum("tkgd,skd->tkgs", query_rows, key_rows, preferred_element_type=jnp.float32)
        * factor
    )
    highest = jnp.maximum(maxima, jnp.max(scores, axis=-1))
    shrink = jnp.exp(maxima - highest)
    weights = jnp.exp(scores - highest[..., None])
    totals = totals * shrink + jnp.sum(weights, axis=-1)
    weighted = weighted * shrink[..., None] + jnp.einsum(
        "tkgs,skd->tkgd",
        weights.astype(jnp.bfloat16),
        value_rows,
        preferred_element_type=jnp.float32,
    )
    return (maxima * 0.0 + highest, totals, weighted)


def per_device(queries, key_states, value_states, out_weight, noise_table, plan):
    ch_dev, tok_dev, heads_local, head_size = queries.shape
    kv_local = key_states.shape[2]
    per_kv = heads_local // kv_local
    span_count = ch_dev * lax.axis_size("span")
    first_span = lax.axis_index("span") * ch_dev
    factor = head_size ** (-0.5)
    grouped = queries.reshape(ch_dev, tok_dev, kv_local, per_kv, head_size)
    start_max = jnp.full((ch_dev, tok_dev, kv_local, per_kv), -1e30, jnp.float32)
    start_tot = jnp.zeros((ch_dev, tok_dev, kv_local, per_kv), jnp.float32)
    start_acc = jnp.zeros((ch_dev, tok_dev, kv_local, per_kv, head_size), jnp.float32)
    span_rows = (
        lax.all_gather(key_states, "seq", axis=1, tiled=True),
        lax.all_gather(value_states, "seq", axis=1, tiled=True),
    )
    key_piece = lax.all_gather(span_rows[0], "span", axis=0, tiled=True)
    value_piece = lax.all_gather(span_rows[1], "span", axis=0, tiled=True)
    new_max = []
    new_tot = []
    new_acc = []
    for q_span in range(ch_dev):
        inner_state = (start_max[q_span], start_tot[q_span], start_acc[q_span])
        for k_span in range(span_count):

            def update(inner, q_span=q_span, k_span=k_span):
                return fold_block(
                    inner, grouped[q_span], key_piece[k_span], value_piece[k_span], factor
                )

            inner_state = lax.cond(
                k_span <= first_span + q_span, update, lambda inner: inner, inner_state
            )
        new_max.append(inner_state[0])
        new_tot.append(inner_state[1])
        new_acc.append(inner_state[2])
    attn = (
        (jnp.stack(new_acc) / jnp.stack(new_tot)[..., None])
        .reshape(ch_dev, tok_dev, heads_local * head_size)
        .astype(jnp.bfloat16)
    )
    columns = jnp.einsum(
        "ctf,fo->cto",
        lax.all_gather(attn, "seq", axis=1, tiled=True),
        out_weight,
        preferred_element_type=jnp.float32,
    )
    partial_out = lax.all_to_all(
        columns.astype(jnp.bfloat16), "seq", split_axis=1, concat_axis=2, tiled=True
    ).astype(columns.dtype)
    summed = lax.psum_scatter(
        partial_out.astype(jnp.bfloat16), "tp", scatter_dimension=2, tiled=True
    ).astype(jnp.float32)
    levels = lax.dynamic_slice_in_dim(plan, first_span, ch_dev)
    picks = (levels[:, None] == jnp.arange(noise_table.shape[0], dtype=jnp.int32)[None, :]).astype(
        jnp.float32
    )
    gates = jnp.dot(picks, noise_table, precision=lax.Precision.HIGHEST)
    return (summed * gates[:, None, :]).astype(jnp.bfloat16)


def choose_parts(cols):
    for parts in (6,):
        if cols % (parts * 128) == 0:
            return parts
    return 0


def dispatch(queries, key_states, value_states, out_weight, noise_table, plan):
    depth, cols = out_weight.shape
    copies = lax.axis_size("rep") * lax.axis_size("span")
    parts = choose_parts(cols)
    pairs = all(lax.axis_size(name) == 2 for name in ("rep", "span", "tp"))
    args = (queries, key_states, value_states, out_weight, noise_table, plan)
    line = lax.axis_size("seq") == 2 * lax.axis_size("tp")
    if pairs and parts and depth % (copies * 16) == 0 and line:
        return fused(parts, *args)
    return per_device(*args)


def solution(mesh):
    placed = (
        P(("rep", "span"), "seq", "tp", None),
        P(("rep", "span"), "seq", "tp", None),
        P(("rep", "span"), "seq", "tp", None),
        P("tp", "seq"),
        P(None, "tp"),
        P("rep"),
    )
    return jax.shard_map(
        dispatch,
        mesh=mesh,
        in_specs=placed,
        out_specs=P(("rep", "span"), "seq", "tp"),
        check_vma=False,
    )
```

```python
import functools
import math

import jax
import jax.numpy as jnp
from jax import lax
from jax.experimental import pallas as pl
from jax.experimental.pallas import tpu as pltpu
from jax.sharding import PartitionSpec as P

MESH = pl.DeviceIdType.MESH


def fused_kernel(
    parts, keep, late, ahead, pick, plan_ref, q_hbm, kv_ref, noise_hbm, w_ref, out_hbm,
    kvbuf, wbuf, abuf, pbuf, xsend, xbuf, csend, cbuf,
    kv_send, kv_recv, kvc_send, kvc_recv, loc, wz_send, wz_recv, wf_send, wf_recv,
    wc_send, wc_recv, wy_send, wy_recv, x_send, x_recv, a_send, a_recv, c_send, c_recv, gates,
    q_ref, noise_ref, out_ref, out_sem,
    gsend, grecv, gpart, g_send, g_recv, wl_send, wl_recv, cs_recv, xs_recv,
):
    y, c = lax.axis_index("rep"), lax.axis_index("span")
    z, t = lax.axis_index("seq"), lax.axis_index("tp")
    n = lax.axis_size("seq")
    cores, tps = lax.axis_size("span"), lax.axis_size("tp")
    spans, heads, tok, hd = q_hbm.shape
    kvh = kv_ref.shape[0]
    per_kv = heads // kvh
    depth, cols = w_ref.shape
    quarter = depth // (cores * lax.axis_size("rep"))
    sub = cols // parts
    owned = n // tps
    rows_own = spans * tok
    first = c * spans
    last = n - 1
    scale = hd ** (-0.5) * math.log2(math.e)
    both = jnp.logical_and

    is_end = jnp.logical_or(z == 0, z == last)
    is_host = jnp.logical_not(is_end)
    inward = jnp.where(2 * z < n, 1, -1)
    way_in = (1 + inward) // 2
    way_out = 1 - way_in
    guest = z - inward
    length = jnp.where(is_end, last, last - 1) * parts

    base = jnp.where(is_end, z + inward, z)

    def order(k):
        behind = both(k >= parts - 1, k < 2 * parts - 1)
        j = jnp.where(behind, k - parts + 1, jnp.minimum(k, parts - 1))
        return behind, j

    def source(e):
        k = e - jnp.where(is_end, parts, 0)
        behind, j = order(k)
        step = jnp.where(k < 0, 0, jnp.where(behind, 2, 1))
        return base + inward * step, jnp.where(k < 0, k + parts, j)

    def place(r, s, j):
        return (jnp.abs(s - r) - 1) * parts + j - keep

    def wanted(r, s, j):
        far = place(r, s, j) >= 0
        return jnp.logical_not(both(jnp.logical_or(r == 0, r == last), far))

    shared = parts - keep

    def summed(r, s, j):
        f = place(r, s, j) + keep
        k = f - parts - pick
        return jnp.logical_or(both(f >= keep, f < parts), both(k >= 0, k < shared))

    def sum_at(r, s, j):
        f = place(r, s, j) + keep
        return jnp.where(f < parts, f - keep, f - parts - pick)

    def whole(s, j):
        final = both(s == z + inward, j == parts - 1)
        return both(is_host, jnp.logical_or(both(s == guest, j >= late), final))

    def rows(yy, cc):
        return pl.ds(pl.multiple_of((yy * cores + cc) * quarter, quarter), quarter)

    def columns(j):
        return pl.ds(pl.multiple_of(j * sub, sub), sub)

    def remote(src, dst, send, recv, where):
        return pltpu.make_async_remote_copy(
            src_ref=src, dst_ref=dst, send_sem=send, recv_sem=recv,
            device_id=where, device_id_type=MESH,
        )

    def turn_of(r, s, j):
        inside = (s - r) * jnp.where(2 * r < n, 1, -1) > 0
        return jnp.where(inside, (jnp.abs(s - r) - 1) * parts, (n - 2) * parts) + j

    def sent(part, sem):
        remote(part, part, sem, sem, {"span": 1 - c}).wait_send()

    def z_copy(s, j, way, own):
        dst = wbuf.at[s, j, rows(y, c)]
        src = w_ref.at[rows(y, c), columns(j)] if own else dst
        to = z + 2 * way - 1
        group = jnp.where(way == way_in, 0, 1) if own else 2
        return remote(src, dst, wz_send.at[group], wz_recv.at[turn_of(to, s, j)], {"seq": to})

    def z_arrival(s, j):
        dst = wbuf.at[s, j, rows(y, c)]
        return remote(dst, dst, wz_send.at[2], wz_recv.at[turn_of(z, s, j)], {"seq": z + inward})

    def rest_copy(s, j):
        src = w_ref.at[rows(1 - y, c), columns(j)]
        return remote(
            src, wbuf.at[s, j, rows(1 - y, c)], wf_send, wf_recv.at[j], {"seq": z + inward}
        )

    def final_copy():
        src = w_ref.at[rows(1 - y, c), columns(parts - 1)]
        return remote(
            src, wbuf.at[z, parts - 1, rows(1 - y, c)], wl_send, wl_recv, {"seq": z + inward}
        )

    def core_copy(s, j, kind):
        part = wbuf.at[s, j, rows(y if kind == 0 else 1 - y, c)]
        return remote(part, part, wc_send, wc_recv.at[turn_of(z, s, j)], {"span": 1 - c})

    def core_arrival(s, j):
        part = wbuf.at[s, j, pl.ds(0, 2 * quarter)]
        return remote(part, part, wc_send, wc_recv.at[turn_of(z, s, j)], {"span": 1 - c})

    def y_copy(s, j):
        part = wbuf.at[s, j, rows(y, c)]
        group = jnp.where(s == guest, 1, jnp.where(s == z + 2 * inward, 2, 0))
        return remote(
            part, part, wy_send.at[group], wy_recv.at[turn_of(z, s, j)], {"rep": 1 - y}
        )

    def x_copy(s, j, src):
        at = lax.rem(s, owned)
        return remote(
            src, xbuf.at[at, j], x_send, x_recv.at[at, j], {"tp": 1 - t}
        )

    def a_copy(i):
        src = abuf.at[pl.ds(pl.multiple_of(i * tok, tok), tok)]
        dst = abuf.at[pl.ds(pl.multiple_of(rows_own + i * tok, tok), tok)]
        return remote(src, dst, a_send, a_recv, {"seq": z + inward})

    def c_copy(f):
        return remote(
            csend.at[f], cbuf.at[f], c_send, c_recv.at[f], {"seq": z - inward}
        )

    def g_copy(k):
        return remote(gsend.at[k], grecv.at[k], g_send, g_recv.at[k], {"tp": 1 - t})

    end_place = 2 * parts - 1 - keep

    def c_part(i):
        at = pl.ds(i * tok, tok)
        return remote(
            csend.at[end_place, at], cbuf.at[end_place, at], c_send, cs_recv.at[i],
            {"seq": z - inward},
        )

    def x_part(i, at, j):
        mine = pl.ds(i * tok, tok)
        return remote(
            cbuf.at[end_place, mine], xbuf.at[at, j, mine], x_send, xs_recv.at[i], {"tp": 1 - t}
        )

    def kv_copy(s, g, way, own):
        dst = kvbuf.at[s, g, :, pl.ds(first, spans)]
        src = kv_ref.at[g] if own else dst
        to = z + 2 * way - 1
        group = jnp.where(way == way_in, 0, 1)
        return remote(src, dst, kv_send.at[group], kv_recv.at[s, g], {"seq": to})

    def kv_core(s, g):
        part = kvbuf.at[s, g, :, pl.ds(0, spans)]
        return remote(part, part, kvc_send, kvc_recv, {"span": 1 - c})

    def local_w(j):
        return pltpu.make_async_copy(w_ref.at[:, columns(j)], wbuf.at[z, j], loc.at[3])

    def all_w():
        return pltpu.make_async_copy(wbuf.at[z], wbuf.at[z], loc.at[3])

    def local_q():
        return pltpu.make_async_copy(q_hbm, q_ref, loc.at[1])

    def local_noise():
        return pltpu.make_async_copy(noise_hbm, noise_ref, loc.at[2])

    def put_copy(s, j):
        at = pl.ds(pl.multiple_of(lax.rem(s, owned) * cols + j * sub, 128), sub)
        return pltpu.make_async_copy(
            out_ref.at[:, at], out_hbm.at[:, at], out_sem
        )

    def local_kv():
        return pltpu.make_async_copy(
            kv_ref, kvbuf.at[z, :, :, pl.ds(first, spans)], loc.at[0]
        )

    reach = ((0, z > 0), (1, z < last))

    barrier = pltpu.get_barrier_semaphore()
    local_kv().start()
    local_q().start()
    local_noise().start()
    for j in range(parts):
        local_w(j).start()
    for way, ok in reach:
        @pl.when(ok)
        def _(way=way):
            to = z - 1 if way == 0 else z + 1
            pl.semaphore_signal(barrier, inc=1, device_id={"seq": to}, device_id_type=MESH)
    pl.semaphore_signal(barrier, inc=1, device_id={"rep": 1 - y}, device_id_type=MESH)
    pl.semaphore_signal(barrier, inc=1, device_id={"span": 1 - c}, device_id_type=MESH)
    pl.semaphore_signal(barrier, inc=1, device_id={"tp": 1 - t}, device_id_type=MESH)
    pl.semaphore_wait(barrier, jnp.where(is_end, 4, 5))

    for g in range(kvh):
        for way, ok in reach:
            @pl.when(ok)
            def _(g=g, way=way):
                kv_copy(z, g, way, True).start()

    def own_weights(way, low, high):
        for j in range(low, high):
            z_copy(z, j, way, True).start()


    @pl.when(is_end)
    def _():
        own_weights(way_in, 0, ahead)

    local_kv().wait()

    @pl.when(c == 0)
    def _():
        for g in range(kvh):
            kv_core(z, g).start()

    def receive(s, g, way):
        kv_copy(s, g, way, False).wait_recv()
        to = z + 2 * way - 1

        @pl.when(both(to >= 0, to < n))
        def _():
            kv_copy(s, g, way, False).start()

        @pl.when(c == 0)
        def _():
            kv_core(s, g).start()

    def arrive(s, j, sign):
        way = (1 - sign) // 2
        onward = z - sign

        @pl.when(wanted(z, s, j))
        def _():
            z_arrival(s, j).wait_recv()

            @pl.when(both(both(onward >= 0, onward < n), wanted(onward, s, j)))
            def _():
                z_copy(s, j, way, False).start()

            @pl.when(jnp.logical_not(whole(s, j)))
            def _():
                y_copy(s, j).start()

            core_copy(s, j, 0).start()

    def pass_on(s, j):
        @pl.when(wanted(z, s, j))
        def _():
            @pl.when(whole(s, j))
            def _():
                final_copy().wait_recv()

            @pl.when(jnp.logical_not(whole(s, j)))
            def _():
                y_copy(s, j).wait_recv()

            core_copy(s, j, 1).start()

    def project(s, j):
        part = jnp.dot(
            abuf[pl.ds(0, rows_own)], wbuf[s, j], preferred_element_type=jnp.float32
        )
        at = lax.rem(s, owned)

        @pl.when(s // owned == t)
        def _():
            pbuf[at, j] = part

        @pl.when(s // owned != t)
        def _():
            xsend[at, j] = part.astype(jnp.bfloat16)
            x_copy(s, j, xsend.at[at, j]).start()

    def project_guest(s, j):
        part = jnp.dot(
            abuf[pl.ds(rows_own, rows_own)], wbuf[s, j], preferred_element_type=jnp.float32
        )
        f = place(guest, s, j)
        k = sum_at(guest, s, j)
        add = summed(guest, s, j)
        mine = s // owned == t

        @pl.when(jnp.logical_not(add))
        def _():
            csend[f] = part.astype(jnp.bfloat16)

            @pl.when(f == end_place)
            def _():
                for i in range(spans):
                    c_part(i).start()

            @pl.when(f != end_place)
            def _():
                c_copy(f).start()

        @pl.when(both(add, mine))
        def _():
            gpart[k] = part

        @pl.when(both(add, jnp.logical_not(mine)))
        def _():
            gsend[k] = part.astype(jnp.bfloat16)
            g_copy(k).start()

    def pass_sum(f):
        s, j = source(f - parts)

        @pl.when(s // owned == t)
        def _():
            f = place(guest, s, j)
            k = sum_at(guest, s, j)
            g_copy(k).wait_recv()
            csend[f] = (gpart[k] + grecv[k].astype(jnp.float32)).astype(jnp.bfloat16)
            c_copy(f).start()

    def gathered(s, j):
        core_arrival(s, j).wait_recv()
        project(s, j)

    def gather_project(s, j):
        @pl.when(wanted(z, s, j))
        def _():
            gathered(s, j)

        @pl.when(jnp.logical_not(jnp.logical_or(wanted(z, s, j), summed(z, s, j))))
        def _():
            f = place(z, s, j)
            away = s // owned != t

            @pl.when(f == end_place)
            def _():
                for i in range(spans):
                    c_part(i).wait_recv()

                    @pl.when(away)
                    def _(i=i):
                        x_part(i, lax.rem(s, owned), j).start()

            @pl.when(f != end_place)
            def _():
                c_copy(f).wait_recv()

                @pl.when(away)
                def _():
                    x_copy(s, j, cbuf.at[f]).start()

    mine = t * owned
    near = z // owned == t
    front = jnp.where(near, z, jnp.where(inward > 0, mine, mine + owned - 1))
    rear = 2 * mine + owned - 1 - front

    def finish(q):
        behind, j = order(q)
        behind = jnp.logical_or(both(near, q >= parts), both(jnp.logical_not(near), behind))
        s, j = jnp.where(behind, rear, front), jnp.where(near, lax.rem(q, parts), j)
        at = lax.rem(s, owned)
        whole_sum = both(is_end, summed(z, s, j))

        @pl.when(whole_sum)
        def _():
            c_copy(place(z, s, j)).wait_recv()

        split = both(is_end, place(z, s, j) == end_place)

        @pl.when(split)
        def _():
            for i in range(spans):
                x_part(i, at, j).wait_recv()

        @pl.when(jnp.logical_not(jnp.logical_or(whole_sum, split)))
        def _():
            x_copy(s, j, xsend.at[at, j]).wait_recv()

        where = pl.ds(pl.multiple_of(at * cols + j * sub, 128), sub)

        def put(total):
            for i in range(spans):
                span = pl.ds(i * tok, tok)
                out_ref[span, where] = (total(span) * gates[i, :, where]).astype(out_ref.dtype)

        def other(span):
            return xbuf[at, j, span, :].astype(jnp.float32)

        def guests(span):
            return cbuf[place(z, s, j), span, :].astype(jnp.float32)

        @pl.when(wanted(z, s, j))
        def _():
            put(lambda span: pbuf[at, j, span, :] + other(span))

        @pl.when(whole_sum)
        def _():
            put(guests)

        @pl.when(jnp.logical_not(jnp.logical_or(wanted(z, s, j), whole_sum)))
        def _():
            put(lambda span: guests(span) + other(span))

        put_copy(s, j).start()

    lag, most = 2, 3
    gap = jnp.where(c == 0, 2, 3)
    lead = per_kv * tok
    units = spans * kvh
    pace = max(parts // 6, 1)

    def inner(e):
        s, j = source(e)

        @pl.when(both(e >= 0, e < length))
        def _():
            arrive(s, j, inward)

    def outer(e):
        @pl.when(both(e >= 0, e < ahead))
        def _():
            arrive(guest, e, -inward)

    @pl.when(is_end)
    def _():
        for d in range(1, n):
            for g in range(kvh):
                receive(z + inward * d, g, way_out)

    @pl.when(is_host)
    def _():
        for g in range(kvh):
            receive(guest, g, way_in)
            receive(z + inward, g, way_out)
        own_weights(way_in, 0, parts - 1)
        for g in range(kvh):
            receive(z + 2 * inward, g, way_out)
        own_weights(way_out, 0, keep)
        for k in range(pace):
            outer(k)
            inner(k)

    local_q().wait()
    local_noise().wait()
    for i in range(spans):
        gates[i] = noise_ref[pl.ds(plan_ref[first + i], 1), :]

    @pl.when(c != 0)
    def _():
        kv_all = kvbuf.at[:, :, :, pl.ds(0, spans)]
        remote(kv_all, kv_all, kvc_send, kvc_recv, {"span": 1 - c}).wait_recv()

    def relay_in(e):
        @pl.when(both(e >= 0, e < length))
        def _():
            pass_on(*source(e))

        @pl.when(both(is_host, both(e >= 0, e < late)))
        def _():
            pass_on(guest, e)

    def attend(u, carry):
        i, g = u // kvh, u % kvh
        query = q_ref[i, pl.ds(g * per_kv, per_kv)].reshape(lead, hd)

        def fold(k, state):
            top, total, mixed = state
            keys = kvbuf[:, g, 0, k].reshape(n * tok, hd)
            values = kvbuf[:, g, 1, k].reshape(n * tok, hd)
            scores = lax.dot_general(
                query, keys, (((1,), (1,)), ((), ())), preferred_element_type=jnp.float32
            )
            high = jnp.maximum(top, jnp.max(scores, axis=1, keepdims=True))
            shrink = jnp.exp2((top - high) * scale)
            weights = jnp.exp2((scores - high) * scale)
            total = total * shrink + jnp.sum(weights, axis=1, keepdims=True)
            mixed = mixed * shrink + jnp.dot(
                weights.astype(jnp.bfloat16), values, preferred_element_type=jnp.float32
            )
            return high, total, mixed

        start = (
            jnp.full((lead, 1), -1e30, jnp.float32),
            jnp.zeros((lead, 1), jnp.float32),
            jnp.zeros((lead, hd), jnp.float32),
        )
        _, total, mixed = lax.fori_loop(0, first + i + 1, fold, start)
        result = (mixed / total).astype(jnp.bfloat16).reshape(per_kv, tok, hd)
        for h in range(per_kv):
            abuf[
                pl.ds(pl.multiple_of(i * tok, tok), tok),
                pl.ds(pl.multiple_of((g * per_kv + h) * hd, hd), hd),
            ] = result[h]

        @pl.when(both(is_end, g == kvh - 1))
        def _():
            a_copy(i).start()

        @pl.when(is_host)
        def _():
            for k in range(pace):
                outer((u + 1) * pace + k)
                inner((u + 1) * pace + k)
                relay_in((u + 1) * pace + k - lag)

        @pl.when(both(is_end, c != 0))
        def _():
            for k in range(pace):
                inner((u - 1) * pace + k)

        return carry

    lax.fori_loop(0, units, attend, 0)

    @pl.when(is_end)
    def _():
        done = jnp.where(c == 0, 0, min((units - 1) * pace, keep))
        lax.fori_loop(done, keep, lambda e, carry: (inner(e), carry)[1], 0)

    def own(j, carry):
        project(z, j)
        return carry

    all_w().wait()
    lax.fori_loop(0, jnp.where(is_end, parts, 0), own, 0)

    turn = jnp.where(c == 0, 4 * pace, 6 * pace)
    shift, due, sums, go, own_at = 3 * pace, 9 * pace, 2 * parts, 3 * pace, jnp.where(c == 0, 6 * pace, 2 * pace)

    def run(e, carry):
        @pl.when(both(is_end, e == go))
        def _():
            own_weights(way_in, ahead, parts)
            for j in range(late, parts):
                rest_copy(z, j).start()

        @pl.when(is_host)
        def _():
            @pl.when(e > units * pace)
            def _():
                inner(e)

            k = e - shift

            @pl.when(both(k >= ahead, k < parts))
            def _():
                arrive(guest, k, -inward)

            @pl.when(k == parts - 1)
            def _():
                own_weights(way_in, parts - 1, parts)
                final_copy().start()

        @pl.when(jnp.logical_or(is_end, e > units * pace))
        def _():
            relay_in(e - lag)

        @pl.when(both(is_host, e == turn))
        def _():
            rows_in = abuf.at[pl.ds(rows_own, rows_own)]
            remote(rows_in, rows_in, a_send, a_recv, {"seq": guest}).wait_recv()

            def catch_up(f, carry):
                project_guest(*source(f - parts))
                return carry

            lax.fori_loop(keep, turn - gap + parts, catch_up, 0)

        f = e - gap

        @pl.when(both(f >= 0, f < length))
        def _():
            gather_project(*source(f))

            @pl.when(both(is_host, e >= turn))
            def _():
                project_guest(*source(f))

        @pl.when(both(is_host, e == turn + 2 * pace))
        def _():
            lax.fori_loop(keep, parts, lambda f, carry: (pass_sum(f), carry)[1], 0)

        k = e - gap - 2 * pace - pick

        @pl.when(both(is_host, both(k >= 0, k < shared)))
        def _():
            pass_sum(parts + pick + k)

        k = e - own_at

        @pl.when(both(is_host, both(k >= 0, k < parts)))
        def _():
            project(z, k)

        k = e - due + late

        @pl.when(both(is_host, both(k >= late, k < parts)))
        def _():
            rest_copy(guest, k).wait_recv()
            core_copy(guest, k, 1).start()

        k = jnp.where(f < late, f, k - 1)

        @pl.when(both(is_host, both(k >= 0, jnp.logical_or(f < late, both(k >= late, k < parts)))))
        def _():
            gathered(guest, k)

        q = e - sums

        @pl.when(both(q >= 0, q < owned * parts))
        def _():
            finish(q)

        return carry

    lax.fori_loop(
        2, max(last * parts + most, due + parts - late + 1, sums + owned * parts), run, 0
    )

    piece = pl.ds(0, quarter)
    pair = pl.ds(0, 2 * quarter)

    @pl.when(is_end)
    def _():
        sent(kv_ref, kv_send.at[0])
        sent(w_ref.at[piece], wz_send.at[0])
        sent(w_ref.at[piece, pl.ds(0, (parts - late) * sub)], wf_send)
        sent(wbuf.at[0, pl.ds(0, keep), pair], wc_send)
        sent(wbuf.at[0, pl.ds(0, keep), piece], wy_send.at[0])
        sent(abuf.at[pl.ds(0, rows_own)], a_send)
        sent(csend.at[pl.ds(0, owned * parts - shared)], x_send)

    @pl.when(is_host)
    def _():
        sent(kvbuf.at[pl.ds(0, 2), :, :, pl.ds(0, spans)], kv_send.at[0])
        sent(kvbuf.at[pl.ds(0, n - 1), :, :, pl.ds(0, spans)], kv_send.at[1])
        sent(w_ref.at[piece], wz_send.at[0])
        sent(w_ref.at[piece, pl.ds(0, keep * sub)], wz_send.at[1])
        sent(wbuf.at[0, :, piece], wz_send.at[2])
        sent(wbuf.at[pl.ds(0, n - 1), :, pair], wc_send)
        sent(wbuf.at[0, pl.ds(0, parts - 1), piece], wy_send.at[0])
        sent(wbuf.at[0, :, piece], wy_send.at[2])
        sent(wbuf.at[0, 0, piece], wl_send)
        sent(w_ref.at[piece, pl.ds(0, late * sub)], wy_send.at[1])
        sent(csend.at[pl.ds(0, csend.shape[0] - shared)], c_send)
        sent(gsend, g_send)
        sent(xsend, x_send)

    @pl.when(c == 0)
    def _():
        sent(kvbuf.at[:, :, :, pl.ds(0, spans)], kvc_send)

    pltpu.make_async_copy(out_ref, out_hbm, out_sem).wait()


def fused(parts, queries, key_states, value_states, out_weight, noise_table, plan):
    spans, tok, heads, hd = queries.shape
    kvh = key_states.shape[2]
    depth, cols = out_weight.shape
    n, tps, cores = lax.axis_size("seq"), lax.axis_size("tp"), lax.axis_size("span")
    sub, owned, wide = cols // parts, n // tps, noise_table.shape[1]
    keep, late, ahead = 4 * parts // 6, parts // 6, 4 * parts // 6
    pick, shared = 3 * parts // 6, parts - keep
    extra, taken = (n - 1) * parts - keep, (n - 1) * parts
    q = jnp.transpose(queries, (0, 2, 1, 3))
    kv = jnp.stack([key_states, value_states], axis=0).transpose(3, 0, 1, 2, 4)
    where_it_is = pl.BlockSpec(memory_space=pl.ANY)
    far = pl.BlockSpec(memory_space=pltpu.HBM)
    dma = pltpu.SemaphoreType.DMA
    tile = (owned, parts, spans * tok, sub)
    out = pl.pallas_call(
        functools.partial(fused_kernel, parts, keep, late, ahead, pick),
        out_shape=jax.ShapeDtypeStruct((spans * tok, wide), jnp.bfloat16),
        in_specs=[
            pl.BlockSpec(memory_space=pltpu.SMEM), far, where_it_is, far, far,
        ],
        out_specs=where_it_is,
        scratch_shapes=[
            pltpu.VMEM((n, kvh, 2, spans * cores, tok, hd), jnp.bfloat16),
            pltpu.VMEM((n, parts, depth, sub), jnp.bfloat16),
            pltpu.VMEM((2 * spans * tok, depth), jnp.bfloat16),
            pltpu.VMEM(tile, jnp.float32),
            pltpu.VMEM(tile, jnp.bfloat16),
            pltpu.VMEM(tile, jnp.bfloat16),
            pltpu.VMEM((extra, spans * tok, sub), jnp.bfloat16),
            pltpu.VMEM((extra, spans * tok, sub), jnp.bfloat16),
            dma((2,)), dma((n, kvh)), dma, dma, dma((4,)),
            dma((3,)), dma((taken,)), dma, dma((parts,)),
            dma, dma((taken,)), dma((3,)), dma((taken,)),
            dma, dma((owned, parts)), dma, dma, dma, dma((extra,)),
            pltpu.VMEM((spans, 1, wide), jnp.float32),
            pltpu.VMEM(q.shape, q.dtype),
            pltpu.VMEM(noise_table.shape, noise_table.dtype),
            pltpu.VMEM((spans * tok, wide), jnp.bfloat16),
            dma,
            pltpu.VMEM((shared, spans * tok, sub), jnp.bfloat16),
            pltpu.VMEM((shared, spans * tok, sub), jnp.bfloat16),
            pltpu.VMEM((shared, spans * tok, sub), jnp.float32),
            dma, dma((shared,)), dma, dma, dma((spans,)), dma((spans,)),
        ],
        compiler_params=pltpu.CompilerParams(
            collective_id=0, has_side_effects=True, vmem_limit_bytes=48 * 1024 * 1024
        ),
        name="relay_attention",
    )(plan, pltpu.with_memory_space_constraint(q, pltpu.HBM), kv, pltpu.with_memory_space_constraint(noise_table, pltpu.HBM), pltpu.with_memory_space_constraint(out_weight, pltpu.HBM))
    return out.reshape(spans, tok, wide)


def fold_block(carried, query_rows, key_rows, value_rows, factor):
    maxima, totals, weighted = carried
    scores = (
        jnp.einsum("tkgd,skd->tkgs", query_rows, key_rows, preferred_element_type=jnp.float32)
        * factor
    )
    highest = jnp.maximum(maxima, jnp.max(scores, axis=-1))
    shrink = jnp.exp(maxima - highest)
    weights = jnp.exp(scores - highest[..., None])
    totals = totals * shrink + jnp.sum(weights, axis=-1)
    weighted = weighted * shrink[..., None] + jnp.einsum(
        "tkgs,skd->tkgd",
        weights.astype(jnp.bfloat16),
        value_rows,
        preferred_element_type=jnp.float32,
    )
    return (maxima * 0.0 + highest, totals, weighted)


def per_device(queries, key_states, value_states, out_weight, noise_table, plan):
    ch_dev, tok_dev, heads_local, head_size = queries.shape
    kv_local = key_states.shape[2]
    per_kv = heads_local // kv_local
    span_count = ch_dev * lax.axis_size("span")
    first_span = lax.axis_index("span") * ch_dev
    factor = head_size ** (-0.5)
    grouped = queries.reshape(ch_dev, tok_dev, kv_local, per_kv, head_size)
    start_max = jnp.full((ch_dev, tok_dev, kv_local, per_kv), -1e30, jnp.float32)
    start_tot = jnp.zeros((ch_dev, tok_dev, kv_local, per_kv), jnp.float32)
    start_acc = jnp.zeros((ch_dev, tok_dev, kv_local, per_kv, head_size), jnp.float32)
    span_rows = (
        lax.all_gather(key_states, "seq", axis=1, tiled=True),
        lax.all_gather(value_states, "seq", axis=1, tiled=True),
    )
    key_piece = lax.all_gather(span_rows[0], "span", axis=0, tiled=True)
    value_piece = lax.all_gather(span_rows[1], "span", axis=0, tiled=True)
    new_max = []
    new_tot = []
    new_acc = []
    for q_span in range(ch_dev):
        inner_state = (start_max[q_span], start_tot[q_span], start_acc[q_span])
        for k_span in range(span_count):

            def update(inner, q_span=q_span, k_span=k_span):
                return fold_block(
                    inner, grouped[q_span], key_piece[k_span], value_piece[k_span], factor
                )

            inner_state = lax.cond(
                k_span <= first_span + q_span, update, lambda inner: inner, inner_state
            )
        new_max.append(inner_state[0])
        new_tot.append(inner_state[1])
        new_acc.append(inner_state[2])
    attn = (
        (jnp.stack(new_acc) / jnp.stack(new_tot)[..., None])
        .reshape(ch_dev, tok_dev, heads_local * head_size)
        .astype(jnp.bfloat16)
    )
    columns = jnp.einsum(
        "ctf,fo->cto",
        lax.all_gather(attn, "seq", axis=1, tiled=True),
        out_weight,
        preferred_element_type=jnp.float32,
    )
    partial_out = lax.all_to_all(
        columns.astype(jnp.bfloat16), "seq", split_axis=1, concat_axis=2, tiled=True
    ).astype(columns.dtype)
    summed = lax.psum_scatter(
        partial_out.astype(jnp.bfloat16), "tp", scatter_dimension=2, tiled=True
    ).astype(jnp.float32)
    levels = lax.dynamic_slice_in_dim(plan, first_span, ch_dev)
    picks = (levels[:, None] == jnp.arange(noise_table.shape[0], dtype=jnp.int32)[None, :]).astype(
        jnp.float32
    )
    gates = jnp.dot(picks, noise_table, precision=lax.Precision.HIGHEST)
    return (summed * gates[:, None, :]).astype(jnp.bfloat16)


def choose_parts(cols):
    for parts in (6,):
        if cols % (parts * 128) == 0:
            return parts
    return 0


def dispatch(queries, key_states, value_states, out_weight, noise_table, plan):
    depth, cols = out_weight.shape
    copies = lax.axis_size("rep") * lax.axis_size("span")
    parts = choose_parts(cols)
    pairs = all(lax.axis_size(name) == 2 for name in ("rep", "span", "tp"))
    args = (queries, key_states, value_states, out_weight, noise_table, plan)
    line = lax.axis_size("seq") == 2 * lax.axis_size("tp")
    if pairs and parts and depth % (copies * 16) == 0 and line:
        return fused(parts, *args)
    return per_device(*args)


def solution(mesh):
    placed = (
        P(("rep", "span"), "seq", "tp", None),
        P(("rep", "span"), "seq", "tp", None),
        P(("rep", "span"), "seq", "tp", None),
        P("tp", "seq"),
        P(None, "tp"),
        P("rep"),
    )
    return jax.shard_map(
        dispatch,
        mesh=mesh,
        in_specs=placed,
        out_specs=P(("rep", "span"), "seq", "tp"),
        check_vma=False,
    )
```
